128 devices in a mesh: dp: 16 (over x, z), expert: 8 (over y, core).
Axes of the slice: x: 4, y: 4, z: 4, core: 2. Of those that a mesh axis runs over, the one named last changes fastest.
Arguments:
- tokens: bfloat16 [16384, 4096], P(('dp', 'expert')), may hold values from -6 to 6
- select: int32 [8, 512], P(None, ('dp', 'expert')), may hold values from -1 to 127, as said below
- gates: float32 [8, 512], P(None, ('dp', 'expert')), may hold values from 0.1 to 1
- w_gate: bfloat16 [8, 4096, 8192], P('expert', None, 'dp'), may hold values from -0.09375 to 0.09375
- w_up: bfloat16 [8, 4096, 8192], P('expert', None, 'dp'), may hold values from -0.09375 to 0.09375
- w_down: bfloat16 [8, 8192, 4096], P('expert', 'dp'), may hold values from -0.0625 to 0.0625
Outputs:
- mixed: bfloat16 [16384, 4096], P(('dp', 'expert'))
The draws below stay inside these ranges and needn't reach their ends.
Inputs may be any that keep to these rules, and one draw needn't show every extreme that they name: `select`: in each block of 4 slots of a row, the live entries come first, distinct and ascending, below 128, followed by -1; every block holds at least one live entry, and every expert fills all 4 slots of some source device.
All inputs are finite; a program needn't handle non-finite values.
Results may differ from the reference program's by a relative error of at most 0.0085.
Values may be sent and summed in bfloat16 or wider, within the bound.
A program may use at most 64 MiB of HBM per device.

```python
import jax
import jax.numpy as jnp

D = 4096
FF = 8192
TOK_DEV = 128
EXPERTS = 8
SLOT = 4
TOKENS = 16384
DEVICES = 128


def draw_select(key, part):
    keys_all = jax.random.split(jax.random.fold_in(key, 11), EXPERTS * DEVICES)

    def one_block(sub_key):
        chosen = jax.random.permutation(sub_key, TOK_DEV)[:SLOT]
        return jnp.sort(chosen)
    picks = jax.vmap(one_block)(keys_all).reshape(EXPERTS, DEVICES, SLOT)
    counts = jax.random.randint(jax.random.fold_in(key, 7), (EXPERTS, DEVICES), 1, SLOT + 1)
    full_src = (jnp.arange(EXPERTS)[:, None] * 37 + 3) % DEVICES
    counts = jnp.where(jnp.arange(DEVICES)[None, :] == full_src, SLOT, counts)
    slot_pos = jnp.arange(SLOT)
    result = jnp.where(slot_pos[None, None, :] < counts[:, :, None], picks, -1)
    return result.reshape(EXPERTS, DEVICES * SLOT).astype(jnp.int32)


def steps_of(key, dims, cuts, least, top_value):
    def one(axis_at, shards_of):
        draws = jax.random.uniform(jax.random.fold_in(jax.random.fold_in(key, 6), axis_at), (shards_of,), jnp.float32, least / len(cuts), top_value / len(cuts))
        return jnp.repeat(jnp.exp(draws), dims[axis_at] // shards_of).reshape((-1,) + (1,) * (len(dims) - axis_at - 1))

    level = one(*cuts[0])
    for cut in cuts[1:]:
        level = level * one(*cut)
    return level


def bell_draw(own_key, extent, scale, bound, pieces=(), held_as=jnp.bfloat16):
    values = jax.random.normal(own_key, extent, jnp.float32) * scale
    if len(pieces) > 0:
        values = steps_of(own_key, extent, pieces, -0.22, 0.18) * values
    return jnp.clip(values, min=-bound, max=bound).astype(held_as)


def setup_inputs(seed: int = 0) -> dict:
    key_of = jax.random.split(jax.random.key(seed), 7)
    tokens = bell_draw(key_of[0], (TOKENS, D), 1.0, 6.0, ((0, 128),))
    select = draw_select(jax.random.fold_in(key_of[6], 71), 0)
    gates = jnp.clip(0.1 + 0.9 * jax.random.uniform(key_of[2], (EXPERTS, DEVICES * SLOT), jnp.float32) ** steps_of(key_of[2], (EXPERTS, DEVICES * SLOT), ((1, 128),), -0.2, 0.2), 0.1, 1.0)
    w_gate = bell_draw(key_of[3], (EXPERTS, D, FF), D ** -0.5, 0.09375, ((0, 8), (2, 16)))
    w_up = bell_draw(key_of[4], (EXPERTS, D, FF), D ** -0.5, 0.09375, ((0, 8), (2, 16)))
    w_down = bell_draw(key_of[5], (EXPERTS, FF, D), FF ** -0.5, 0.0625, ((0, 8), (1, 16)))
    return {"tokens": tokens, "select": select, "gates": gates, "w_gate": w_gate, "w_up": w_up, "w_down": w_down}


def reference(tokens, select, gates, w_gate, w_up, w_down):
    mixed = jnp.zeros((TOKENS, D), jnp.float32)
    source = (jnp.arange(DEVICES * SLOT) // SLOT).astype(jnp.int32)
    for expert_id in range(EXPERTS):
        index_row = select[expert_id]
        is_live = index_row >= 0
        global_idx = (source * TOK_DEV + jnp.where(is_live, index_row, 0)).astype(jnp.int32)
        sel_rows = jnp.where(is_live[:, None], tokens[global_idx], 0).astype(jnp.bfloat16)
        gate_val = jnp.dot(sel_rows, w_gate[expert_id], preferred_element_type=jnp.float32)
        up_val = jnp.dot(sel_rows, w_up[expert_id], preferred_element_type=jnp.float32)
        hidden = (jax.nn.silu(gate_val) * up_val).astype(jnp.bfloat16)
        expert_out = jnp.dot(hidden, w_down[expert_id], preferred_element_type=jnp.float32).astype(jnp.bfloat16)
        weight_col = jnp.where(is_live, gates[expert_id], 0.0).astype(jnp.float32)
        mixed = mixed.at[global_idx].add(weight_col[:, None] * expert_out.astype(jnp.float32))
    return mixed.astype(jnp.bfloat16)
```

```python
import functools

import jax
import jax.numpy as jnp
from jax import lax
from jax.experimental import pallas as pl
from jax.experimental.pallas import tpu as pltpu
from jax.sharding import PartitionSpec as P

MESH = pl.DeviceIdType.MESH
BF16, F32 = jnp.bfloat16, jnp.float32
RING = 4
N_SEM = 256
RSET, LSET = (0, 3), (2, 1)


def kernel(
    sel_ref, gate_ref, tok_ref, wg_ref, wu_ref, wd_ref, out_ref,
    wg_v, wu_v, wd_v, send4, recv4, ret4, rows, part, hid, relay, fin_l, fin_r, summed,
    relay1, fin1_l, fin1_r, slots32, comb, send_sem, recv_sem, w_sem,
):
    slot = sel_ref.shape[1]
    tok_dev, width = tok_ref.shape
    groups = 2 * RING
    n_slots = groups * slot
    halfw = width // 2
    quart = width // 4
    chunk = rows.shape[2]

    dp = lax.axis_index("dp")
    ex = lax.axis_index("expert")
    my_x, my_z = dp // RING, dp % RING
    my_y, my_c = ex // 2, ex % 2

    def at_x(step):
        return (((my_x + step + RING) % RING) * RING + my_z, ex)

    def at_z(step):
        return (my_x * RING + (my_z + step + RING) % RING, ex)

    def expert_at(g):
        return ((my_y + g // 2) % RING) * 2 + (my_c + g % 2) % 2

    def at_group(g):
        return (dp, expert_at(g))

    def back(g):
        return ((RING - g // 2) % RING) * 2 + g % 2

    barrier = pltpu.get_barrier_semaphore()
    partners = [at_x(1), at_x(-1), at_z(1), at_z(-1)] + [at_group(g) for g in range(1, groups)]
    for who in partners:
        pl.semaphore_signal(barrier, inc=1, device_id=who, device_id_type=MESH)

    loads = [
        pltpu.make_async_copy(wg_ref, wg_v, w_sem.at[0]),
        pltpu.make_async_copy(wu_ref, wu_v, w_sem.at[1]),
        pltpu.make_async_copy(wd_ref, wd_v, w_sem.at[2]),
    ]
    for load in loads:
        load.start()

    used = []

    def remote(src, dst, who):
        i = len(used)
        copy = pltpu.make_async_remote_copy(
            src_ref=src, dst_ref=dst, send_sem=send_sem.at[i], recv_sem=recv_sem.at[i],
            device_id=who, device_id_type=MESH,
        )
        used.append(copy)
        copy.start()
        return copy

    row_id = lax.broadcasted_iota(jnp.int32, (n_slots, tok_dev), 0)
    lane_id = lax.broadcasted_iota(jnp.int32, (n_slots, tok_dev), 1)
    idx = jnp.full((n_slots, tok_dev), -1, jnp.int32)
    lane8 = lax.broadcasted_iota(jnp.int32, (8, 128), 1)
    idx_l = jnp.full((8, 128), -1, jnp.int32)
    gate_l = jnp.zeros((8, 128), F32)
    for g in range(groups):
        e = expert_at(g)
        for j in range(slot):
            k = g * slot + j
            v = sel_ref[e, j]
            idx = jnp.where(row_id == k, v, idx)
            here = lane8 % n_slots == k
            idx_l = jnp.where(here, v, idx_l)
            gate_l = jnp.where(here, gate_ref[e, j], gate_l)
    onehot = jnp.where(lane_id == idx, 1.0, 0.0).astype(BF16)
    for c in range(0, width, 1024):
        cols = slice(c, c + 1024)
        slots32[:, cols] = jnp.dot(onehot, tok_ref[:, cols], preferred_element_type=F32)
    recv4[0] = slots32[0:slot, :].astype(BF16)
    for g in range(1, groups):
        send4[g] = slots32[g * slot : (g + 1) * slot, :].astype(BF16)

    pl.semaphore_wait(barrier, len(partners))
    near = [1, 6, 7]
    far = [4, 5, 2, 3]
    sent = {}
    for g in near + far:
        sent[g] = remote(send4.at[g], recv4.at[back(g)], at_group(g))

    g1 = gate_l.astype(BF16).astype(F32)
    rest = gate_l - g1
    g2 = rest.astype(BF16).astype(F32)
    g3 = (rest - g2).astype(BF16).astype(F32)
    term = lane8 // n_slots
    gate3 = jnp.where(term == 0, g1, jnp.where(term == 1, g2, jnp.where(term == 2, g3, 0.0)))
    tok_id = lax.broadcasted_iota(jnp.int32, (tok_dev, 128), 0)
    hit = tok_id == idx_l[0:1, :]
    comb[...] = jnp.where(hit, gate3[0:1, :], 0.0).astype(BF16)

    def cut(p, lo=0, n=halfw):
        return pl.ds(p * halfw + lo, n)

    def pos(p, d1, d2):
        d1, d2 = d1 % RING, d2 % RING
        return d2 * RING + d1 if p == 0 else d1 * RING + d2

    def first(p, step):
        return at_x(step) if p == 0 else at_z(step)

    def second(p, step):
        return at_z(step) if p == 0 else at_x(step)

    def to_first(h, p, d1, step, lo=0, n=halfw):
        return remote(
            rows.at[h, pos(p, d1, 0), :, cut(p, lo, n)],
            rows.at[h, pos(p, d1 - step, 0), :, cut(p, lo, n)], first(p, step),
        )

    def to_second(h, p, d1, d2, step):
        return remote(
            rows.at[h, pos(p, d1, d2), :, cut(p)],
            rows.at[h, pos(p, d1, d2 - step), :, cut(p)], second(p, step),
        )

    got = {}

    def enter(h):
        for g in range(4 * h, 4 * h + 4):
            if g > 0:
                sent[back(g)].wait_recv()
        for i in range(4):
            slots32[i * slot : (i + 1) * slot, :] = recv4[4 * h + i].astype(F32)
        rows[h, 0] = slots32[0:chunk, :].astype(BF16)

    def gather0(h):
        for p in range(2):
            for step in (1, -1):
                got[h, p, "f", step] = to_first(h, p, 0, step)
        for p in range(2):
            for step in (1, -1):
                got[h, p, "s", 0, step] = to_second(h, p, 0, 0, step)

    def gather1(h):
        for p in range(2):
            for step, lo in ((1, 0), (-1, quart)):
                got[h, p, "f", step].wait_recv()
                got[h, p, "r", step] = to_first(h, p, -step, step, lo, quart)
        for p in range(2):
            for d1 in (-1, 1):
                for step in (1, -1):
                    got[h, p, "s", d1 % RING, step] = to_second(h, p, d1, 0, step)

    def relay2(h, p, d1):
        step = 1 if d1 in RSET else -1
        got[h, p, "s", d1, step].wait_recv()
        got[h, p, "t", d1] = to_second(h, p, d1, -step, step)

    def gather2(h):
        for p in range(2):
            for step in (1, -1):
                got[h, p, "r", step].wait_recv()
            for step in (1, -1):
                got[h, p, "s", 2, step] = to_second(h, p, 2, 0, step)

    def relays(h, which):
        for d1 in which:
            for p in range(2):
                relay2(h, p, d1)

    def gathered(h):
        for p in range(2):
            for d1 in range(RING):
                step = -1 if d1 in RSET else 1
                got[h, p, "s", d1, step].wait_recv()
        for p in range(2):
            for d1 in range(RING):
                got[h, p, "t", d1].wait_recv()

    ff = hid.shape[1]
    tn = 256

    def up_piece(h, n):
        lhs = rows[h].reshape(RING * RING * chunk, width)
        gate_val = jnp.dot(lhs, wg_v[:, n * tn : (n + 1) * tn], preferred_element_type=F32)
        up_val = jnp.dot(lhs, wu_v[:, n * tn : (n + 1) * tn], preferred_element_type=F32)
        act = gate_val / (1.0 + jnp.exp(-gate_val)) * up_val
        hid[:, n * tn : (n + 1) * tn] = act.astype(BF16)

    dn = 512

    def down_piece(h, n):
        cols = slice(n * dn, (n + 1) * dn)
        val = jnp.dot(hid[...], wd_v[:, cols], preferred_element_type=F32)
        part[h, :, :, cols] = val.astype(BF16).reshape(RING * RING, chunk, dn)

    red = {}

    def scatter0(h, p):
        for d1r, d1l in zip(RSET, LSET):
            red[h, p, "far", d1r] = remote(
                part.at[h, pos(p, d1r, 2), :, cut(p)], relay.at[h, p, d1r], second(p, 1))
            red[h, p, "far", d1l] = remote(
                part.at[h, pos(p, d1l, 2), :, cut(p)], relay.at[h, p, d1l], second(p, -1))
        for d1r, d1l in zip(RSET, LSET):
            red[h, p, "l", d1l] = remote(
                part.at[h, pos(p, d1l, 1), :, cut(p)], fin_l.at[h, p, d1l], second(p, 1))
            red[h, p, "r", d1r] = remote(
                part.at[h, pos(p, d1r, 3), :, cut(p)], fin_r.at[h, p, d1r], second(p, -1))

    def scatter1(h, p, d1):
        red[h, p, "far", d1].wait_recv()
        right = d1 in RSET
        own = part[h, pos(p, d1, 1 if right else 3), :, cut(p)]
        relay[h, p, d1] = (relay[h, p, d1].astype(F32) + own.astype(F32)).astype(BF16)
        if right:
            red[h, p, "l", d1] = remote(relay.at[h, p, d1], fin_l.at[h, p, d1], second(p, 1))
        else:
            red[h, p, "r", d1] = remote(relay.at[h, p, d1], fin_r.at[h, p, d1], second(p, -1))

    def scatter2(h, p, d1):
        red[h, p, "l", d1].wait_recv()
        red[h, p, "r", d1].wait_recv()
        own = part[h, pos(p, d1, 0), :, cut(p)]
        total = own.astype(F32) + fin_l[h, p, d1].astype(F32) + fin_r[h, p, d1].astype(F32)
        summed[h, p, d1] = total.astype(BF16)
        lo, hi = pl.ds(0, quart), pl.ds(quart, quart)
        if d1 == 2:
            red[h, p, "far1", 1] = remote(
                summed.at[h, p, 2, :, lo], relay1.at[h, p, :, lo], first(p, 1))
            red[h, p, "far1", -1] = remote(
                summed.at[h, p, 2, :, hi], relay1.at[h, p, :, hi], first(p, -1))
        elif d1 == 1:
            red[h, p, "l1", 1] = remote(
                summed.at[h, p, 1, :, hi], fin1_l.at[h, p, :, hi], first(p, 1))
        elif d1 == 3:
            red[h, p, "r1", 0] = remote(
                summed.at[h, p, 3, :, lo], fin1_r.at[h, p, :, lo], first(p, -1))

    def scatter3(h, p):
        for step, at, d1 in ((1, 0, 1), (-1, quart, 3)):
            cols = pl.ds(at, quart)
            red[h, p, "far1", step].wait_recv()
            relay1[h, p, :, cols] = (
                relay1[h, p, :, cols].astype(F32) + summed[h, p, d1, :, cols].astype(F32)
            ).astype(BF16)
            if step == 1:
                red[h, p, "l1", 0] = remote(
                    relay1.at[h, p, :, cols], fin1_l.at[h, p, :, cols], first(p, 1))
            else:
                red[h, p, "r1", 1] = remote(
                    relay1.at[h, p, :, cols], fin1_r.at[h, p, :, cols], first(p, -1))

    def scatter4(h, p):
        for i in range(2):
            red[h, p, "l1", i].wait_recv()
            red[h, p, "r1", i].wait_recv()
        total = (
            summed[h, p, 0].astype(F32) + fin1_l[h, p].astype(F32) + fin1_r[h, p].astype(F32)
        )
        slots32[0:chunk, cut(p)] = total

    returned = {}

    def leave(h):
        for i in range(4):
            g = 4 * h + i
            value = slots32[i * slot : (i + 1) * slot, :].astype(BF16)
            if g == 0:
                ret4[0] = value
            else:
                send4[g] = value
                returned[g] = remote(send4.at[g], ret4.at[back(g)], at_group(g))

    def sums(h, d1s):
        for d1 in d1s:
            for p in range(2):
                scatter2(h, p, d1)

    enter(0)
    gather0(0)
    enter(1)
    gather0(1)
    gather1(0)
    relays(0, (0,))
    gather2(0)
    relays(0, (3, 1, 2))
    gather1(1)
    relays(1, (0,))
    gathered(0)
    for load in loads:
        load.wait()
    up_piece(0, 0)
    gather2(1)
    relays(1, (3, 1))
    up_piece(0, 1)
    relays(1, (2,))
    n_down = width // dn
    for n in range(n_down // 2):
        down_piece(0, n)
    scatter0(0, 0)
    for n in range(n_down // 2, n_down):
        down_piece(0, n)
    scatter0(0, 1)
    gathered(1)
    up_piece(1, 0)
    for d1 in (2, 3, 1, 0):
        for p in range(2):
            scatter1(0, p, d1)
    up_piece(1, 1)
    for n in range(n_down // 2):
        down_piece(1, n)
    scatter0(1, 0)
    for n in range(n_down // 2, n_down):
        down_piece(1, n)
    scatter0(1, 1)
    sums(0, (2, 1, 3, 0))
    for p in range(2):
        scatter3(0, p)
    for d1 in (2, 3, 1, 0):
        for p in range(2):
            scatter1(1, p, d1)
    for p in range(2):
        scatter4(0, p)
    for g in range(1, groups):
        sent[g].wait_send()
    leave(0)
    sums(1, (2, 1, 3, 0))
    for p in range(2):
        scatter3(1, p)
    for p in range(2):
        scatter4(1, p)
    leave(1)

    for g in range(1, groups):
        returned[g].wait_recv()
    for g in range(groups):
        slots32[g * slot : (g + 1) * slot, :] = ret4[g].astype(F32)
    for c in range(0, width, 512):
        cols = slice(c, c + 512)
        value = slots32[:, cols].astype(BF16)
        stack = jnp.concatenate([value, value, value, jnp.zeros_like(value)], axis=0)
        out_ref[:, cols] = jnp.dot(comb[...], stack, preferred_element_type=F32).astype(BF16)

    firsts = [sent[g] for g in range(1, groups)]
    for copy in used:
        if not any(copy is f for f in firsts):
            copy.wait_send()


def per_device(tokens, select, gates, w_gate, w_up, w_down):
    tok_dev, width = tokens.shape
    slot = select.shape[1]
    ff = w_gate.shape[2]
    chunk = RING * slot
    halfw, quart = width // 2, width // 4
    vmem, any_ = pl.BlockSpec(memory_space=pltpu.VMEM), pl.BlockSpec(memory_space=pl.ANY)
    smem = pl.BlockSpec(memory_space=pltpu.SMEM)
    return pl.pallas_call(
        kernel,
        out_shape=jax.ShapeDtypeStruct((tok_dev, width), BF16),
        in_specs=[smem, smem, vmem, any_, any_, any_],
        out_specs=vmem,
        scratch_shapes=[
            pltpu.VMEM((width, ff), BF16),
            pltpu.VMEM((width, ff), BF16),
            pltpu.VMEM((ff, width), BF16),
            pltpu.VMEM((8, slot, width), BF16),
            pltpu.VMEM((8, slot, width), BF16),
            pltpu.VMEM((8, slot, width), BF16),
            pltpu.VMEM((2, 16, chunk, width), BF16),
            pltpu.VMEM((2, 16, chunk, width), BF16),
            pltpu.VMEM((16 * chunk, ff), BF16),
            pltpu.VMEM((2, 2, 4, chunk, halfw), BF16),
            pltpu.VMEM((2, 2, 4, chunk, halfw), BF16),
            pltpu.VMEM((2, 2, 4, chunk, halfw), BF16),
            pltpu.VMEM((2, 2, 4, chunk, halfw), BF16),
            pltpu.VMEM((2, 2, chunk, halfw), BF16),
            pltpu.VMEM((2, 2, chunk, halfw), BF16),
            pltpu.VMEM((2, 2, chunk, halfw), BF16),
            pltpu.VMEM((8 * slot, width), F32),
            pltpu.VMEM((tok_dev, 128), BF16),
            pltpu.SemaphoreType.DMA((N_SEM,)),
            pltpu.SemaphoreType.DMA((N_SEM,)),
            pltpu.SemaphoreType.DMA((3,)),
        ],
        compiler_params=pltpu.CompilerParams(
            collective_id=0, has_side_effects=True, vmem_limit_bytes=60 * 1024 * 1024
        ),
        name="moe",
    )(
        select, gates, tokens, w_gate[0], w_up[0], w_down[0],
    )


def solution(mesh):
    return jax.shard_map(
        per_device,
        mesh=mesh,
        in_specs=(
            P(("dp", "expert"), None),
            P(None, ("dp", "expert")),
            P(None, ("dp", "expert")),
            P("expert", None, "dp"),
            P("expert", None, "dp"),
            P("expert", "dp", None),
        ),
        out_specs=P(("dp", "expert"), None),
        check_vma=False,
    )
```

```python
import functools

import jax
import jax.numpy as jnp
from jax import lax
from jax.experimental import pallas as pl
from jax.experimental.pallas import tpu as pltpu
from jax.sharding import PartitionSpec as P

MESH = pl.DeviceIdType.MESH
BF16, F32 = jnp.bfloat16, jnp.float32
RING = 4
N_SEM = 256
RSET, LSET = (0, 3), (2, 1)


def kernel(
    sel_ref, gate_ref, tok_ref, wg_ref, wu_ref, wd_ref, out_ref,
    wg_v, wu_v, wd_v, send4, recv4, ret4, rows, part, hid, relay, fin_l, fin_r, summed,
    relay1, fin1_l, fin1_r, slots32, comb, send_sem, recv_sem, w_sem,
):
    slot = sel_ref.shape[0]
    tok_dev, width = tok_ref.shape
    groups = 2 * RING
    n_slots = groups * slot
    halfw = width // 2
    quart = width // 4
    chunk = rows.shape[2]

    dp = lax.axis_index("dp")
    ex = lax.axis_index("expert")
    my_x, my_z = dp // RING, dp % RING
    my_y, my_c = ex // 2, ex % 2

    def at_x(step):
        return (((my_x + step + RING) % RING) * RING + my_z, ex)

    def at_z(step):
        return (my_x * RING + (my_z + step + RING) % RING, ex)

    def expert_at(g):
        return ((my_y + g // 2) % RING) * 2 + (my_c + g % 2) % 2

    def at_group(g):
        return (dp, expert_at(g))

    def back(g):
        return ((RING - g // 2) % RING) * 2 + g % 2

    barrier = pltpu.get_barrier_semaphore()
    partners = [at_x(1), at_x(-1), at_z(1), at_z(-1)] + [at_group(g) for g in range(1, groups)]
    for who in partners:
        pl.semaphore_signal(barrier, inc=1, device_id=who, device_id_type=MESH)

    loads = [
        pltpu.make_async_copy(wg_ref, wg_v, w_sem.at[0]),
        pltpu.make_async_copy(wu_ref, wu_v, w_sem.at[1]),
        pltpu.make_async_copy(wd_ref, wd_v, w_sem.at[2]),
    ]
    for load in loads:
        load.start()

    used = []

    def remote(src, dst, who):
        i = len(used)
        copy = pltpu.make_async_remote_copy(
            src_ref=src, dst_ref=dst, send_sem=send_sem.at[i], recv_sem=recv_sem.at[i],
            device_id=who, device_id_type=MESH,
        )
        used.append(copy)
        copy.start()
        return copy

    row_id = lax.broadcasted_iota(jnp.int32, (n_slots, tok_dev), 0)
    lane_id = lax.broadcasted_iota(jnp.int32, (n_slots, tok_dev), 1)
    idx = jnp.full((n_slots, tok_dev), -1, jnp.int32)
    lane8 = lax.broadcasted_iota(jnp.int32, (8, 128), 1)
    idx_l = jnp.full((8, 128), -1, jnp.int32)
    gate_l = jnp.zeros((8, 128), F32)
    for g in range(groups):
        e = expert_at(g)
        for j in range(slot):
            k = g * slot + j
            v = sel_ref[j, e]
            idx = jnp.where(row_id == k, v, idx)
            here = lane8 % n_slots == k
            idx_l = jnp.where(here, v, idx_l)
            gate_l = jnp.where(here, gate_ref[j, e], gate_l)
    onehot = jnp.where(lane_id == idx, 1.0, 0.0).astype(BF16)
    for c in range(0, width, 1024):
        cols = slice(c, c + 1024)
        slots32[:, cols] = jnp.dot(onehot, tok_ref[:, cols], preferred_element_type=F32)
    recv4[0] = slots32[0:slot, :].astype(BF16)
    for g in range(1, groups):
        send4[g] = slots32[g * slot : (g + 1) * slot, :].astype(BF16)

    with jax.named_scope("barrier"):
        pl.semaphore_wait(barrier, len(partners))
    near = [1, 6, 7]
    far = [4, 5, 2, 3]
    sent = {}
    for g in near + far:
        sent[g] = remote(send4.at[g], recv4.at[back(g)], at_group(g))

    g1 = gate_l.astype(BF16).astype(F32)
    rest = gate_l - g1
    g2 = rest.astype(BF16).astype(F32)
    g3 = (rest - g2).astype(BF16).astype(F32)
    term = lane8 // n_slots
    gate3 = jnp.where(term == 0, g1, jnp.where(term == 1, g2, jnp.where(term == 2, g3, 0.0)))
    tok_id = lax.broadcasted_iota(jnp.int32, (tok_dev, 128), 0)
    hit = tok_id == idx_l[0:1, :]
    comb[...] = jnp.where(hit, gate3[0:1, :], 0.0).astype(BF16)

    def cut(p, lo=0, n=halfw):
        return pl.ds(p * halfw + lo, n)

    def pos(p, d1, d2):
        d1, d2 = d1 % RING, d2 % RING
        return d2 * RING + d1 if p == 0 else d1 * RING + d2

    def first(p, step):
        return at_x(step) if p == 0 else at_z(step)

    def second(p, step):
        return at_z(step) if p == 0 else at_x(step)

    def to_first(h, p, d1, step, lo=0, n=halfw):
        return remote(
            rows.at[h, pos(p, d1, 0), :, cut(p, lo, n)],
            rows.at[h, pos(p, d1 - step, 0), :, cut(p, lo, n)], first(p, step),
        )

    def to_second(h, p, d1, d2, step):
        return remote(
            rows.at[h, pos(p, d1, d2), :, cut(p)],
            rows.at[h, pos(p, d1, d2 - step), :, cut(p)], second(p, step),
        )

    got = {}

    def enter(h):
        for g in range(4 * h, 4 * h + 4):
            if g > 0:
                sent[back(g)].wait_recv()
        for i in range(4):
            slots32[i * slot : (i + 1) * slot, :] = recv4[4 * h + i].astype(F32)
        rows[h, 0] = slots32[0:chunk, :].astype(BF16)

    def gather0(h):
        for p in range(2):
            for step in (1, -1):
                got[h, p, "f", step] = to_first(h, p, 0, step)
        for p in range(2):
            for step in (1, -1):
                got[h, p, "s", 0, step] = to_second(h, p, 0, 0, step)

    def gather1(h):
        for p in range(2):
            for step, lo in ((1, 0), (-1, quart)):
                got[h, p, "f", step].wait_recv()
                got[h, p, "r", step] = to_first(h, p, -step, step, lo, quart)
        for p in range(2):
            for d1 in (-1, 1):
                for step in (1, -1):
                    got[h, p, "s", d1 % RING, step] = to_second(h, p, d1, 0, step)

    def relay2(h, p, d1):
        step = 1 if d1 in RSET else -1
        got[h, p, "s", d1, step].wait_recv()
        got[h, p, "t", d1] = to_second(h, p, d1, -step, step)

    def gather2(h):
        for p in range(2):
            for step in (1, -1):
                got[h, p, "r", step].wait_recv()
            for step in (1, -1):
                got[h, p, "s", 2, step] = to_second(h, p, 2, 0, step)

    def relays(h, which):
        for d1 in which:
            for p in range(2):
                relay2(h, p, d1)

    def gathered(h):
        for p in range(2):
            for d1 in range(RING):
                step = -1 if d1 in RSET else 1
                got[h, p, "s", d1, step].wait_recv()
        for p in range(2):
            for d1 in range(RING):
                got[h, p, "t", d1].wait_recv()

    ff = hid.shape[1]
    tn = 256

    def up_piece(h, n):
        lhs = rows[h].reshape(RING * RING * chunk, width)
        gate_val = jnp.dot(lhs, wg_v[:, n * tn : (n + 1) * tn], preferred_element_type=F32)
        up_val = jnp.dot(lhs, wu_v[:, n * tn : (n + 1) * tn], preferred_element_type=F32)
        act = gate_val / (1.0 + jnp.exp(-gate_val)) * up_val
        hid[:, n * tn : (n + 1) * tn] = act.astype(BF16)

    dn = 512

    def down_piece(h, n):
        cols = slice(n * dn, (n + 1) * dn)
        val = jnp.dot(hid[...], wd_v[:, cols], preferred_element_type=F32)
        part[h, :, :, cols] = val.astype(BF16).reshape(RING * RING, chunk, dn)

    red = {}

    def scatter0(h, p):
        for d1r, d1l in zip(RSET, LSET):
            red[h, p, "far", d1r] = remote(
                part.at[h, pos(p, d1r, 2), :, cut(p)], relay.at[h, p, d1r], second(p, 1))
            red[h, p, "far", d1l] = remote(
                part.at[h, pos(p, d1l, 2), :, cut(p)], relay.at[h, p, d1l], second(p, -1))
        for d1r, d1l in zip(RSET, LSET):
            red[h, p, "l", d1l] = remote(
                part.at[h, pos(p, d1l, 1), :, cut(p)], fin_l.at[h, p, d1l], second(p, 1))
            red[h, p, "r", d1r] = remote(
                part.at[h, pos(p, d1r, 3), :, cut(p)], fin_r.at[h, p, d1r], second(p, -1))

    def scatter1(h, p, d1):
        red[h, p, "far", d1].wait_recv()
        right = d1 in RSET
        own = part[h, pos(p, d1, 1 if right else 3), :, cut(p)]
        relay[h, p, d1] = (relay[h, p, d1].astype(F32) + own.astype(F32)).astype(BF16)
        if right:
            red[h, p, "l", d1] = remote(relay.at[h, p, d1], fin_l.at[h, p, d1], second(p, 1))
        else:
            red[h, p, "r", d1] = remote(relay.at[h, p, d1], fin_r.at[h, p, d1], second(p, -1))

    def scatter2(h, p, d1):
        red[h, p, "l", d1].wait_recv()
        red[h, p, "r", d1].wait_recv()
        own = part[h, pos(p, d1, 0), :, cut(p)]
        total = own.astype(F32) + fin_l[h, p, d1].astype(F32) + fin_r[h, p, d1].astype(F32)
        summed[h, p, d1] = total.astype(BF16)
        lo, hi = pl.ds(0, quart), pl.ds(quart, quart)
        if d1 == 2:
            red[h, p, "far1", 1] = remote(
                summed.at[h, p, 2, :, lo], relay1.at[h, p, :, lo], first(p, 1))
            red[h, p, "far1", -1] = remote(
                summed.at[h, p, 2, :, hi], relay1.at[h, p, :, hi], first(p, -1))
        elif d1 == 1:
            red[h, p, "l1", 1] = remote(
                summed.at[h, p, 1, :, hi], fin1_l.at[h, p, :, hi], first(p, 1))
        elif d1 == 3:
            red[h, p, "r1", 0] = remote(
                summed.at[h, p, 3, :, lo], fin1_r.at[h, p, :, lo], first(p, -1))

    def scatter3(h, p):
        for step, at, d1 in ((1, 0, 1), (-1, quart, 3)):
            cols = pl.ds(at, quart)
            red[h, p, "far1", step].wait_recv()
            relay1[h, p, :, cols] = (
                relay1[h, p, :, cols].astype(F32) + summed[h, p, d1, :, cols].astype(F32)
            ).astype(BF16)
            if step == 1:
                red[h, p, "l1", 0] = remote(
                    relay1.at[h, p, :, cols], fin1_l.at[h, p, :, cols], first(p, 1))
            else:
                red[h, p, "r1", 1] = remote(
                    relay1.at[h, p, :, cols], fin1_r.at[h, p, :, cols], first(p, -1))

    def scatter4(h, p):
        for i in range(2):
            red[h, p, "l1", i].wait_recv()
            red[h, p, "r1", i].wait_recv()
        total = (
            summed[h, p, 0].astype(F32) + fin1_l[h, p].astype(F32) + fin1_r[h, p].astype(F32)
        )
        slots32[0:chunk, cut(p)] = total

    returned = {}

    def leave(h):
        for i in range(4):
            g = 4 * h + i
            value = slots32[i * slot : (i + 1) * slot, :].astype(BF16)
            if g == 0:
                ret4[0] = value
            else:
                send4[g] = value
                returned[g] = remote(send4.at[g], ret4.at[back(g)], at_group(g))

    def sums(h, d1s):
        for d1 in d1s:
            for p in range(2):
                scatter2(h, p, d1)

    n_down = width // dn

    def downs(h, p):
        for n in range(p * n_down // 2, (p + 1) * n_down // 2):
            down_piece(h, n)
        scatter0(h, p)

    def weights():
        for load in loads:
            load.wait()

    def relay_adds(h):
        for d1 in (2, 3, 1, 0):
            for p in range(2):
                scatter1(h, p, d1)

    def both(step, h):
        for p in range(2):
            step(h, p)

    def sent_slots():
        for g in range(1, groups):
            sent[g].wait_send()

    for name, step, *args in (
        ("enter0", enter, 0),
        ("g0_0", gather0, 0),
        ("enter1", enter, 1),
        ("g0_1", gather0, 1),
        ("g1_0", gather1, 0),
        ("rel0_0", relays, 0, (0,)),
        ("g2_0", gather2, 0),
        ("rel0", relays, 0, (3, 1, 2)),
        ("g1_1", gather1, 1),
        ("rel1_0", relays, 1, (0,)),
        ("gathered0", gathered, 0),
        ("weights", weights),
        ("up0_0", up_piece, 0, 0),
        ("g2_1", gather2, 1),
        ("rel1_31", relays, 1, (3, 1)),
        ("up0_1", up_piece, 0, 1),
        ("rel1_2", relays, 1, (2,)),
        ("down0_0", downs, 0, 0),
        ("down0_1", downs, 0, 1),
        ("gathered1", gathered, 1),
        ("up1_0", up_piece, 1, 0),
        ("add0", relay_adds, 0),
        ("up1_1", up_piece, 1, 1),
        ("down1_0", downs, 1, 0),
        ("down1_1", downs, 1, 1),
        ("sums0", sums, 0, (2, 1, 3, 0)),
        ("s3_0", both, scatter3, 0),
        ("add1", relay_adds, 1),
        ("s4_0", both, scatter4, 0),
        ("sent", sent_slots),
        ("leave0", leave, 0),
        ("sums1", sums, 1, (2, 1, 3, 0)),
        ("s3_1", both, scatter3, 1),
        ("s4_1", both, scatter4, 1),
        ("leave1", leave, 1),
    ):
        with jax.named_scope(name):
            step(*args)

    with jax.named_scope("returned"):
        for g in range(1, groups):
            returned[g].wait_recv()
    for g in range(groups):
        slots32[g * slot : (g + 1) * slot, :] = ret4[g].astype(F32)
    for c in range(0, width, 512):
        cols = slice(c, c + 512)
        value = slots32[:, cols].astype(BF16)
        stack = jnp.concatenate([value, value, value, jnp.zeros_like(value)], axis=0)
        out_ref[:, cols] = jnp.dot(comb[...], stack, preferred_element_type=F32).astype(BF16)

    firsts = [sent[g] for g in range(1, groups)]
    for copy in used:
        if not any(copy is f for f in firsts):
            copy.wait_send()


def per_device(tokens, select, gates, w_gate, w_up, w_down):
    tok_dev, width = tokens.shape
    slot = select.shape[1]
    ff = w_gate.shape[2]
    chunk = RING * slot
    halfw, quart = width // 2, width // 4
    vmem, any_ = pl.BlockSpec(memory_space=pltpu.VMEM), pl.BlockSpec(memory_space=pl.ANY)
    smem = pl.BlockSpec(memory_space=pltpu.SMEM)
    return pl.pallas_call(
        kernel,
        out_shape=jax.ShapeDtypeStruct((tok_dev, width), BF16),
        in_specs=[smem, smem, vmem, any_, any_, any_],
        out_specs=vmem,
        scratch_shapes=[
            pltpu.VMEM((width, ff), BF16),
            pltpu.VMEM((width, ff), BF16),
            pltpu.VMEM((ff, width), BF16),
            pltpu.VMEM((8, slot, width), BF16),
            pltpu.VMEM((8, slot, width), BF16),
            pltpu.VMEM((8, slot, width), BF16),
            pltpu.VMEM((2, 16, chunk, width), BF16),
            pltpu.VMEM((2, 16, chunk, width), BF16),
            pltpu.VMEM((16 * chunk, ff), BF16),
            pltpu.VMEM((2, 2, 4, chunk, halfw), BF16),
            pltpu.VMEM((2, 2, 4, chunk, halfw), BF16),
            pltpu.VMEM((2, 2, 4, chunk, halfw), BF16),
            pltpu.VMEM((2, 2, 4, chunk, halfw), BF16),
            pltpu.VMEM((2, 2, chunk, halfw), BF16),
            pltpu.VMEM((2, 2, chunk, halfw), BF16),
            pltpu.VMEM((2, 2, chunk, halfw), BF16),
            pltpu.VMEM((8 * slot, width), F32),
            pltpu.VMEM((tok_dev, 128), BF16),
            pltpu.SemaphoreType.DMA((N_SEM,)),
            pltpu.SemaphoreType.DMA((N_SEM,)),
            pltpu.SemaphoreType.DMA((3,)),
        ],
        compiler_params=pltpu.CompilerParams(
            collective_id=0, has_side_effects=True, vmem_limit_bytes=60 * 1024 * 1024
        ),
        name="moe",
    )(
        select.T, gates.T, tokens, w_gate[0], w_up[0], w_down[0],
    )


def solution(mesh):
    return jax.shard_map(
        per_device,
        mesh=mesh,
        in_specs=(
            P(("dp", "expert"), None),
            P(None, ("dp", "expert")),
            P(None, ("dp", "expert")),
            P("expert", None, "dp"),
            P("expert", None, "dp"),
            P("expert", "dp", None),
        ),
        out_specs=P(("dp", "expert"), None),
        check_vma=False,
    )
```

```python
import jax
import jax.numpy as jnp
from jax import lax
from jax.experimental import pallas as pl
from jax.experimental.pallas import tpu as pltpu
from jax.sharding import PartitionSpec as P

MESH = pl.DeviceIdType.MESH
BF16, F32 = jnp.bfloat16, jnp.float32
RING = 4
SUB = 2
N_SEM = 320
RSET, LSET = (0, 3), (2, 1)
HALVES = ((0, 1, 2, 6), (3, 7, 4, 5))

ORDER = (
    ("own", 0), ("f", 0, 0, -1), ("f", 0, 1, -1), ("f", 0, 0, 1), ("f", 0, 1, 1), ("s", 0, 1, 0, 1),
    ("s", 0, 1, 0, -1), ("s", 0, 0, 0, -1), ("s", 0, 0, 0, 1), ("own", 1), ("s", 1, 1, 0, 1), ("f", 1, 1, -1),
    ("f", 1, 0, 1), ("s", 1, 0, 0, 1), ("f", 1, 0, -1), ("s", 1, 1, 0, -1), ("f", 1, 1, 1), ("s", 1, 0, 0, -1),
    ("r", 0, 0, -1), ("s", 0, 1, 1, -1), ("r", 0, 1, -1), ("r", 0, 0, 1), ("r", 0, 1, 1), ("s", 0, 1, 3, 1),
    ("s", 0, 1, 3, -1), ("s", 0, 0, 1, 1), ("s", 0, 1, 1, 1), ("s", 0, 0, 3, -1), ("s", 0, 0, 3, 1),
    ("s", 0, 0, 1, -1), ("t", 0, 1, 0), ("t", 0, 0, 0), ("r", 1, 0, -1), ("r", 1, 1, -1), ("s", 1, 1, 1, -1),
    ("t", 1, 1, 0), ("s", 1, 1, 1, 1), ("t", 1, 0, 0), ("s", 1, 0, 1, -1), ("s", 1, 0, 1, 1), ("s", 1, 0, 3, 1),
    ("s", 1, 1, 3, 1), ("r", 1, 1, 1), ("s", 1, 0, 3, -1), ("r", 1, 0, 1), ("s", 1, 1, 3, -1), ("s", 0, 0, 2, -1),
    ("s", 0, 0, 2, 1), ("s", 0, 1, 2, 1), ("s", 0, 1, 2, -1), ("t", 0, 1, 1), ("t", 0, 1, 3), ("t", 0, 0, 1),
    ("t", 0, 0, 3), ("t", 1, 1, 1), ("t", 1, 0, 1), ("t", 0, 1, 2), ("t", 0, 0, 2), ("t", 1, 1, 3), ("t", 1, 0, 3),
    ("s", 1, 0, 2, 1), ("s", 1, 1, 2, -1), ("s", 1, 0, 2, -1), ("s", 1, 1, 2, 1), ("up", 0, 0), ("up", 0, 1),
    ("t", 1, 1, 2), ("t", 1, 0, 2), ("down", 0, 0, 1), ("L", 0, 0, 2, 1), ("F", 0, 0, 0, 1), ("F", 0, 0, 3, 1),
    ("down", 0, 0, 0), ("F", 0, 0, 1, 0), ("F", 0, 0, 2, 0), ("R", 0, 0, 3, 1), ("L", 0, 0, 1, 1), ("R", 0, 0, 3, 0),
    ("F", 0, 0, 3, 0), ("R", 0, 0, 0, 1), ("down", 0, 1, 0), ("F", 0, 1, 2, 0), ("L", 0, 1, 1, 0), ("L", 0, 1, 2, 0),
    ("F", 0, 1, 1, 0), ("F", 0, 1, 3, 0), ("R", 0, 1, 0, 0), ("F", 0, 0, 2, 1), ("F", 0, 0, 1, 1), ("F", 0, 1, 0, 0),
    ("R", 0, 1, 3, 0), ("down", 0, 1, 1), ("F", 0, 1, 2, 1), ("R", 0, 1, 3, 1), ("L", 0, 1, 2, 1), ("L", 0, 1, 1, 1),
    ("F", 0, 1, 1, 1), ("F", 0, 1, 0, 1), ("L", 0, 0, 1, 0), ("R", 0, 1, 0, 1), ("L", 0, 0, 2, 0), ("F", 0, 0, 0, 0),
    ("F", 0, 1, 3, 1), ("R", 0, 0, 0, 0), ("up", 1, 0), ("A", 0, 0, 1, 0), ("up", 1, 1), ("down", 1, 1, 0),
    ("R", 1, 1, 3, 0), ("F", 1, 1, 3, 0), ("F", 1, 1, 0, 0), ("F", 1, 1, 2, 0), ("down", 1, 0, 1), ("F", 1, 0, 2, 1),
    ("R", 1, 0, 0, 1), ("F", 1, 0, 3, 1), ("L", 1, 0, 2, 1), ("down", 1, 0, 0), ("L", 1, 0, 2, 0), ("F", 1, 0, 3, 0),
    ("R", 1, 0, 3, 0), ("A", 0, 1, 2, 1), ("R", 1, 0, 0, 0), ("A", 0, 1, 1, 0), ("F", 1, 0, 2, 0), ("L", 1, 1, 2, 0),
    ("L", 1, 1, 1, 0), ("down", 1, 1, 1), ("A", 0, 0, 2, 1), ("L", 1, 1, 2, 1), ("F", 1, 1, 2, 1), ("F", 1, 1, 3, 1),
    ("L", 1, 1, 1, 1), ("A", 0, 0, 3, 1), ("R", 1, 1, 3, 1), ("F", 1, 1, 1, 0), ("R", 1, 0, 3, 1), ("F", 1, 0, 0, 1),
    ("A", 0, 0, 2, 0), ("L", 1, 0, 1, 0), ("F", 1, 0, 1, 0), ("F", 1, 1, 1, 1), ("A", 0, 1, 2, 0), ("L", 1, 0, 1, 1),
    ("F", 1, 1, 0, 1), ("F", 1, 0, 0, 0), ("F", 1, 0, 1, 1), ("R", 1, 1, 0, 1), ("R", 1, 1, 0, 0), ("A", 0, 1, 0, 0),
    ("A", 0, 0, 3, 0), ("A", 0, 0, 0, 0), ("A", 0, 0, 0, 1), ("A", 0, 1, 3, 0), ("A", 0, 1, 0, 1), ("A", 0, 1, 1, 1),
    ("A", 0, 0, 1, 1), ("A", 0, 1, 3, 1), ("A", 1, 1, 3, 0), ("S", 0, 0, 1, 0), ("A", 1, 0, 3, 1), ("A", 1, 1, 0, 0),
    ("A", 1, 1, 2, 0), ("A", 1, 0, 2, 1), ("S", 0, 1, 2, 1), ("S", 0, 1, 1, 0), ("A", 1, 0, 3, 0), ("A", 1, 1, 2, 1),
    ("S", 0, 0, 3, 1), ("A", 1, 1, 3, 1), ("A", 1, 0, 2, 0), ("A", 1, 0, 0, 1), ("A", 1, 1, 1, 0), ("S", 0, 0, 2, 1),
    ("A", 1, 1, 0, 1), ("A", 1, 1, 1, 1), ("S", 0, 1, 0, 0), ("S", 0, 1, 2, 0), ("S", 0, 0, 2, 0), ("A", 1, 0, 0, 0),
    ("S", 0, 1, 3, 0), ("A", 1, 0, 1, 0), ("S", 0, 0, 3, 0), ("S", 0, 1, 0, 1), ("A", 1, 0, 1, 1), ("S", 0, 0, 0, 0),
    ("S", 0, 1, 3, 1), ("S", 0, 1, 1, 1), ("S", 0, 0, 1, 1), ("S", 0, 0, 0, 1), ("S", 1, 1, 3, 0), ("S", 1, 1, 2, 0),
    ("S", 1, 0, 2, 1), ("S", 1, 0, 3, 1), ("B", 0, 1, -1, 1), ("B", 0, 1, 1, 1), ("S", 1, 1, 2, 1), ("S", 1, 1, 0, 0),
    ("S", 1, 0, 2, 0), ("B", 0, 1, -1, 0), ("S", 1, 0, 3, 0), ("S", 1, 1, 3, 1), ("S", 1, 1, 1, 0), ("B", 0, 0, 1, 1),
    ("B", 0, 0, -1, 1), ("S", 1, 0, 0, 1), ("S", 1, 0, 1, 0), ("B", 0, 1, 1, 0), ("S", 1, 1, 0, 1), ("S", 1, 1, 1, 1),
    ("B", 0, 0, 1, 0), ("B", 0, 0, -1, 0), ("S", 1, 0, 1, 1), ("S", 1, 0, 0, 0), ("B", 1, 0, 1, 1),
    ("B", 1, 0, -1, 1), ("B", 1, 1, 1, 0), ("B", 1, 0, 1, 0), ("B", 1, 1, -1, 0), ("B", 1, 0, -1, 0), ("Z", 0, 1, 1),
    ("B", 1, 1, 1, 1), ("B", 1, 1, -1, 1), ("Z", 0, 0, 1), ("Z", 0, 1, 0), ("Z", 0, 0, 0), ("Z", 1, 0, 1),
    ("Z", 1, 1, 0), ("Z", 1, 0, 0), ("X", 0, 1, 1), ("Z", 1, 1, 1), ("X", 0, 0, 1), ("X", 0, 1, 0), ("X", 0, 0, 0),
    ("X", 1, 0, 1), ("X", 1, 1, 0), ("X", 1, 0, 0), ("X", 1, 1, 1),
)


def kernel(
    sel_ref, gate_ref, tok_ref, wg_ref, wu_ref, wd_ref, slots_ref, comb_ref,
    tok_v, wg_v, wu_v, wd_v, send4, recv4, exit4, ret4, rows, part, hid, relay, fin_l, fin_r, summed,
    relay1, fin1_l, fin1_r, slots32, send_sem, recv_sem, load_sem,
):
    slot = sel_ref.shape[0]
    tok_dev, width = tok_ref.shape
    groups = 2 * RING
    n_slots = groups * slot
    halfw = width // 2
    quart = width // 4
    subw = halfw // SUB
    chunk = rows.shape[2]

    dp = lax.axis_index("dp")
    ex = lax.axis_index("expert")
    my_x, my_z = dp // RING, dp % RING
    my_y, my_c = ex // 2, ex % 2

    def at_x(step):
        return (((my_x + step + RING) % RING) * RING + my_z, ex)

    def at_z(step):
        return (my_x * RING + (my_z + step + RING) % RING, ex)

    def expert_at(g):
        return ((my_y + g // 2) % RING) * 2 + (my_c + g % 2) % 2

    def at_group(g):
        return (dp, expert_at(g))

    def back(g):
        return ((RING - g // 2) % RING) * 2 + g % 2

    barrier = pltpu.get_barrier_semaphore()
    partners = [at_x(1), at_x(-1), at_z(1), at_z(-1)] + [at_group(g) for g in range(1, groups)]
    for who in partners:
        pl.semaphore_signal(barrier, inc=1, device_id=who, device_id_type=MESH)

    loads = {}
    for i, (name, src, dst) in enumerate(
        (("tok", tok_ref, tok_v), ("wg", wg_ref, wg_v), ("wu", wu_ref, wu_v), ("wd", wd_ref, wd_v))
    ):
        loads[name] = pltpu.make_async_copy(src, dst, load_sem.at[i])
        loads[name].start()

    def loaded(*names):
        for name in names:
            if name in loads:
                loads.pop(name).wait()

    used = []
    copies = {}

    def remote(key, src, dst, who):
        i = len(used)
        copy = pltpu.make_async_remote_copy(
            src_ref=src, dst_ref=dst, send_sem=send_sem.at[i], recv_sem=recv_sem.at[i],
            device_id=who, device_id_type=MESH,
        )
        used.append(copy)
        copies[key] = copy
        copy.start()

    def need(*keys):
        for key in keys:
            if copies[key] is not None:
                copies[key].wait_recv()
                copies[key] = None

    row_id = lax.broadcasted_iota(jnp.int32, (n_slots, tok_dev), 0)
    lane_id = lax.broadcasted_iota(jnp.int32, (n_slots, tok_dev), 1)
    idx = jnp.full((n_slots, tok_dev), -1, jnp.int32)
    for g in range(groups):
        e = expert_at(g)
        for j in range(slot):
            idx = jnp.where(row_id == g * slot + j, sel_ref[j, e], idx)
    onehot = jnp.where(lane_id == idx, 1.0, 0.0).astype(BF16)
    loaded("tok")
    for c in range(0, width, 1024):
        cols = slice(c, c + 1024)
        slots32[:, cols] = jnp.dot(onehot, tok_v[:, cols], preferred_element_type=F32)
    recv4[0] = slots32[0:slot, :].astype(BF16)
    near = [back(g) for g in HALVES[0] if g > 0]
    far = [back(g) for g in HALVES[1]]
    for g in near + far:
        send4[g] = slots32[g * slot : (g + 1) * slot, :].astype(BF16)
    with jax.named_scope("barrier"):
        pl.semaphore_wait(barrier, len(partners))
    for g in near + far:
        remote(("in", back(g)), send4.at[g], recv4.at[back(g)], at_group(g))

    lane8 = lax.broadcasted_iota(jnp.int32, (8, 128), 1)
    idx_l = jnp.full((8, 128), -1, jnp.int32)
    gate_l = jnp.zeros((8, 128), F32)
    for g in range(groups):
        e = expert_at(g)
        for j in range(slot):
            here = lane8 % n_slots == g * slot + j
            idx_l = jnp.where(here, sel_ref[j, e], idx_l)
            gate_l = jnp.where(here, gate_ref[j, e], gate_l)
    g1 = gate_l.astype(BF16).astype(F32)
    rest = gate_l - g1
    g2 = rest.astype(BF16).astype(F32)
    g3 = (rest - g2).astype(BF16).astype(F32)
    term = lane8 // n_slots
    gate3 = jnp.where(term == 0, g1, jnp.where(term == 1, g2, jnp.where(term == 2, g3, 0.0)))
    tok_id = lax.broadcasted_iota(jnp.int32, (tok_dev, 128), 0)
    hit = tok_id == idx_l[0:1, :]
    comb_ref[...] = jnp.where(hit, gate3[0:1, :], 0.0).astype(BF16)

    def cut(p, lo=0, n=halfw):
        return pl.ds(p * halfw + lo, n)

    def pos(p, d1, d2):
        d1, d2 = d1 % RING, d2 % RING
        return d2 * RING + d1 if p == 0 else d1 * RING + d2

    def first(p, step):
        return at_x(step) if p == 0 else at_z(step)

    def second(p, step):
        return at_z(step) if p == 0 else at_x(step)

    def own(h):
        need(*[("in", g) for g in HALVES[h] if g > 0])
        for i, g in enumerate(HALVES[h]):
            slots32[i * slot : (i + 1) * slot, :] = recv4[g].astype(F32)
        rows[h, 0] = slots32[0:chunk, :].astype(BF16)

    def to_first(key, h, p, d1, step, lo, n):
        remote(
            key, rows.at[h, pos(p, d1, 0), :, cut(p, lo, n)],
            rows.at[h, pos(p, d1 - step, 0), :, cut(p, lo, n)], first(p, step),
        )

    def to_second(key, h, p, d1, d2, step):
        remote(
            key, rows.at[h, pos(p, d1, d2), :, cut(p)],
            rows.at[h, pos(p, d1, d2 - step), :, cut(p)], second(p, step),
        )

    def send_first(h, p, step):
        to_first(("f", h, p, step), h, p, 0, step, 0, halfw)

    def pass_first(h, p, step):
        need(("f", h, p, step))
        to_first(("r", h, p, step), h, p, -step, step, 0 if step == 1 else quart, quart)

    def send_second(h, p, d1, step):
        if d1 == 2:
            need(("r", h, p, 1), ("r", h, p, -1))
        elif d1 != 0:
            need(("f", h, p, 1 if d1 == 3 else -1))
        to_second(("s", h, p, d1, step), h, p, d1, 0, step)

    def pass_second(h, p, d1):
        step = 1 if d1 in RSET else -1
        need(("s", h, p, d1, step))
        to_second(("t", h, p, d1), h, p, d1, -step, step)

    tn = hid.shape[1] // 2

    def up(h, n):
        for p in range(2):
            for d1 in range(RING):
                need(("s", h, p, d1, 1), ("s", h, p, d1, -1), ("t", h, p, d1))
        loaded("wg", "wu")
        lhs = rows[h].reshape(RING * RING * chunk, width)
        cols = slice(n * tn, (n + 1) * tn)
        gate_val = jnp.dot(lhs, wg_v[:, cols], preferred_element_type=F32)
        up_val = jnp.dot(lhs, wu_v[:, cols], preferred_element_type=F32)
        hid[:, cols] = (gate_val / (1.0 + jnp.exp(-gate_val)) * up_val).astype(BF16)

    dn = 512

    def down(h, p, i):
        loaded("wd")
        start = p * halfw + i * subw
        for c in range(start, start + subw, dn):
            cols = slice(c, c + dn)
            val = jnp.dot(hid[...], wd_v[:, cols], preferred_element_type=F32)
            part[h, :, :, cols] = val.astype(BF16).reshape(RING * RING, chunk, dn)

    def sub(i, lo=0, n=subw):
        return pl.ds(i * subw + lo, n)

    def psub(p, i):
        return cut(p, i * subw, subw)

    def send_far(h, p, d1, i):
        step = 1 if d1 in RSET else -1
        remote(
            ("F", h, p, d1, i), part.at[h, pos(p, d1, 2), :, psub(p, i)],
            relay.at[h, p, d1, :, sub(i)], second(p, step),
        )

    def send_left_of(h, p, d1, i):
        remote(
            ("L", h, p, d1, i), part.at[h, pos(p, d1, 1), :, psub(p, i)],
            fin_l.at[h, p, d1, :, sub(i)], second(p, 1),
        )

    def send_right_of(h, p, d1, i):
        remote(
            ("R", h, p, d1, i), part.at[h, pos(p, d1, 3), :, psub(p, i)],
            fin_r.at[h, p, d1, :, sub(i)], second(p, -1),
        )

    def add_far(h, p, d1, i):
        need(("F", h, p, d1, i))
        right = d1 in RSET
        mine = part[h, pos(p, d1, 1 if right else 3), :, psub(p, i)]
        here = relay.at[h, p, d1, :, sub(i)]
        here[...] = (here[...].astype(F32) + mine.astype(F32)).astype(BF16)
        if right:
            remote(("L", h, p, d1, i), here, fin_l.at[h, p, d1, :, sub(i)], second(p, 1))
        else:
            remote(("R", h, p, d1, i), here, fin_r.at[h, p, d1, :, sub(i)], second(p, -1))

    def add_up(h, p, d1, i):
        need(("L", h, p, d1, i), ("R", h, p, d1, i))
        mine = part[h, pos(p, d1, 0), :, psub(p, i)]
        total = (
            mine.astype(F32)
            + fin_l[h, p, d1, :, sub(i)].astype(F32)
            + fin_r[h, p, d1, :, sub(i)].astype(F32)
        )
        summed[h, p, d1, :, sub(i)] = total.astype(BF16)
        lo, hi = sub(i, 0, subw // 2), sub(i, subw // 2, subw // 2)
        if d1 == 2:
            remote(("F1", h, p, 1, i), summed.at[h, p, 2, :, lo], relay1.at[h, p, :, lo], first(p, 1))
            remote(("F1", h, p, -1, i), summed.at[h, p, 2, :, hi], relay1.at[h, p, :, hi], first(p, -1))
        elif d1 == 1:
            remote(("l1", h, p, i), summed.at[h, p, 1, :, hi], fin1_l.at[h, p, :, hi], first(p, 1))
        elif d1 == 3:
            remote(("r1", h, p, i), summed.at[h, p, 3, :, lo], fin1_r.at[h, p, :, lo], first(p, -1))

    def add_first(h, p, step, i):
        need(("F1", h, p, step, i))
        d1 = 1 if step == 1 else 3
        cols = sub(i, 0 if step == 1 else subw // 2, subw // 2)
        here = relay1.at[h, p, :, cols]
        here[...] = (here[...].astype(F32) + summed[h, p, d1, :, cols].astype(F32)).astype(BF16)
        dst = fin1_l if step == 1 else fin1_r
        remote(("b", h, p, step, i), here, dst.at[h, p, :, cols], first(p, step))

    def finish(h, p, i):
        need(("l1", h, p, i), ("r1", h, p, i), ("b", h, p, 1, i), ("b", h, p, -1, i))
        slots32[0:chunk, psub(p, i)] = (
            summed[h, p, 0, :, sub(i)].astype(F32)
            + fin1_l[h, p, :, sub(i)].astype(F32)
            + fin1_r[h, p, :, sub(i)].astype(F32)
        )
        for r, g in enumerate(HALVES[h]):
            value = slots32[r * slot : (r + 1) * slot, psub(p, i)].astype(BF16)
            if g == 0:
                ret4[0, :, psub(p, i)] = value
            else:
                exit4[g, :, psub(p, i)] = value
                remote(
                    ("X", h, p, i, back(g)), exit4.at[g, :, psub(p, i)],
                    ret4.at[back(g), :, psub(p, i)], at_group(g),
                )

    def take(h, p, i):
        for g in HALVES[h]:
            if g > 0:
                need(("X", h, p, i, g))
            slots_ref[g * slot : (g + 1) * slot, psub(p, i)] = ret4[g, :, psub(p, i)].astype(F32)

    steps = {
        "own": own, "f": send_first, "r": pass_first, "s": send_second, "t": pass_second,
        "up": up, "down": down, "F": send_far, "L": send_left_of, "R": send_right_of,
        "A": add_far, "S": add_up, "B": add_first, "Z": finish, "X": take,
    }
    last = max(i for i, entry in enumerate(ORDER) if entry[0] == "Z")
    for at, (name, *args) in enumerate(ORDER):
        with jax.named_scope("_".join(str(a) for a in (name, *args))):
            steps[name](*args)
        if at == last:
            drained = len(used)
            for copy in used[: drained - 24]:
                copy.wait_send()
    for copy in used[drained - 24 :]:
        copy.wait_send()


def combine_kernel(slots_ref, comb_ref, out_ref, out_v, out_sem):
    width = slots_ref.shape[1]
    n = 1024
    stores = []
    for k, c in enumerate(range(0, width, n)):
        value = slots_ref[:, c : c + n].astype(BF16)
        stack = jnp.concatenate([value, value, value, jnp.zeros_like(value)], axis=0)
        out_v[:, c : c + n] = jnp.dot(
            comb_ref[...], stack, preferred_element_type=F32).astype(BF16)
        store = pltpu.make_async_copy(
            out_v.at[:, pl.ds(c, n)], out_ref.at[:, pl.ds(c, n)], out_sem.at[k])
        store.start()
        stores.append(store)
    for store in stores:
        store.wait()


def per_device(tokens, select, gates, w_gate, w_up, w_down):
    tok_dev, width = tokens.shape
    slot = select.shape[1]
    ff = w_gate.shape[2]
    chunk = RING * slot
    halfw = width // 2
    vmem, hbm = pl.BlockSpec(memory_space=pltpu.VMEM), pl.BlockSpec(memory_space=pltpu.HBM)
    smem = pl.BlockSpec(memory_space=pltpu.SMEM)
    slots, comb = pl.pallas_call(
        kernel,
        out_shape=(pltpu.VMEM((8 * slot, width), F32), pltpu.VMEM((tok_dev, 128), BF16)),
        in_specs=[smem, smem, hbm, hbm, hbm, hbm],
        out_specs=(vmem, vmem),
        scratch_shapes=[
            pltpu.VMEM((tok_dev, width), BF16),
            pltpu.VMEM((width, ff), BF16),
            pltpu.VMEM((width, ff), BF16),
            pltpu.VMEM((ff, width), BF16),
            pltpu.VMEM((8, slot, width), BF16),
            pltpu.VMEM((8, slot, width), BF16),
            pltpu.VMEM((8, slot, width), BF16),
            pltpu.VMEM((8, slot, width), BF16),
            pltpu.VMEM((2, 16, chunk, width), BF16),
            pltpu.VMEM((2, 16, chunk, width), BF16),
            pltpu.VMEM((16 * chunk, ff), BF16),
            pltpu.VMEM((2, 2, 4, chunk, halfw), BF16),
            pltpu.VMEM((2, 2, 4, chunk, halfw), BF16),
            pltpu.VMEM((2, 2, 4, chunk, halfw), BF16),
            pltpu.VMEM((2, 2, 4, chunk, halfw), BF16),
            pltpu.VMEM((2, 2, chunk, halfw), BF16),
            pltpu.VMEM((2, 2, chunk, halfw), BF16),
            pltpu.VMEM((2, 2, chunk, halfw), BF16),
            pltpu.VMEM((8 * slot, width), F32),
            pltpu.SemaphoreType.DMA((N_SEM,)),
            pltpu.SemaphoreType.DMA((N_SEM,)),
            pltpu.SemaphoreType.DMA((4,)),
        ],
        compiler_params=pltpu.CompilerParams(
            collective_id=0, has_side_effects=True, vmem_limit_bytes=56 * 1024 * 1024
        ),
        name="moe",
    )(
        select.T, gates.T, tokens, w_gate[0], w_up[0], w_down[0],
    )
    return pl.pallas_call(
        combine_kernel,
        out_shape=jax.ShapeDtypeStruct((tok_dev, width), BF16),
        in_specs=[vmem, vmem],
        out_specs=hbm,
        scratch_shapes=[pltpu.VMEM((tok_dev, width), BF16), pltpu.SemaphoreType.DMA((4,))],
        compiler_params=pltpu.CompilerParams(vmem_limit_bytes=8 * 1024 * 1024),
        name="combine",
    )(slots, comb)


def solution(mesh):
    return jax.shard_map(
        per_device,
        mesh=mesh,
        in_specs=(
            P(("dp", "expert"), None),
            P(None, ("dp", "expert")),
            P(None, ("dp", "expert")),
            P("expert", None, "dp"),
            P("expert", None, "dp"),
            P("expert", "dp", None),
        ),
        out_specs=P(("dp", "expert"), None),
        check_vma=False,
    )
```

```python
import jax
import jax.numpy as jnp
from jax import lax
from jax.experimental import pallas as pl
from jax.experimental.pallas import tpu as pltpu
from jax.sharding import PartitionSpec as P

MESH = pl.DeviceIdType.MESH
BF16, F32 = jnp.bfloat16, jnp.float32
RING = 4
SUB = 2
N_RECV = 128
RSET, LSET = (0, 3), (2, 1)
HALVES = ((0, 1, 2, 6), (3, 7, 4, 5))

ORDER = (
    ("own", 0), ("f", 0, 0, -1), ("f", 0, 1, -1), ("f", 0, 0, 1), ("f", 0, 1, 1), ("s", 0, 1, 0, 1),
    ("s", 0, 1, 0, -1), ("s", 0, 0, 0, -1), ("s", 0, 0, 0, 1), ("own", 1), ("s", 1, 1, 0, 1), ("f", 1, 1, -1),
    ("f", 1, 0, 1), ("s", 1, 0, 0, 1), ("f", 1, 0, -1), ("s", 1, 1, 0, -1), ("f", 1, 1, 1), ("s", 1, 0, 0, -1),
    ("r", 0, 0, -1), ("s", 0, 1, 1, -1), ("r", 0, 1, -1), ("r", 0, 0, 1), ("r", 0, 1, 1), ("s", 0, 1, 3, 1),
    ("s", 0, 1, 3, -1), ("s", 0, 0, 1, 1), ("s", 0, 1, 1, 1), ("s", 0, 0, 3, -1), ("s", 0, 0, 3, 1),
    ("s", 0, 0, 1, -1), ("t", 0, 1, 0), ("t", 0, 0, 0), ("r", 1, 0, -1), ("r", 1, 1, -1), ("s", 1, 1, 1, -1),
    ("t", 1, 1, 0), ("s", 1, 1, 1, 1), ("t", 1, 0, 0), ("s", 1, 0, 1, -1), ("s", 1, 0, 1, 1), ("s", 1, 0, 3, 1),
    ("s", 1, 1, 3, 1), ("r", 1, 1, 1), ("s", 1, 0, 3, -1), ("r", 1, 0, 1), ("s", 1, 1, 3, -1), ("s", 0, 0, 2, -1),
    ("s", 0, 0, 2, 1), ("s", 0, 1, 2, 1), ("s", 0, 1, 2, -1), ("t", 0, 1, 1), ("t", 0, 1, 3), ("t", 0, 0, 1),
    ("t", 0, 0, 3), ("t", 1, 1, 1), ("t", 1, 0, 1), ("t", 0, 1, 2), ("t", 0, 0, 2), ("t", 1, 1, 3), ("t", 1, 0, 3),
    ("s", 1, 0, 2, 1), ("s", 1, 1, 2, -1), ("s", 1, 0, 2, -1), ("s", 1, 1, 2, 1), ("up", 0, 0), ("up", 0, 1),
    ("t", 1, 1, 2), ("t", 1, 0, 2), ("down", 0, 0, 1), ("L", 0, 0, 2, 1), ("F", 0, 0, 0, 1), ("F", 0, 0, 3, 1),
    ("down", 0, 0, 0), ("F", 0, 0, 1, 0), ("F", 0, 0, 2, 0), ("R", 0, 0, 3, 1), ("L", 0, 0, 1, 1), ("R", 0, 0, 3, 0),
    ("F", 0, 0, 3, 0), ("R", 0, 0, 0, 1), ("down", 0, 1, 0), ("F", 0, 1, 2, 0), ("L", 0, 1, 1, 0), ("L", 0, 1, 2, 0),
    ("F", 0, 1, 1, 0), ("F", 0, 1, 3, 0), ("R", 0, 1, 0, 0), ("F", 0, 0, 2, 1), ("F", 0, 0, 1, 1), ("F", 0, 1, 0, 0),
    ("R", 0, 1, 3, 0), ("down", 0, 1, 1), ("F", 0, 1, 2, 1), ("R", 0, 1, 3, 1), ("L", 0, 1, 2, 1), ("L", 0, 1, 1, 1),
    ("F", 0, 1, 1, 1), ("F", 0, 1, 0, 1), ("L", 0, 0, 1, 0), ("R", 0, 1, 0, 1), ("L", 0, 0, 2, 0), ("F", 0, 0, 0, 0),
    ("F", 0, 1, 3, 1), ("R", 0, 0, 0, 0), ("up", 1, 0), ("A", 0, 0, 1, 0), ("up", 1, 1), ("down", 1, 1, 0),
    ("R", 1, 1, 3, 0), ("F", 1, 1, 3, 0), ("F", 1, 1, 0, 0), ("F", 1, 1, 2, 0), ("down", 1, 0, 1), ("F", 1, 0, 2, 1),
    ("R", 1, 0, 0, 1), ("F", 1, 0, 3, 1), ("L", 1, 0, 2, 1), ("down", 1, 0, 0), ("L", 1, 0, 2, 0), ("F", 1, 0, 3, 0),
    ("R", 1, 0, 3, 0), ("A", 0, 1, 2, 1), ("R", 1, 0, 0, 0), ("A", 0, 1, 1, 0), ("F", 1, 0, 2, 0), ("L", 1, 1, 2, 0),
    ("L", 1, 1, 1, 0), ("down", 1, 1, 1), ("A", 0, 0, 2, 1), ("L", 1, 1, 2, 1), ("F", 1, 1, 2, 1), ("F", 1, 1, 3, 1),
    ("L", 1, 1, 1, 1), ("A", 0, 0, 3, 1), ("R", 1, 1, 3, 1), ("F", 1, 1, 1, 0), ("R", 1, 0, 3, 1), ("F", 1, 0, 0, 1),
    ("A", 0, 0, 2, 0), ("L", 1, 0, 1, 0), ("F", 1, 0, 1, 0), ("F", 1, 1, 1, 1), ("A", 0, 1, 2, 0), ("L", 1, 0, 1, 1),
    ("F", 1, 1, 0, 1), ("F", 1, 0, 0, 0), ("F", 1, 0, 1, 1), ("R", 1, 1, 0, 1), ("R", 1, 1, 0, 0), ("A", 0, 1, 0, 0),
    ("A", 0, 0, 3, 0), ("A", 0, 0, 0, 0), ("A", 0, 0, 0, 1), ("A", 0, 1, 3, 0), ("A", 0, 1, 0, 1), ("A", 0, 1, 1, 1),
    ("A", 0, 0, 1, 1), ("A", 0, 1, 3, 1), ("A", 1, 1, 3, 0), ("S", 0, 0, 1, 0), ("A", 1, 0, 3, 1), ("A", 1, 1, 0, 0),
    ("A", 1, 1, 2, 0), ("A", 1, 0, 2, 1), ("S", 0, 1, 2, 1), ("S", 0, 1, 1, 0), ("A", 1, 0, 3, 0), ("A", 1, 1, 2, 1),
    ("S", 0, 0, 3, 1), ("A", 1, 1, 3, 1), ("A", 1, 0, 2, 0), ("A", 1, 0, 0, 1), ("A", 1, 1, 1, 0), ("S", 0, 0, 2, 1),
    ("A", 1, 1, 0, 1), ("A", 1, 1, 1, 1), ("S", 0, 1, 0, 0), ("S", 0, 1, 2, 0), ("S", 0, 0, 2, 0), ("A", 1, 0, 0, 0),
    ("S", 0, 1, 3, 0), ("A", 1, 0, 1, 0), ("S", 0, 0, 3, 0), ("S", 0, 1, 0, 1), ("A", 1, 0, 1, 1), ("S", 0, 0, 0, 0),
    ("S", 0, 1, 3, 1), ("S", 0, 1, 1, 1), ("S", 0, 0, 1, 1), ("S", 0, 0, 0, 1), ("S", 1, 1, 3, 0), ("S", 1, 1, 2, 0),
    ("S", 1, 0, 2, 1), ("S", 1, 0, 3, 1), ("B", 0, 1, -1, 1), ("B", 0, 1, 1, 1), ("S", 1, 1, 2, 1), ("S", 1, 1, 0, 0),
    ("S", 1, 0, 2, 0), ("B", 0, 1, -1, 0), ("S", 1, 0, 3, 0), ("S", 1, 1, 3, 1), ("S", 1, 1, 1, 0), ("B", 0, 0, 1, 1),
    ("B", 0, 0, -1, 1), ("S", 1, 0, 0, 1), ("S", 1, 0, 1, 0), ("B", 0, 1, 1, 0), ("S", 1, 1, 0, 1), ("S", 1, 1, 1, 1),
    ("B", 0, 0, 1, 0), ("B", 0, 0, -1, 0), ("S", 1, 0, 1, 1), ("S", 1, 0, 0, 0), ("B", 1, 0, 1, 1),
    ("B", 1, 0, -1, 1), ("B", 1, 1, 1, 0), ("B", 1, 0, 1, 0), ("B", 1, 1, -1, 0), ("B", 1, 0, -1, 0), ("Z", 0, 1, 1),
    ("B", 1, 1, 1, 1), ("B", 1, 1, -1, 1), ("Z", 0, 0, 1), ("Z", 0, 1, 0), ("Z", 0, 0, 0), ("Z", 1, 0, 1),
    ("Z", 1, 1, 0), ("Z", 1, 0, 0), ("X", 0, 1, 1), ("Z", 1, 1, 1), ("X", 0, 0, 1), ("X", 0, 1, 0), ("X", 0, 0, 0),
    ("X", 1, 0, 1), ("X", 1, 1, 0), ("X", 1, 0, 0), ("X", 1, 1, 1),
)


def kernel(
    sel_ref, gate_ref, tok_ref, wg_ref, wu_ref, wd_ref, slots_ref, comb_ref,
    tok_v, wg_v, wu_v, wd_v, send4, recv4, exit4, ret4, rows, part, hid, relay, fin_l, fin_r, summed,
    relay1, fin1_l, fin1_r, slots32, send_sem, recv_sem, load_sem,
):
    slot = sel_ref.shape[0]
    tok_dev, width = tok_ref.shape
    groups = 2 * RING
    n_slots = groups * slot
    halfw = width // 2
    quart = width // 4
    subw = halfw // SUB
    chunk = rows.shape[2]

    dp = lax.axis_index("dp")
    ex = lax.axis_index("expert")
    my_x, my_z = dp // RING, dp % RING
    my_y, my_c = ex // 2, ex % 2

    def at_x(step):
        return (((my_x + step + RING) % RING) * RING + my_z, ex)

    def at_z(step):
        return (my_x * RING + (my_z + step + RING) % RING, ex)

    def expert_at(g):
        return ((my_y + g // 2) % RING) * 2 + (my_c + g % 2) % 2

    def at_group(g):
        return (dp, expert_at(g))

    def back(g):
        return ((RING - g // 2) % RING) * 2 + g % 2

    barrier = pltpu.get_barrier_semaphore()
    partners = [at_x(1), at_x(-1), at_z(1), at_z(-1)] + [at_group(g) for g in range(1, groups)]
    for who in partners:
        pl.semaphore_signal(barrier, inc=1, device_id=who, device_id_type=MESH)

    loads = {}
    for i, (name, src, dst) in enumerate(
        (("tok", tok_ref, tok_v), ("wg", wg_ref, wg_v), ("wu", wu_ref, wu_v), ("wd", wd_ref, wd_v))
    ):
        loads[name] = pltpu.make_async_copy(src, dst, load_sem.at[i])
        loads[name].start()

    def loaded(*names):
        for name in names:
            if name in loads:
                loads.pop(name).wait()

    recv_of, recv_bytes, send_bytes = {}, {}, {}

    def together(key):
        kind, h = key[0], key[1]
        if kind == "in":
            return ("own", 0 if h in HALVES[0] else 1)
        if kind == "r":
            return key[:3]
        if kind == "t" or (kind == "s" and key[4] != (1 if key[3] in RSET else -1)):
            return ("up", h)
        if kind in ("L", "R"):
            return ("S", *key[1:])
        if kind in ("l1", "r1"):
            return ("Z", *key[1:])
        if kind == "b":
            return ("Z", h, key[2], key[4])
        return key[:4] if kind == "X" else key

    def outbox(key):
        kind, h = key[0], key[1]
        if kind == "in":
            return 0
        return (1 if kind in "fsrt" else 3 if kind != "X" else 5) + h

    def size(ref):
        n = 2
        for dim in ref.shape:
            n *= dim
        return n

    def wait_for(sem, n):
        row = 2 * chunk * width
        if n % row == 0:
            ref = rows.at[0, pl.ds(0, n // row)]
        elif n % (row // 4) == 0:
            ref = exit4.at[pl.ds(0, 4 * n // row)]
        else:
            ref = exit4.at[pl.ds(0, 16 * n // row), :, pl.ds(0, width // 4)]
        assert size(ref) == n
        pltpu.make_async_copy(ref, ref, sem).wait()

    def remote(key, src, dst, who):
        name, box = together(key), outbox(key)
        i = recv_of.setdefault(name, len(recv_of))
        recv_bytes[name] = recv_bytes.get(name, 0) + size(dst)
        send_bytes[box] = send_bytes.get(box, 0) + size(src)
        pltpu.make_async_remote_copy(
            src_ref=src, dst_ref=dst, send_sem=send_sem.at[box], recv_sem=recv_sem.at[i],
            device_id=who, device_id_type=MESH,
        ).start()

    def need(*names):
        for name in names:
            if name in recv_bytes:
                wait_for(recv_sem.at[recv_of[name]], recv_bytes.pop(name))

    def drain(*boxes):
        for box in boxes:
            wait_for(send_sem.at[box], send_bytes.pop(box))

    row_id = lax.broadcasted_iota(jnp.int32, (n_slots, tok_dev), 0)
    lane_id = lax.broadcasted_iota(jnp.int32, (n_slots, tok_dev), 1)
    idx = jnp.full((n_slots, tok_dev), -1, jnp.int32)
    for g in range(groups):
        e = expert_at(g)
        for j in range(slot):
            idx = jnp.where(row_id == g * slot + j, sel_ref[j, e], idx)
    onehot = jnp.where(lane_id == idx, 1.0, 0.0).astype(BF16)
    loaded("tok")
    for c in range(0, width, 1024):
        cols = slice(c, c + 1024)
        slots32[:, cols] = jnp.dot(onehot, tok_v[:, cols], preferred_element_type=F32)
    recv4[0] = slots32[0:slot, :].astype(BF16)
    near = [back(g) for g in HALVES[0] if g > 0]
    far = [back(g) for g in HALVES[1]]
    for g in near + far:
        send4[g] = slots32[g * slot : (g + 1) * slot, :].astype(BF16)
    with jax.named_scope("barrier"):
        pl.semaphore_wait(barrier, len(partners))
    for g in near + far:
        remote(("in", back(g)), send4.at[g], recv4.at[back(g)], at_group(g))

    lane8 = lax.broadcasted_iota(jnp.int32, (8, 128), 1)
    idx_l = jnp.full((8, 128), -1, jnp.int32)
    gate_l = jnp.zeros((8, 128), F32)
    for g in range(groups):
        e = expert_at(g)
        for j in range(slot):
            here = lane8 % n_slots == g * slot + j
            idx_l = jnp.where(here, sel_ref[j, e], idx_l)
            gate_l = jnp.where(here, gate_ref[j, e], gate_l)
    g1 = gate_l.astype(BF16).astype(F32)
    rest = gate_l - g1
    g2 = rest.astype(BF16).astype(F32)
    g3 = (rest - g2).astype(BF16).astype(F32)
    term = lane8 // n_slots
    gate3 = jnp.where(term == 0, g1, jnp.where(term == 1, g2, jnp.where(term == 2, g3, 0.0)))
    tok_id = lax.broadcasted_iota(jnp.int32, (tok_dev, 128), 0)
    hit = tok_id == idx_l[0:1, :]
    comb_ref[...] = jnp.where(hit, gate3[0:1, :], 0.0).astype(BF16)

    def cut(p, lo=0, n=halfw):
        return pl.ds(p * halfw + lo, n)

    def pos(p, d1, d2):
        d1, d2 = d1 % RING, d2 % RING
        return d2 * RING + d1 if p == 0 else d1 * RING + d2

    def first(p, step):
        return at_x(step) if p == 0 else at_z(step)

    def second(p, step):
        return at_z(step) if p == 0 else at_x(step)

    def own(h):
        need(("own", h))
        for i, g in enumerate(HALVES[h]):
            slots32[i * slot : (i + 1) * slot, :] = recv4[g].astype(F32)
        rows[h, 0] = slots32[0:chunk, :].astype(BF16)

    def to_first(key, h, p, d1, step, lo, n):
        remote(
            key, rows.at[h, pos(p, d1, 0), :, cut(p, lo, n)],
            rows.at[h, pos(p, d1 - step, 0), :, cut(p, lo, n)], first(p, step),
        )

    def to_second(key, h, p, d1, d2, step):
        remote(
            key, rows.at[h, pos(p, d1, d2), :, cut(p)],
            rows.at[h, pos(p, d1, d2 - step), :, cut(p)], second(p, step),
        )

    def send_first(h, p, step):
        to_first(("f", h, p, step), h, p, 0, step, 0, halfw)

    def pass_first(h, p, step):
        need(("f", h, p, step))
        to_first(("r", h, p, step), h, p, -step, step, 0 if step == 1 else quart, quart)

    def send_second(h, p, d1, step):
        if d1 == 2:
            need(("r", h, p))
        elif d1 != 0:
            need(("f", h, p, 1 if d1 == 3 else -1))
        to_second(("s", h, p, d1, step), h, p, d1, 0, step)

    def pass_second(h, p, d1):
        step = 1 if d1 in RSET else -1
        need(("s", h, p, d1, step))
        to_second(("t", h, p, d1), h, p, d1, -step, step)

    tn = hid.shape[1] // 2

    def up(h, n):
        need(("up", h))
        loaded("wg", "wu")
        lhs = rows[h].reshape(RING * RING * chunk, width)
        cols = slice(n * tn, (n + 1) * tn)
        gate_val = jnp.dot(lhs, wg_v[:, cols], preferred_element_type=F32)
        up_val = jnp.dot(lhs, wu_v[:, cols], preferred_element_type=F32)
        hid[:, cols] = (gate_val / (1.0 + jnp.exp(-gate_val)) * up_val).astype(BF16)

    dn = 512

    def down(h, p, i):
        loaded("wd")
        start = p * halfw + i * subw
        for c in range(start, start + subw, dn):
            cols = slice(c, c + dn)
            val = jnp.dot(hid[...], wd_v[:, cols], preferred_element_type=F32)
            part[h, :, :, cols] = val.astype(BF16).reshape(RING * RING, chunk, dn)

    def sub(i, lo=0, n=subw):
        return pl.ds(i * subw + lo, n)

    def psub(p, i):
        return cut(p, i * subw, subw)

    def send_far(h, p, d1, i):
        step = 1 if d1 in RSET else -1
        remote(
            ("F", h, p, d1, i), part.at[h, pos(p, d1, 2), :, psub(p, i)],
            relay.at[h, p, d1, :, sub(i)], second(p, step),
        )

    def send_left_of(h, p, d1, i):
        remote(
            ("L", h, p, d1, i), part.at[h, pos(p, d1, 1), :, psub(p, i)],
            fin_l.at[h, p, d1, :, sub(i)], second(p, 1),
        )

    def send_right_of(h, p, d1, i):
        remote(
            ("R", h, p, d1, i), part.at[h, pos(p, d1, 3), :, psub(p, i)],
            fin_r.at[h, p, d1, :, sub(i)], second(p, -1),
        )

    def add_far(h, p, d1, i):
        need(("F", h, p, d1, i))
        right = d1 in RSET
        mine = part[h, pos(p, d1, 1 if right else 3), :, psub(p, i)]
        here = relay.at[h, p, d1, :, sub(i)]
        here[...] = (here[...].astype(F32) + mine.astype(F32)).astype(BF16)
        if right:
            remote(("L", h, p, d1, i), here, fin_l.at[h, p, d1, :, sub(i)], second(p, 1))
        else:
            remote(("R", h, p, d1, i), here, fin_r.at[h, p, d1, :, sub(i)], second(p, -1))

    def add_up(h, p, d1, i):
        need(("S", h, p, d1, i))
        mine = part[h, pos(p, d1, 0), :, psub(p, i)]
        total = (
            mine.astype(F32)
            + fin_l[h, p, d1, :, sub(i)].astype(F32)
            + fin_r[h, p, d1, :, sub(i)].astype(F32)
        )
        summed[h, p, d1, :, sub(i)] = total.astype(BF16)
        lo, hi = sub(i, 0, subw // 2), sub(i, subw // 2, subw // 2)
        if d1 == 2:
            remote(("F1", h, p, 1, i), summed.at[h, p, 2, :, lo], relay1.at[h, p, :, lo], first(p, 1))
            remote(("F1", h, p, -1, i), summed.at[h, p, 2, :, hi], relay1.at[h, p, :, hi], first(p, -1))
        elif d1 == 1:
            remote(("l1", h, p, i), summed.at[h, p, 1, :, hi], fin1_l.at[h, p, :, hi], first(p, 1))
        elif d1 == 3:
            remote(("r1", h, p, i), summed.at[h, p, 3, :, lo], fin1_r.at[h, p, :, lo], first(p, -1))

    def add_first(h, p, step, i):
        need(("F1", h, p, step, i))
        d1 = 1 if step == 1 else 3
        cols = sub(i, 0 if step == 1 else subw // 2, subw // 2)
        here = relay1.at[h, p, :, cols]
        here[...] = (here[...].astype(F32) + summed[h, p, d1, :, cols].astype(F32)).astype(BF16)
        dst = fin1_l if step == 1 else fin1_r
        remote(("b", h, p, step, i), here, dst.at[h, p, :, cols], first(p, step))

    def finish(h, p, i):
        need(("Z", h, p, i))
        slots32[0:chunk, psub(p, i)] = (
            summed[h, p, 0, :, sub(i)].astype(F32)
            + fin1_l[h, p, :, sub(i)].astype(F32)
            + fin1_r[h, p, :, sub(i)].astype(F32)
        )
        for r, g in enumerate(HALVES[h]):
            value = slots32[r * slot : (r + 1) * slot, psub(p, i)].astype(BF16)
            if g == 0:
                ret4[0, :, psub(p, i)] = value
            else:
                exit4[g, :, psub(p, i)] = value
                remote(
                    ("X", h, p, i, back(g)), exit4.at[g, :, psub(p, i)],
                    ret4.at[back(g), :, psub(p, i)], at_group(g),
                )

    def take(h, p, i):
        need(("X", h, p, i))
        for g in HALVES[h]:
            slots_ref[g * slot : (g + 1) * slot, psub(p, i)] = ret4[g, :, psub(p, i)].astype(F32)

    steps = {
        "own": own, "f": send_first, "r": pass_first, "s": send_second, "t": pass_second,
        "up": up, "down": down, "F": send_far, "L": send_left_of, "R": send_right_of,
        "A": add_far, "S": add_up, "B": add_first, "Z": finish, "X": take,
    }
    ends = [i for i, entry in enumerate(ORDER) if entry[0] == "Z"]
    for at, (name, *args) in enumerate(ORDER):
        with jax.named_scope("_".join(str(a) for a in (name, *args))):
            steps[name](*args)
        if at == ends[-1]:
            with jax.named_scope("drain"):
                drain(0, 1, 2, 3, 4, 5)
    with jax.named_scope("last_sends"):
        drain(6)


def combine_kernel(slots_ref, comb_ref, out_ref, out_v, out_sem):
    width = slots_ref.shape[1]
    n = 1024
    stores = []
    for k, c in enumerate(range(0, width, n)):
        value = slots_ref[:, c : c + n].astype(BF16)
        stack = jnp.concatenate([value, value, value, jnp.zeros_like(value)], axis=0)
        out_v[:, c : c + n] = jnp.dot(
            comb_ref[...], stack, preferred_element_type=F32).astype(BF16)
        store = pltpu.make_async_copy(
            out_v.at[:, pl.ds(c, n)], out_ref.at[:, pl.ds(c, n)], out_sem.at[k])
        store.start()
        stores.append(store)
    for store in stores:
        store.wait()


def per_device(tokens, select, gates, w_gate, w_up, w_down):
    tok_dev, width = tokens.shape
    slot = select.shape[1]
    ff = w_gate.shape[2]
    chunk = RING * slot
    halfw = width // 2
    vmem, hbm = pl.BlockSpec(memory_space=pltpu.VMEM), pl.BlockSpec(memory_space=pltpu.HBM)
    smem = pl.BlockSpec(memory_space=pltpu.SMEM)
    slots, comb = pl.pallas_call(
        kernel,
        out_shape=(pltpu.VMEM((8 * slot, width), F32), pltpu.VMEM((tok_dev, 128), BF16)),
        in_specs=[smem, smem, hbm, hbm, hbm, hbm],
        out_specs=(vmem, vmem),
        scratch_shapes=[
            pltpu.VMEM((tok_dev, width), BF16),
            pltpu.VMEM((width, ff), BF16),
            pltpu.VMEM((width, ff), BF16),
            pltpu.VMEM((ff, width), BF16),
            pltpu.VMEM((8, slot, width), BF16),
            pltpu.VMEM((8, slot, width), BF16),
            pltpu.VMEM((8, slot, width), BF16),
            pltpu.VMEM((8, slot, width), BF16),
            pltpu.VMEM((2, 16, chunk, width), BF16),
            pltpu.VMEM((2, 16, chunk, width), BF16),
            pltpu.VMEM((16 * chunk, ff), BF16),
            pltpu.VMEM((2, 2, 4, chunk, halfw), BF16),
            pltpu.VMEM((2, 2, 4, chunk, halfw), BF16),
            pltpu.VMEM((2, 2, 4, chunk, halfw), BF16),
            pltpu.VMEM((2, 2, 4, chunk, halfw), BF16),
            pltpu.VMEM((2, 2, chunk, halfw), BF16),
            pltpu.VMEM((2, 2, chunk, halfw), BF16),
            pltpu.VMEM((2, 2, chunk, halfw), BF16),
            pltpu.VMEM((8 * slot, width), F32),
            pltpu.SemaphoreType.DMA((7,)),
            pltpu.SemaphoreType.DMA((N_RECV,)),
            pltpu.SemaphoreType.DMA((4,)),
        ],
        compiler_params=pltpu.CompilerParams(
            collective_id=0, has_side_effects=True, vmem_limit_bytes=56 * 1024 * 1024
        ),
        name="moe",
    )(
        select.T, gates.T, tokens, w_gate[0], w_up[0], w_down[0],
    )
    return pl.pallas_call(
        combine_kernel,
        out_shape=jax.ShapeDtypeStruct((tok_dev, width), BF16),
        in_specs=[vmem, vmem],
        out_specs=hbm,
        scratch_shapes=[pltpu.VMEM((tok_dev, width), BF16), pltpu.SemaphoreType.DMA((4,))],
        compiler_params=pltpu.CompilerParams(vmem_limit_bytes=8 * 1024 * 1024),
        name="combine",
    )(slots, comb)


def solution(mesh):
    return jax.shard_map(
        per_device,
        mesh=mesh,
        in_specs=(
            P(("dp", "expert"), None),
            P(None, ("dp", "expert")),
            P(None, ("dp", "expert")),
            P("expert", None, "dp"),
            P("expert", None, "dp"),
            P("expert", "dp", None),
        ),
        out_specs=P(("dp", "expert"), None),
        check_vma=False,
    )
```

```python
import jax
import jax.numpy as jnp
from jax import lax
from jax.experimental import pallas as pl
from jax.experimental.pallas import tpu as pltpu
from jax.sharding import PartitionSpec as P

MESH = pl.DeviceIdType.MESH
BF16, F32 = jnp.bfloat16, jnp.float32
RING = 4
SUB = 2
N_RECV = 130
RSET, LSET = (0, 3), (2, 1)
EARLY = tuple((z, x) for z in (0, 1, 3) for x in (0, 1, 3))
LATE = tuple((z, x) for z in range(RING) for x in range(RING) if 2 in (z, x))
PLACE = {at: i for i, at in enumerate(EARLY + LATE)}
HALVES = ((0, 1, 2, 6), (3, 7, 4, 5))

ORDER = (
    ("own", 0), ("s", 0, 1, 0, -1), ("s", 0, 0, 0, -1), ("f", 0, 0, -1), ("s", 0, 0, 0, 1), ("f", 0, 0, 1),
    ("f", 0, 1, -1), ("s", 0, 1, 0, 1), ("f", 0, 1, 1), ("own", 1), ("f", 1, 1, -1), ("s", 1, 0, 0, 1),
    ("s", 1, 1, 0, -1), ("f", 1, 1, 1), ("s", 1, 0, 0, -1), ("f", 1, 0, -1), ("s", 1, 1, 0, 1), ("f", 1, 0, 1),
    ("t", 0, 0, 0), ("s", 0, 0, 3, -1), ("r", 0, 0, 1), ("s", 0, 0, 3, 1), ("s", 0, 0, 1, 1), ("s", 0, 0, 1, -1),
    ("s", 0, 1, 1, -1), ("r", 0, 0, -1), ("s", 0, 1, 3, 1), ("s", 0, 1, 3, -1), ("s", 0, 1, 1, 1), ("r", 0, 1, -1),
    ("t", 0, 1, 0), ("r", 0, 1, 1), ("r", 1, 1, -1), ("s", 1, 1, 1, -1), ("s", 1, 1, 1, 1), ("t", 1, 0, 0),
    ("t", 1, 1, 0), ("s", 1, 0, 1, -1), ("s", 1, 0, 1, 1), ("r", 1, 0, -1), ("s", 1, 1, 3, -1), ("s", 1, 0, 3, 1),
    ("s", 1, 0, 3, -1), ("r", 1, 0, 1), ("r", 1, 1, 1), ("s", 1, 1, 3, 1), ("t", 0, 1, 1), ("s", 0, 0, 2, 1),
    ("s", 0, 0, 2, -1), ("t", 0, 1, 3), ("t", 0, 0, 1), ("t", 0, 0, 3), ("up", 0, 0, 0), ("s", 0, 1, 2, -1),
    ("up", 0, 0, 1), ("t", 1, 0, 1), ("s", 0, 1, 2, 1), ("t", 1, 1, 1), ("down", 0, 0, 0, 1), ("L", 0, 0, 1, 1),
    ("down", 0, 0, 1, 1), ("L", 0, 1, 1, 1), ("R", 0, 1, 0, 1), ("R", 0, 1, 3, 1), ("R", 0, 0, 0, 1),
    ("R", 0, 0, 3, 1), ("down", 0, 0, 1, 0), ("R", 0, 1, 0, 0), ("R", 0, 1, 3, 0), ("L", 0, 1, 1, 0),
    ("down", 0, 0, 0, 0), ("R", 0, 0, 3, 0), ("L", 0, 0, 1, 0), ("R", 0, 0, 0, 0), ("t", 0, 0, 2), ("s", 1, 0, 2, 1),
    ("s", 1, 0, 2, -1), ("t", 1, 0, 3), ("t", 0, 1, 2), ("s", 1, 1, 2, 1), ("s", 1, 1, 2, -1), ("up", 1, 0, 0),
    ("up", 1, 0, 1), ("down", 1, 0, 0, 0), ("R", 1, 0, 0, 0), ("R", 1, 0, 3, 0), ("down", 1, 0, 1, 1),
    ("R", 1, 1, 0, 1), ("L", 1, 1, 1, 1), ("L", 1, 0, 1, 0), ("down", 1, 0, 1, 0), ("L", 1, 1, 1, 0),
    ("R", 1, 1, 0, 0), ("R", 1, 1, 3, 1), ("R", 1, 1, 3, 0), ("t", 1, 1, 3), ("down", 1, 0, 0, 1), ("R", 1, 0, 3, 1),
    ("R", 1, 0, 0, 1), ("L", 1, 0, 1, 1), ("up", 0, 1, 0), ("up", 0, 1, 1), ("down", 0, 1, 0, 0), ("F", 0, 0, 0, 0),
    ("t", 1, 0, 2), ("t", 1, 1, 2), ("F", 0, 0, 2, 0), ("down", 0, 1, 0, 1), ("F", 0, 0, 3, 1), ("L", 0, 0, 2, 1),
    ("F", 0, 0, 2, 1), ("down", 0, 1, 1, 0), ("F", 0, 1, 2, 0), ("F", 0, 1, 3, 0), ("L", 0, 1, 2, 0),
    ("F", 0, 1, 1, 0), ("F", 0, 1, 0, 0), ("L", 0, 0, 2, 0), ("F", 0, 0, 0, 1), ("F", 0, 0, 1, 0), ("F", 0, 0, 3, 0),
    ("down", 0, 1, 1, 1), ("F", 0, 1, 0, 1), ("F", 0, 1, 2, 1), ("F", 0, 1, 3, 1), ("L", 0, 1, 2, 1),
    ("F", 0, 1, 1, 1), ("F", 0, 0, 1, 1), ("A", 0, 0, 0, 0), ("A", 0, 1, 3, 0), ("A", 0, 0, 3, 1), ("up", 1, 1, 0),
    ("up", 1, 1, 1), ("down", 1, 1, 1, 0), ("A", 0, 0, 2, 1), ("F", 1, 1, 0, 0), ("F", 1, 1, 1, 0), ("L", 1, 1, 2, 0),
    ("down", 1, 1, 0, 0), ("F", 1, 0, 0, 0), ("F", 1, 0, 2, 0), ("down", 1, 1, 1, 1), ("F", 1, 1, 0, 1),
    ("L", 1, 1, 2, 1), ("L", 1, 0, 2, 0), ("F", 1, 1, 3, 1), ("A", 0, 1, 1, 0), ("A", 0, 0, 1, 0), ("A", 0, 1, 2, 1),
    ("F", 1, 1, 2, 0), ("A", 0, 0, 0, 1), ("F", 1, 1, 2, 1), ("F", 1, 0, 1, 0), ("F", 1, 0, 3, 0), ("F", 1, 1, 3, 0),
    ("A", 0, 1, 3, 1), ("A", 0, 1, 0, 0), ("down", 1, 1, 0, 1), ("F", 1, 0, 2, 1), ("F", 1, 0, 0, 1),
    ("F", 1, 0, 1, 1), ("L", 1, 0, 2, 1), ("F", 1, 0, 3, 1), ("A", 0, 1, 2, 0), ("F", 1, 1, 1, 1), ("A", 0, 0, 2, 0),
    ("A", 0, 0, 3, 0), ("A", 0, 1, 0, 1), ("A", 0, 1, 1, 1), ("A", 0, 0, 1, 1), ("S", 0, 0, 0, 0), ("S", 0, 1, 3, 0),
    ("S", 0, 0, 3, 1), ("S", 0, 0, 2, 1), ("A", 1, 1, 0, 0), ("A", 1, 1, 1, 0), ("A", 1, 0, 0, 0), ("A", 1, 0, 2, 0),
    ("S", 0, 1, 1, 0), ("S", 0, 0, 1, 0), ("S", 0, 1, 2, 1), ("A", 1, 1, 0, 1), ("S", 0, 0, 0, 1), ("A", 1, 0, 1, 0),
    ("A", 1, 1, 2, 0), ("A", 1, 0, 3, 0), ("A", 1, 0, 2, 1), ("A", 1, 1, 3, 1), ("A", 1, 1, 2, 1), ("A", 1, 0, 0, 1),
    ("A", 1, 0, 1, 1), ("A", 1, 1, 3, 0), ("S", 0, 1, 2, 0), ("S", 0, 0, 2, 0), ("S", 0, 1, 3, 1), ("A", 1, 1, 1, 1),
    ("A", 1, 0, 3, 1), ("S", 0, 0, 1, 1), ("S", 0, 1, 1, 1), ("S", 0, 1, 0, 0), ("S", 0, 0, 3, 0), ("S", 0, 1, 0, 1),
    ("B", 0, 0, -1, 1), ("S", 1, 0, 0, 0), ("S", 1, 0, 2, 0), ("B", 0, 0, 1, 1), ("B", 0, 1, -1, 1),
    ("S", 1, 1, 1, 0), ("B", 0, 1, 1, 1), ("S", 1, 1, 0, 0), ("S", 1, 0, 1, 0), ("S", 1, 1, 2, 0), ("S", 1, 0, 3, 0),
    ("S", 1, 0, 2, 1), ("S", 1, 1, 2, 1), ("S", 1, 1, 0, 1), ("S", 1, 0, 0, 1), ("B", 0, 0, -1, 0), ("B", 0, 1, 1, 0),
    ("S", 1, 0, 1, 1), ("S", 1, 1, 3, 1), ("B", 0, 1, -1, 0), ("S", 1, 1, 1, 1), ("S", 1, 0, 3, 1), ("S", 1, 1, 3, 0),
    ("B", 0, 0, 1, 0), ("B", 1, 1, -1, 0), ("B", 1, 0, -1, 0), ("Z", 0, 1, 1), ("B", 1, 0, 1, 0), ("B", 1, 1, 1, 0),
    ("B", 1, 1, -1, 1), ("Z", 0, 0, 1), ("B", 1, 0, -1, 1), ("B", 1, 1, 1, 1), ("B", 1, 0, 1, 1), ("Z", 0, 1, 0),
    ("Z", 0, 0, 0), ("Z", 1, 0, 0), ("Z", 1, 1, 0), ("Z", 1, 1, 1), ("Z", 1, 0, 1), ("X", 0, 1, 1), ("X", 0, 0, 1),
    ("X", 0, 1, 0), ("X", 0, 0, 0), ("X", 1, 0, 0), ("X", 1, 1, 0), ("X", 1, 1, 1), ("X", 1, 0, 1),
)


def kernel(
    sel_hbm, gate_hbm, tok_ref, wg_ref, wu_ref, wd_ref, slots_ref, comb_ref,
    sel_ref, gate_ref, tok_v, wg_v, wu_v, wd_v, send4, recv4, exit4, ret4, rows, part, hid, relay, fin_l, fin_r, summed,
    relay1, fin1_l, fin1_r, slots32, send_sem, recv_sem, load_sem,
):
    slot = sel_hbm.shape[0]
    tok_dev, width = tok_ref.shape
    groups = 2 * RING
    n_slots = groups * slot
    halfw = width // 2
    quart = width // 4
    subw = halfw // SUB
    chunk = rows.shape[2]

    dp = lax.axis_index("dp")
    ex = lax.axis_index("expert")
    my_x, my_z = dp // RING, dp % RING
    my_y, my_c = ex // 2, ex % 2

    def at_x(step):
        return (((my_x + step + RING) % RING) * RING + my_z, ex)

    def at_z(step):
        return (my_x * RING + (my_z + step + RING) % RING, ex)

    def expert_at(g):
        return ((my_y + g // 2) % RING) * 2 + (my_c + g % 2) % 2

    def at_group(g):
        return (dp, expert_at(g))

    def back(g):
        return ((RING - g // 2) % RING) * 2 + g % 2

    barrier = pltpu.get_barrier_semaphore()
    partners = [at_x(1), at_x(-1), at_z(1), at_z(-1)] + [at_group(g) for g in range(1, groups)]
    for who in partners:
        pl.semaphore_signal(barrier, inc=1, device_id=who, device_id_type=MESH)

    loads = {}
    loads["sel"] = pltpu.make_async_copy(sel_hbm, sel_ref, load_sem.at[7])
    loads["gate"] = pltpu.make_async_copy(gate_hbm, gate_ref, load_sem.at[8])
    loads["sel"].start()
    tokw = width // 4
    for i in range(4):
        cols = pl.ds(i * tokw, tokw)
        loads[i] = pltpu.make_async_copy(tok_ref.at[:, cols], tok_v.at[:, cols], load_sem.at[i])
        loads[i].start()
    for i, (name, src, dst) in enumerate(
        (("wg", wg_ref, wg_v), ("wu", wu_ref, wu_v), ("wd", wd_ref, wd_v)), 4
    ):
        loads[name] = pltpu.make_async_copy(src, dst, load_sem.at[i])
        loads[name].start()

    loads["gate"].start()

    def loaded(*names):
        for name in names:
            if name in loads:
                loads.pop(name).wait()

    recv_of, recv_bytes, send_bytes = {}, {}, {}

    def together(key):
        kind, h = key[0], key[1]
        if kind == "in":
            return ("own", 0 if h in HALVES[0] else 1)
        if kind == "r":
            return key[:3]
        if kind == "t":
            return ("up", h, 1)
        if kind == "s" and key[4] != (1 if key[3] in RSET else -1):
            return ("up", h, int(key[3] == 2))
        if kind in ("L", "R"):
            return ("S", *key[1:])
        if kind in ("l1", "r1"):
            return ("Z", *key[1:])
        if kind == "b":
            return ("Z", h, key[2], key[4])
        return key[:4] if kind == "X" else key

    def outbox(key):
        kind, h = key[0], key[1]
        if kind == "in":
            return 0
        return (1 if kind in "fsrt" else 3 if kind != "X" else 5) + h

    def size(ref):
        n = 2
        for dim in ref.shape:
            n *= dim
        return n

    def wait_for(sem, n):
        row = 2 * chunk * width
        if n % row == 0:
            ref = rows.at[0, pl.ds(0, n // row)]
        elif n % (row // 4) == 0:
            ref = exit4.at[pl.ds(0, 4 * n // row)]
        else:
            ref = exit4.at[pl.ds(0, 16 * n // row), :, pl.ds(0, width // 4)]
        assert size(ref) == n
        pltpu.make_async_copy(ref, ref, sem).wait()

    def remote(key, src, dst, who):
        name, box = together(key), outbox(key)
        i = recv_of.setdefault(name, len(recv_of))
        recv_bytes[name] = recv_bytes.get(name, 0) + size(dst)
        send_bytes[box] = send_bytes.get(box, 0) + size(src)
        pltpu.make_async_remote_copy(
            src_ref=src, dst_ref=dst, send_sem=send_sem.at[box], recv_sem=recv_sem.at[i],
            device_id=who, device_id_type=MESH,
        ).start()

    def need(*names):
        for name in names:
            if name in recv_bytes:
                wait_for(recv_sem.at[recv_of[name]], recv_bytes.pop(name))

    def drain(*boxes):
        for box in boxes:
            wait_for(send_sem.at[box], send_bytes.pop(box))

    near = [back(g) for g in HALVES[0] if g > 0]
    far = [back(g) for g in HALVES[1]]
    with jax.named_scope("pick"):
        loaded("sel")
        row_id = lax.broadcasted_iota(jnp.int32, (n_slots, tok_dev), 0)
        lane_id = lax.broadcasted_iota(jnp.int32, (n_slots, tok_dev), 1)
        idx = jnp.full((n_slots, tok_dev), -1, jnp.int32)
        for g in range(groups):
            e = expert_at(g)
            for j in range(slot):
                idx = jnp.where(row_id == g * slot + j, sel_ref[j, e], idx)
        onehot = jnp.where(lane_id == idx, 1.0, 0.0).astype(BF16)
    for i in range(4):
        with jax.named_scope("tok"):
            loaded(i)
        with jax.named_scope("sel"):
            cols = slice(i * tokw, (i + 1) * tokw)
            slots32[:, cols] = jnp.dot(onehot, tok_v[:, cols], preferred_element_type=F32)
            for g in near:
                send4[g, :, cols] = slots32[g * slot : (g + 1) * slot, cols].astype(BF16)
    with jax.named_scope("barrier"):
        pl.semaphore_wait(barrier, len(partners))
    for g in near:
        remote(("in", back(g)), send4.at[g], recv4.at[back(g)], at_group(g))
    for g in far:
        send4[g] = slots32[g * slot : (g + 1) * slot, :].astype(BF16)
        remote(("in", back(g)), send4.at[g], recv4.at[back(g)], at_group(g))
    recv4[0] = slots32[0:slot, :].astype(BF16)
    loaded("gate")

    lane8 = lax.broadcasted_iota(jnp.int32, (8, 128), 1)
    idx_l = jnp.full((8, 128), -1, jnp.int32)
    gate_l = jnp.zeros((8, 128), F32)
    for g in range(groups):
        e = expert_at(g)
        for j in range(slot):
            here = lane8 % n_slots == g * slot + j
            idx_l = jnp.where(here, sel_ref[j, e], idx_l)
            gate_l = jnp.where(here, gate_ref[j, e], gate_l)
    g1 = gate_l.astype(BF16).astype(F32)
    rest = gate_l - g1
    g2 = rest.astype(BF16).astype(F32)
    g3 = (rest - g2).astype(BF16).astype(F32)
    term = lane8 // n_slots
    gate3 = jnp.where(term == 0, g1, jnp.where(term == 1, g2, jnp.where(term == 2, g3, 0.0)))
    tok_id = lax.broadcasted_iota(jnp.int32, (tok_dev, 128), 0)
    hit = tok_id == idx_l[0:1, :]
    comb_ref[...] = jnp.where(hit, gate3[0:1, :], 0.0).astype(BF16)

    def cut(p, lo=0, n=halfw):
        return pl.ds(p * halfw + lo, n)

    def pos(p, d1, d2):
        d1, d2 = d1 % RING, d2 % RING
        return PLACE[(d2, d1) if p == 0 else (d1, d2)]

    def first(p, step):
        return at_x(step) if p == 0 else at_z(step)

    def second(p, step):
        return at_z(step) if p == 0 else at_x(step)

    def own(h):
        need(("own", h))
        for i, g in enumerate(HALVES[h]):
            slots32[i * slot : (i + 1) * slot, :] = recv4[g].astype(F32)
        rows[h, 0] = slots32[0:chunk, :].astype(BF16)

    def to_first(key, h, p, d1, step, lo, n):
        remote(
            key, rows.at[h, pos(p, d1, 0), :, cut(p, lo, n)],
            rows.at[h, pos(p, d1 - step, 0), :, cut(p, lo, n)], first(p, step),
        )

    def to_second(key, h, p, d1, d2, step):
        remote(
            key, rows.at[h, pos(p, d1, d2), :, cut(p)],
            rows.at[h, pos(p, d1, d2 - step), :, cut(p)], second(p, step),
        )

    def send_first(h, p, step):
        to_first(("f", h, p, step), h, p, 0, step, 0, halfw)

    def pass_first(h, p, step):
        need(("f", h, p, step))
        to_first(("r", h, p, step), h, p, -step, step, 0 if step == 1 else quart, quart)

    def send_second(h, p, d1, step):
        if d1 == 2:
            need(("r", h, p))
        elif d1 != 0:
            need(("f", h, p, 1 if d1 == 3 else -1))
        to_second(("s", h, p, d1, step), h, p, d1, 0, step)

    def pass_second(h, p, d1):
        step = 1 if d1 in RSET else -1
        need(("s", h, p, d1, step))
        to_second(("t", h, p, d1), h, p, d1, -step, step)

    tn = hid.shape[2] // 2
    batches = (slice(0, len(EARLY)), slice(len(EARLY), RING * RING))

    def held(b):
        return slice(batches[b].start * chunk, batches[b].stop * chunk)

    def up(h, b, n):
        for p in range(2):
            if b == 1:
                need(("r", h, p))
            for step in (1, -1):
                need(("f", h, p, step))
                for d1 in RSET if step == 1 else LSET:
                    if b == 1 or d1 != 2:
                        need(("s", h, p, d1, step))
        need(("up", h, b))
        loaded("wg", "wu")
        lhs = rows[h, batches[b]].reshape(-1, width)
        cols = slice(n * tn, (n + 1) * tn)
        gate_val = jnp.dot(lhs, wg_v[:, cols], preferred_element_type=F32)
        up_val = jnp.dot(lhs, wu_v[:, cols], preferred_element_type=F32)
        hid[h, held(b), cols] = (gate_val / (1.0 + jnp.exp(-gate_val)) * up_val).astype(BF16)

    dn = 512

    def down(h, b, p, i):
        loaded("wd")
        start = p * halfw + i * subw
        for c in range(start, start + subw, dn):
            cols = slice(c, c + dn)
            val = jnp.dot(hid[h, held(b), :], wd_v[:, cols], preferred_element_type=F32)
            part[h, batches[b], :, cols] = val.astype(BF16).reshape(-1, chunk, dn)

    def sub(i, lo=0, n=subw):
        return pl.ds(i * subw + lo, n)

    def psub(p, i):
        return cut(p, i * subw, subw)

    def send_far(h, p, d1, i):
        step = 1 if d1 in RSET else -1
        remote(
            ("F", h, p, d1, i), part.at[h, pos(p, d1, 2), :, psub(p, i)],
            relay.at[h, p, d1, :, sub(i)], second(p, step),
        )

    def send_left_of(h, p, d1, i):
        remote(
            ("L", h, p, d1, i), part.at[h, pos(p, d1, 1), :, psub(p, i)],
            fin_l.at[h, p, d1, :, sub(i)], second(p, 1),
        )

    def send_right_of(h, p, d1, i):
        remote(
            ("R", h, p, d1, i), part.at[h, pos(p, d1, 3), :, psub(p, i)],
            fin_r.at[h, p, d1, :, sub(i)], second(p, -1),
        )

    def add_far(h, p, d1, i):
        need(("F", h, p, d1, i))
        right = d1 in RSET
        mine = part[h, pos(p, d1, 1 if right else 3), :, psub(p, i)]
        here = relay.at[h, p, d1, :, sub(i)]
        here[...] = (here[...].astype(F32) + mine.astype(F32)).astype(BF16)
        if right:
            remote(("L", h, p, d1, i), here, fin_l.at[h, p, d1, :, sub(i)], second(p, 1))
        else:
            remote(("R", h, p, d1, i), here, fin_r.at[h, p, d1, :, sub(i)], second(p, -1))

    def add_up(h, p, d1, i):
        need(("S", h, p, d1, i))
        mine = part[h, pos(p, d1, 0), :, psub(p, i)]
        total = (
            mine.astype(F32)
            + fin_l[h, p, d1, :, sub(i)].astype(F32)
            + fin_r[h, p, d1, :, sub(i)].astype(F32)
        )
        summed[h, p, d1, :, sub(i)] = total.astype(BF16)
        lo, hi = sub(i, 0, subw // 2), sub(i, subw // 2, subw // 2)
        if d1 == 2:
            remote(("F1", h, p, 1, i), summed.at[h, p, 2, :, lo], relay1.at[h, p, :, lo], first(p, 1))
            remote(("F1", h, p, -1, i), summed.at[h, p, 2, :, hi], relay1.at[h, p, :, hi], first(p, -1))
        elif d1 == 1:
            remote(("l1", h, p, i), summed.at[h, p, 1, :, hi], fin1_l.at[h, p, :, hi], first(p, 1))
        elif d1 == 3:
            remote(("r1", h, p, i), summed.at[h, p, 3, :, lo], fin1_r.at[h, p, :, lo], first(p, -1))

    def add_first(h, p, step, i):
        need(("F1", h, p, step, i))
        d1 = 1 if step == 1 else 3
        cols = sub(i, 0 if step == 1 else subw // 2, subw // 2)
        here = relay1.at[h, p, :, cols]
        here[...] = (here[...].astype(F32) + summed[h, p, d1, :, cols].astype(F32)).astype(BF16)
        dst = fin1_l if step == 1 else fin1_r
        remote(("b", h, p, step, i), here, dst.at[h, p, :, cols], first(p, step))

    def finish(h, p, i):
        need(("Z", h, p, i))
        slots32[0:chunk, psub(p, i)] = (
            summed[h, p, 0, :, sub(i)].astype(F32)
            + fin1_l[h, p, :, sub(i)].astype(F32)
            + fin1_r[h, p, :, sub(i)].astype(F32)
        )
        for r, g in enumerate(HALVES[h]):
            value = slots32[r * slot : (r + 1) * slot, psub(p, i)].astype(BF16)
            if g == 0:
                ret4[0, :, psub(p, i)] = value
            else:
                exit4[g, :, psub(p, i)] = value
                remote(
                    ("X", h, p, i, back(g)), exit4.at[g, :, psub(p, i)],
                    ret4.at[back(g), :, psub(p, i)], at_group(g),
                )

    def take(h, p, i):
        need(("X", h, p, i))
        for g in HALVES[h]:
            slots_ref[g * slot : (g + 1) * slot, psub(p, i)] = ret4[g, :, psub(p, i)].astype(F32)

    steps = {
        "own": own, "f": send_first, "r": pass_first, "s": send_second, "t": pass_second,
        "up": up, "down": down, "F": send_far, "L": send_left_of, "R": send_right_of,
        "A": add_far, "S": add_up, "B": add_first, "Z": finish, "X": take,
    }
    ends = [i for i, entry in enumerate(ORDER) if entry[0] == "Z"]
    for at, (name, *args) in enumerate(ORDER):
        with jax.named_scope("_".join(str(a) for a in (name, *args))):
            steps[name](*args)
        if at == ends[-1]:
            with jax.named_scope("drain"):
                drain(0, 1, 2, 3, 4, 5)
    with jax.named_scope("last_sends"):
        drain(6)


def combine_kernel(slots_ref, comb_ref, out_ref, out_v, out_sem):
    width = slots_ref.shape[1]
    n = 1024
    stores = []
    for k, c in enumerate(range(0, width, n)):
        value = slots_ref[:, c : c + n].astype(BF16)
        stack = jnp.concatenate([value, value, value, jnp.zeros_like(value)], axis=0)
        out_v[:, c : c + n] = jnp.dot(
            comb_ref[...], stack, preferred_element_type=F32).astype(BF16)
        store = pltpu.make_async_copy(
            out_v.at[:, pl.ds(c, n)], out_ref.at[:, pl.ds(c, n)], out_sem.at[k])
        store.start()
        stores.append(store)
    for store in stores:
        store.wait()


def per_device(tokens, select, gates, w_gate, w_up, w_down):
    tok_dev, width = tokens.shape
    slot = select.shape[1]
    ff = w_gate.shape[2]
    chunk = RING * slot
    halfw = width // 2
    vmem, hbm = pl.BlockSpec(memory_space=pltpu.VMEM), pl.BlockSpec(memory_space=pltpu.HBM)
    slots, comb = pl.pallas_call(
        kernel,
        out_shape=(pltpu.VMEM((8 * slot, width), F32), pltpu.VMEM((tok_dev, 128), BF16)),
        in_specs=[hbm] * 6,
        out_specs=(vmem, vmem),
        scratch_shapes=[
            pltpu.SMEM((slot, 8), jnp.int32),
            pltpu.SMEM((slot, 8), F32),
            pltpu.VMEM((tok_dev, width), BF16),
            pltpu.VMEM((width, ff), BF16),
            pltpu.VMEM((width, ff), BF16),
            pltpu.VMEM((ff, width), BF16),
            pltpu.VMEM((8, slot, width), BF16),
            pltpu.VMEM((8, slot, width), BF16),
            pltpu.VMEM((8, slot, width), BF16),
            pltpu.VMEM((8, slot, width), BF16),
            pltpu.VMEM((2, 16, chunk, width), BF16),
            pltpu.VMEM((2, 16, chunk, width), BF16),
            pltpu.VMEM((2, 16 * chunk, ff), BF16),
            pltpu.VMEM((2, 2, 4, chunk, halfw), BF16),
            pltpu.VMEM((2, 2, 4, chunk, halfw), BF16),
            pltpu.VMEM((2, 2, 4, chunk, halfw), BF16),
            pltpu.VMEM((2, 2, 4, chunk, halfw), BF16),
            pltpu.VMEM((2, 2, chunk, halfw), BF16),
            pltpu.VMEM((2, 2, chunk, halfw), BF16),
            pltpu.VMEM((2, 2, chunk, halfw), BF16),
            pltpu.VMEM((8 * slot, width), F32),
            pltpu.SemaphoreType.DMA((7,)),
            pltpu.SemaphoreType.DMA((N_RECV,)),
            pltpu.SemaphoreType.DMA((9,)),
        ],
        compiler_params=pltpu.CompilerParams(
            collective_id=0, has_side_effects=True, vmem_limit_bytes=56 * 1024 * 1024
        ),
        name="moe",
    )(
        select.T, gates.T, tokens, w_gate[0], w_up[0], w_down[0],
    )
    return pl.pallas_call(
        combine_kernel,
        out_shape=jax.ShapeDtypeStruct((tok_dev, width), BF16),
        in_specs=[vmem, vmem],
        out_specs=hbm,
        scratch_shapes=[pltpu.VMEM((tok_dev, width), BF16), pltpu.SemaphoreType.DMA((4,))],
        compiler_params=pltpu.CompilerParams(vmem_limit_bytes=8 * 1024 * 1024),
        name="combine",
    )(slots, comb)


def solution(mesh):
    return jax.shard_map(
        per_device,
        mesh=mesh,
        in_specs=(
            P(("dp", "expert"), None),
            P(None, ("dp", "expert")),
            P(None, ("dp", "expert")),
            P("expert", None, "dp"),
            P("expert", None, "dp"),
            P("expert", "dp", None),
        ),
        out_specs=P(("dp", "expert"), None),
        check_vma=False,
    )
```

```python
import jax
import jax.numpy as jnp
from jax import lax
from jax.experimental import pallas as pl
from jax.experimental.pallas import tpu as pltpu
from jax.sharding import PartitionSpec as P

MESH = pl.DeviceIdType.MESH
BF16, F32 = jnp.bfloat16, jnp.float32
RING = 4
SUB = 2
N_RECV = 122
DIRECT = (1,)
RSET, LSET = (0, 3), (2, 1)
EARLY = tuple((z, x) for z in (0, 1, 3) for x in (0, 1, 3))
LATE = tuple((z, x) for z in range(RING) for x in range(RING) if 2 in (z, x))
PLACE = {at: i for i, at in enumerate(EARLY + LATE)}
HALVES = ((0, 1, 2, 6), (3, 7, 4, 5))

ORDER = (
    ("own", 0), ("s", 0, 0, 0, -1), ("f", 0, 0, -1), ("f", 0, 0, 1), ("f", 0, 1, 1), ("s", 0, 1, 0, 1),
    ("f", 0, 1, -1), ("s", 0, 1, 0, -1), ("s", 0, 0, 0, 1), ("own", 1), ("s", 1, 1, 0, 1), ("s", 1, 0, 0, 1),
    ("f", 1, 0, -1), ("s", 1, 1, 0, -1), ("f", 1, 1, 1), ("f", 1, 1, -1), ("s", 1, 0, 0, -1), ("f", 1, 0, 1),
    ("s", 0, 0, 1, 1), ("r", 0, 0, -1), ("s", 0, 0, 3, -1), ("r", 0, 1, 1), ("s", 0, 1, 3, -1), ("r", 0, 0, 1),
    ("s", 0, 0, 1, -1), ("s", 0, 0, 3, 1), ("s", 0, 1, 3, 1), ("s", 0, 1, 1, 1), ("s", 0, 1, 1, -1), ("r", 0, 1, -1),
    ("t", 0, 0, 0), ("t", 0, 1, 0), ("r", 1, 1, -1), ("s", 1, 0, 1, -1), ("t", 1, 1, 0), ("r", 1, 0, -1),
    ("s", 1, 1, 1, -1), ("s", 1, 1, 1, 1), ("s", 1, 0, 1, 1), ("t", 1, 0, 0), ("r", 1, 0, 1), ("s", 1, 1, 3, 1),
    ("r", 1, 1, 1), ("s", 1, 1, 3, -1), ("s", 1, 0, 3, -1), ("s", 1, 0, 3, 1), ("s", 0, 0, 2, -1), ("s", 0, 0, 2, 1),
    ("t", 0, 1, 3), ("t", 0, 0, 1), ("s", 0, 1, 2, -1), ("t", 0, 1, 1), ("s", 0, 1, 2, 1), ("t", 0, 0, 3),
    ("up", 0, 0, 0), ("up", 0, 0, 1), ("down", 0, 0, 0, 1), ("R", 0, 0, 3, 1), ("down", 0, 0, 1, 0),
    ("down", 0, 0, 1, 1), ("R", 0, 1, 3, 1), ("R", 0, 1, 3, 0), ("R", 0, 1, 0, 0), ("L", 0, 1, 1, 1), ("t", 1, 1, 1),
    ("down", 0, 0, 0, 0), ("R", 0, 0, 0, 0), ("R", 0, 0, 3, 0), ("L", 0, 1, 1, 0), ("R", 0, 1, 0, 1),
    ("L", 0, 0, 1, 1), ("L", 0, 0, 1, 0), ("t", 1, 0, 1), ("R", 0, 0, 0, 1), ("t", 0, 0, 2), ("t", 0, 1, 2),
    ("s", 1, 0, 2, 1), ("s", 1, 1, 2, -1), ("s", 1, 1, 2, 1), ("s", 1, 0, 2, -1), ("t", 1, 1, 3), ("up", 1, 0, 0),
    ("t", 1, 0, 3), ("up", 1, 0, 1), ("down", 1, 0, 0, 1), ("L", 1, 0, 1, 1), ("down", 1, 0, 1, 0), ("R", 1, 1, 3, 0),
    ("down", 1, 0, 0, 0), ("R", 1, 0, 0, 0), ("R", 1, 0, 0, 1), ("L", 1, 0, 1, 0), ("down", 1, 0, 1, 1),
    ("R", 1, 1, 3, 1), ("L", 1, 1, 1, 0), ("R", 1, 1, 0, 1), ("R", 1, 1, 0, 0), ("L", 1, 1, 1, 1), ("R", 1, 0, 3, 1),
    ("R", 1, 0, 3, 0), ("up", 0, 1, 0), ("up", 0, 1, 1), ("t", 1, 1, 2), ("t", 1, 0, 2), ("down", 0, 1, 1, 0),
    ("F", 0, 1, 0, 0), ("down", 0, 1, 0, 1), ("F", 0, 0, 3, 1), ("F", 0, 0, 1, 1), ("F", 0, 0, 0, 1),
    ("F", 0, 1, 3, 0), ("L", 0, 0, 2, 1), ("F", 0, 1, 2, 0), ("down", 0, 1, 1, 1), ("F", 0, 1, 2, 1),
    ("F", 0, 1, 0, 1), ("L", 0, 1, 2, 1), ("F", 0, 1, 1, 1), ("F", 0, 0, 2, 1), ("L", 0, 1, 2, 0),
    ("down", 0, 1, 0, 0), ("F", 0, 0, 0, 0), ("F", 0, 0, 3, 0), ("F", 0, 0, 1, 0), ("F", 0, 0, 2, 0),
    ("L", 0, 0, 2, 0), ("F", 0, 1, 1, 0), ("F", 0, 1, 3, 1), ("A", 0, 1, 0, 0), ("A", 0, 0, 3, 1), ("up", 1, 1, 0),
    ("A", 0, 0, 0, 1), ("A", 0, 1, 3, 0), ("A", 0, 1, 2, 0), ("A", 0, 0, 1, 1), ("up", 1, 1, 1), ("A", 0, 1, 2, 1),
    ("A", 0, 0, 2, 1), ("A", 0, 1, 0, 1), ("down", 1, 1, 1, 0), ("F", 1, 1, 0, 0), ("F", 1, 1, 1, 0),
    ("F", 1, 1, 3, 0), ("A", 0, 0, 0, 0), ("L", 1, 1, 2, 0), ("F", 1, 1, 2, 0), ("down", 1, 1, 0, 1),
    ("F", 1, 0, 3, 1), ("L", 1, 0, 2, 1), ("F", 1, 0, 2, 1), ("A", 0, 0, 1, 0), ("down", 1, 1, 1, 1),
    ("L", 1, 1, 2, 1), ("F", 1, 1, 2, 1), ("F", 1, 1, 1, 1), ("F", 1, 0, 0, 1), ("A", 0, 0, 3, 0), ("A", 0, 1, 1, 0),
    ("A", 0, 0, 2, 0), ("down", 1, 1, 0, 0), ("L", 1, 0, 2, 0), ("F", 1, 0, 2, 0), ("F", 1, 1, 3, 1),
    ("F", 1, 1, 0, 1), ("A", 0, 1, 3, 1), ("F", 1, 0, 3, 0), ("F", 1, 0, 1, 1), ("F", 1, 0, 0, 0), ("A", 0, 1, 1, 1),
    ("F", 1, 0, 1, 0), ("S", 0, 1, 0, 0), ("S", 0, 0, 3, 1), ("S", 0, 1, 2, 0), ("S", 0, 0, 1, 1), ("S", 0, 1, 3, 0),
    ("S", 0, 0, 0, 1), ("S", 0, 1, 2, 1), ("S", 0, 0, 2, 1), ("S", 0, 1, 0, 1), ("S", 0, 0, 0, 0), ("A", 1, 1, 1, 0),
    ("A", 1, 0, 2, 1), ("A", 1, 1, 0, 0), ("A", 1, 0, 3, 1), ("A", 1, 1, 2, 0), ("S", 0, 0, 1, 0), ("A", 1, 1, 3, 0),
    ("A", 1, 1, 2, 1), ("S", 0, 0, 2, 0), ("A", 1, 0, 0, 1), ("A", 1, 1, 1, 1), ("A", 1, 0, 2, 0), ("S", 0, 0, 3, 0),
    ("S", 0, 1, 1, 0), ("A", 1, 0, 1, 1), ("A", 1, 1, 3, 1), ("S", 0, 1, 1, 1), ("A", 1, 0, 1, 0), ("A", 1, 1, 0, 1),
    ("B", 0, 1, -1, 0), ("A", 1, 0, 3, 0), ("B", 0, 0, -1, 1), ("S", 0, 1, 3, 1), ("B", 0, 1, -1, 1),
    ("A", 1, 0, 0, 0), ("S", 1, 1, 1, 0), ("B", 0, 1, 1, 0), ("B", 0, 0, 1, 1), ("S", 1, 0, 2, 1), ("B", 0, 1, 1, 1),
    ("S", 1, 1, 2, 0), ("S", 1, 1, 0, 0), ("S", 1, 0, 2, 0), ("S", 1, 0, 3, 1), ("S", 1, 1, 2, 1), ("B", 0, 0, -1, 0),
    ("S", 1, 0, 1, 1), ("S", 1, 0, 0, 1), ("S", 1, 1, 3, 0), ("B", 0, 0, 1, 0), ("S", 1, 1, 1, 1), ("S", 1, 0, 1, 0),
    ("S", 1, 1, 3, 1), ("S", 1, 0, 3, 0), ("S", 1, 1, 0, 1), ("S", 1, 0, 0, 0), ("Z", 0, 0, 1), ("Z", 0, 1, 0),
    ("Z", 0, 1, 1), ("Z", 1, 0, 1), ("Z", 0, 0, 0), ("Z", 1, 1, 0), ("Z", 1, 0, 0), ("Z", 1, 1, 1), ("X", 0, 0, 1),
    ("X", 0, 1, 0), ("X", 0, 1, 1), ("X", 1, 0, 1), ("X", 0, 0, 0), ("X", 1, 1, 0), ("X", 1, 0, 0), ("X", 1, 1, 1),
)


def kernel(
    sel_hbm, gate_hbm, tok_ref, wg_ref, wu_ref, wd_ref, slots_ref, comb_ref,
    sel_ref, gate_ref, tok_v, wg_v, wu_v, wd_v, send4, recv4, exit4, ret4, rows, part, hid, relay, fin_l, fin_r, summed,
    relay1, fin1_l, fin1_r, slots32, send_sem, recv_sem, load_sem,
):
    slot = sel_hbm.shape[0]
    tok_dev, width = tok_ref.shape
    groups = 2 * RING
    n_slots = groups * slot
    halfw = width // 2
    quart = width // 4
    subw = halfw // SUB
    chunk = rows.shape[2]

    dp = lax.axis_index("dp")
    ex = lax.axis_index("expert")
    my_x, my_z = dp // RING, dp % RING
    my_y, my_c = ex // 2, ex % 2

    def at_x(step):
        return (((my_x + step + RING) % RING) * RING + my_z, ex)

    def at_z(step):
        return (my_x * RING + (my_z + step + RING) % RING, ex)

    def expert_at(g):
        return ((my_y + g // 2) % RING) * 2 + (my_c + g % 2) % 2

    def at_group(g):
        return (dp, expert_at(g))

    def back(g):
        return ((RING - g // 2) % RING) * 2 + g % 2

    barrier = pltpu.get_barrier_semaphore()
    partners = [at(step) for at in (at_x, at_z) for step in (1, -1, 2)] + [at_group(g) for g in range(1, groups)]
    for who in partners:
        pl.semaphore_signal(barrier, inc=1, device_id=who, device_id_type=MESH)

    loads = {}
    loads["sel"] = pltpu.make_async_copy(sel_hbm, sel_ref, load_sem.at[7])
    loads["gate"] = pltpu.make_async_copy(gate_hbm, gate_ref, load_sem.at[8])
    loads["sel"].start()
    tokw = width // 4
    for i in range(4):
        cols = pl.ds(i * tokw, tokw)
        loads[i] = pltpu.make_async_copy(tok_ref.at[:, cols], tok_v.at[:, cols], load_sem.at[i])
        loads[i].start()
    for i, (name, src, dst) in enumerate(
        (("wg", wg_ref, wg_v), ("wu", wu_ref, wu_v), ("wd", wd_ref, wd_v)), 4
    ):
        loads[name] = pltpu.make_async_copy(src, dst, load_sem.at[i])
        loads[name].start()

    loads["gate"].start()

    def loaded(*names):
        for name in names:
            if name in loads:
                loads.pop(name).wait()

    recv_of, recv_bytes, send_bytes = {}, {}, {}

    def together(key):
        kind, h = key[0], key[1]
        if kind == "in":
            return ("own", 0 if h in HALVES[0] else 1)
        if kind == "r":
            return key[:3]
        if kind == "t":
            return ("up", h, 1)
        if kind == "s" and key[4] != (1 if key[3] in RSET else -1):
            return ("up", h, int(key[3] == 2))
        if kind in ("L", "R"):
            return ("S", *key[1:])
        if kind in ("l1", "r1") or (kind == "F1" and h in DIRECT):
            return ("Z", *key[1:])
        if kind == "b":
            return ("Z", h, key[2], key[4])
        return key[:4] if kind == "X" else key

    def outbox(key):
        kind, h = key[0], key[1]
        if kind == "in":
            return 0
        return (1 if kind in "fsrt" else 3 if kind != "X" else 5) + h

    def size(ref):
        n = 2
        for dim in ref.shape:
            n *= dim
        return n

    def wait_for(sem, n):
        row = 2 * chunk * width
        if n % row == 0:
            ref = rows.at[0, pl.ds(0, n // row)]
        elif n % (row // 4) == 0:
            ref = exit4.at[pl.ds(0, 4 * n // row)]
        else:
            ref = exit4.at[pl.ds(0, 16 * n // row), :, pl.ds(0, width // 4)]
        assert size(ref) == n
        pltpu.make_async_copy(ref, ref, sem).wait()

    def remote(key, src, dst, who):
        name, box = together(key), outbox(key)
        i = recv_of.setdefault(name, len(recv_of))
        recv_bytes[name] = recv_bytes.get(name, 0) + size(dst)
        send_bytes[box] = send_bytes.get(box, 0) + size(src)
        pltpu.make_async_remote_copy(
            src_ref=src, dst_ref=dst, send_sem=send_sem.at[box], recv_sem=recv_sem.at[i],
            device_id=who, device_id_type=MESH,
        ).start()

    def need(*names):
        for name in names:
            if name in recv_bytes:
                wait_for(recv_sem.at[recv_of[name]], recv_bytes.pop(name))

    def drain(*boxes):
        for box in boxes:
            wait_for(send_sem.at[box], send_bytes.pop(box))

    near = [back(g) for g in HALVES[0] if g > 0]
    far = [back(g) for g in HALVES[1]]
    with jax.named_scope("pick"):
        loaded("sel")
        row_id = lax.broadcasted_iota(jnp.int32, (n_slots, tok_dev), 0)
        lane_id = lax.broadcasted_iota(jnp.int32, (n_slots, tok_dev), 1)
        idx = jnp.full((n_slots, tok_dev), -1, jnp.int32)
        for g in range(groups):
            e = expert_at(g)
            for j in range(slot):
                idx = jnp.where(row_id == g * slot + j, sel_ref[j, e], idx)
        onehot = jnp.where(lane_id == idx, 1.0, 0.0).astype(BF16)
    for i in range(4):
        with jax.named_scope("tok"):
            loaded(i)
        with jax.named_scope("sel"):
            cols = slice(i * tokw, (i + 1) * tokw)
            slots32[:, cols] = jnp.dot(onehot, tok_v[:, cols], preferred_element_type=F32)
            for g in near:
                send4[g, :, cols] = slots32[g * slot : (g + 1) * slot, cols].astype(BF16)
    with jax.named_scope("barrier"):
        pl.semaphore_wait(barrier, len(partners))
    for g in near:
        remote(("in", back(g)), send4.at[g], recv4.at[back(g)], at_group(g))
    for g in far:
        send4[g] = slots32[g * slot : (g + 1) * slot, :].astype(BF16)
        remote(("in", back(g)), send4.at[g], recv4.at[back(g)], at_group(g))
    recv4[0] = slots32[0:slot, :].astype(BF16)
    loaded("gate")

    lane8 = lax.broadcasted_iota(jnp.int32, (8, 128), 1)
    idx_l = jnp.full((8, 128), -1, jnp.int32)
    gate_l = jnp.zeros((8, 128), F32)
    for g in range(groups):
        e = expert_at(g)
        for j in range(slot):
            here = lane8 % n_slots == g * slot + j
            idx_l = jnp.where(here, sel_ref[j, e], idx_l)
            gate_l = jnp.where(here, gate_ref[j, e], gate_l)
    g1 = gate_l.astype(BF16).astype(F32)
    rest = gate_l - g1
    g2 = rest.astype(BF16).astype(F32)
    g3 = (rest - g2).astype(BF16).astype(F32)
    term = lane8 // n_slots
    gate3 = jnp.where(term == 0, g1, jnp.where(term == 1, g2, jnp.where(term == 2, g3, 0.0)))
    tok_id = lax.broadcasted_iota(jnp.int32, (tok_dev, 128), 0)
    hit = tok_id == idx_l[0:1, :]
    comb_ref[...] = jnp.where(hit, gate3[0:1, :], 0.0).astype(BF16)

    def cut(p, lo=0, n=halfw):
        return pl.ds(p * halfw + lo, n)

    def pos(p, d1, d2):
        d1, d2 = d1 % RING, d2 % RING
        return PLACE[(d2, d1) if p == 0 else (d1, d2)]

    def first(p, step):
        return at_x(step) if p == 0 else at_z(step)

    def second(p, step):
        return at_z(step) if p == 0 else at_x(step)

    def own(h):
        need(("own", h))
        for i, g in enumerate(HALVES[h]):
            slots32[i * slot : (i + 1) * slot, :] = recv4[g].astype(F32)
        rows[h, 0] = slots32[0:chunk, :].astype(BF16)

    def to_first(key, h, p, d1, step, lo, n):
        remote(
            key, rows.at[h, pos(p, d1, 0), :, cut(p, lo, n)],
            rows.at[h, pos(p, d1 - step, 0), :, cut(p, lo, n)], first(p, step),
        )

    def to_second(key, h, p, d1, d2, step):
        remote(
            key, rows.at[h, pos(p, d1, d2), :, cut(p)],
            rows.at[h, pos(p, d1, d2 - step), :, cut(p)], second(p, step),
        )

    def send_first(h, p, step):
        to_first(("f", h, p, step), h, p, 0, step, 0, halfw)

    def pass_first(h, p, step):
        need(("f", h, p, step))
        to_first(("r", h, p, step), h, p, -step, step, 0 if step == 1 else quart, quart)

    def send_second(h, p, d1, step):
        if d1 == 2:
            need(("r", h, p))
        elif d1 != 0:
            need(("f", h, p, 1 if d1 == 3 else -1))
        to_second(("s", h, p, d1, step), h, p, d1, 0, step)

    def pass_second(h, p, d1):
        step = 1 if d1 in RSET else -1
        need(("s", h, p, d1, step))
        to_second(("t", h, p, d1), h, p, d1, -step, step)

    tn = hid.shape[2] // 2
    batches = (slice(0, len(EARLY)), slice(len(EARLY), RING * RING))

    def held(b):
        return slice(batches[b].start * chunk, batches[b].stop * chunk)

    def up(h, b, n):
        for p in range(2):
            if b == 1:
                need(("r", h, p))
            for step in (1, -1):
                need(("f", h, p, step))
                for d1 in RSET if step == 1 else LSET:
                    if b == 1 or d1 != 2:
                        need(("s", h, p, d1, step))
        need(("up", h, b))
        loaded("wg", "wu")
        lhs = rows[h, batches[b]].reshape(-1, width)
        cols = slice(n * tn, (n + 1) * tn)
        gate_val = jnp.dot(lhs, wg_v[:, cols], preferred_element_type=F32)
        up_val = jnp.dot(lhs, wu_v[:, cols], preferred_element_type=F32)
        hid[h, held(b), cols] = (gate_val / (1.0 + jnp.exp(-gate_val)) * up_val).astype(BF16)

    dn = 512

    def down(h, b, p, i):
        loaded("wd")
        start = p * halfw + i * subw
        for c in range(start, start + subw, dn):
            cols = slice(c, c + dn)
            val = jnp.dot(hid[h, held(b), :], wd_v[:, cols], preferred_element_type=F32)
            part[h, batches[b], :, cols] = val.astype(BF16).reshape(-1, chunk, dn)

    def sub(i, lo=0, n=subw):
        return pl.ds(i * subw + lo, n)

    def psub(p, i):
        return cut(p, i * subw, subw)

    def send_far(h, p, d1, i):
        step = 1 if d1 in RSET else -1
        remote(
            ("F", h, p, d1, i), part.at[h, pos(p, d1, 2), :, psub(p, i)],
            relay.at[h, p, d1, :, sub(i)], second(p, step),
        )

    def send_left_of(h, p, d1, i):
        remote(
            ("L", h, p, d1, i), part.at[h, pos(p, d1, 1), :, psub(p, i)],
            fin_l.at[h, p, d1, :, sub(i)], second(p, 1),
        )

    def send_right_of(h, p, d1, i):
        remote(
            ("R", h, p, d1, i), part.at[h, pos(p, d1, 3), :, psub(p, i)],
            fin_r.at[h, p, d1, :, sub(i)], second(p, -1),
        )

    def add_far(h, p, d1, i):
        need(("F", h, p, d1, i))
        right = d1 in RSET
        mine = part[h, pos(p, d1, 1 if right else 3), :, psub(p, i)]
        here = relay.at[h, p, d1, :, sub(i)]
        here[...] = (here[...].astype(F32) + mine.astype(F32)).astype(BF16)
        if right:
            remote(("L", h, p, d1, i), here, fin_l.at[h, p, d1, :, sub(i)], second(p, 1))
        else:
            remote(("R", h, p, d1, i), here, fin_r.at[h, p, d1, :, sub(i)], second(p, -1))

    def add_up(h, p, d1, i):
        need(("S", h, p, d1, i))
        mine = part[h, pos(p, d1, 0), :, psub(p, i)]
        total = (
            mine.astype(F32)
            + fin_l[h, p, d1, :, sub(i)].astype(F32)
            + fin_r[h, p, d1, :, sub(i)].astype(F32)
        )
        summed[h, p, d1, :, sub(i)] = total.astype(BF16)
        lo, hi = sub(i, 0, subw // 2), sub(i, subw // 2, subw // 2)
        if h in DIRECT:
            if d1 != 0:
                name, dst, step = {2: ("F1", relay1, 2), 1: ("l1", fin1_l, 1), 3: ("r1", fin1_r, -1)}[d1]
                remote(
                    (name, h, p, i), summed.at[h, p, d1, :, sub(i)], dst.at[h, p, :, sub(i)],
                    first(p, step),
                )
            return
        if d1 == 2:
            remote(("F1", h, p, 1, i), summed.at[h, p, 2, :, lo], relay1.at[h, p, :, lo], first(p, 1))
            remote(("F1", h, p, -1, i), summed.at[h, p, 2, :, hi], relay1.at[h, p, :, hi], first(p, -1))
        elif d1 == 1:
            remote(("l1", h, p, i), summed.at[h, p, 1, :, hi], fin1_l.at[h, p, :, hi], first(p, 1))
        elif d1 == 3:
            remote(("r1", h, p, i), summed.at[h, p, 3, :, lo], fin1_r.at[h, p, :, lo], first(p, -1))

    def add_first(h, p, step, i):
        need(("F1", h, p, step, i))
        d1 = 1 if step == 1 else 3
        cols = sub(i, 0 if step == 1 else subw // 2, subw // 2)
        here = relay1.at[h, p, :, cols]
        here[...] = (here[...].astype(F32) + summed[h, p, d1, :, cols].astype(F32)).astype(BF16)
        dst = fin1_l if step == 1 else fin1_r
        remote(("b", h, p, step, i), here, dst.at[h, p, :, cols], first(p, step))

    def finish(h, p, i):
        need(("Z", h, p, i))
        total = (
            summed[h, p, 0, :, sub(i)].astype(F32)
            + fin1_l[h, p, :, sub(i)].astype(F32)
            + fin1_r[h, p, :, sub(i)].astype(F32)
        )
        if h in DIRECT:
            total += relay1[h, p, :, sub(i)].astype(F32)
        slots32[0:chunk, psub(p, i)] = total
        for r, g in enumerate(HALVES[h]):
            value = slots32[r * slot : (r + 1) * slot, psub(p, i)].astype(BF16)
            if g == 0:
                ret4[0, :, psub(p, i)] = value
            else:
                exit4[g, :, psub(p, i)] = value
                remote(
                    ("X", h, p, i, back(g)), exit4.at[g, :, psub(p, i)],
                    ret4.at[back(g), :, psub(p, i)], at_group(g),
                )

    def take(h, p, i):
        need(("X", h, p, i))
        for g in HALVES[h]:
            slots_ref[g * slot : (g + 1) * slot, psub(p, i)] = ret4[g, :, psub(p, i)].astype(F32)

    steps = {
        "own": own, "f": send_first, "r": pass_first, "s": send_second, "t": pass_second,
        "up": up, "down": down, "F": send_far, "L": send_left_of, "R": send_right_of,
        "A": add_far, "S": add_up, "B": add_first, "Z": finish, "X": take,
    }
    ends = [i for i, entry in enumerate(ORDER) if entry[0] == "Z"]
    for at, (name, *args) in enumerate(ORDER):
        with jax.named_scope("_".join(str(a) for a in (name, *args))):
            steps[name](*args)
        if at == ends[-1]:
            with jax.named_scope("drain"):
                drain(0, 1, 2, 3, 4, 5)
    with jax.named_scope("last_sends"):
        drain(6)


def combine_kernel(slots_ref, comb_ref, out_ref, out_v, out_sem):
    width = slots_ref.shape[1]
    n = 1024
    stores = []
    for k, c in enumerate(range(0, width, n)):
        value = slots_ref[:, c : c + n].astype(BF16)
        stack = jnp.concatenate([value, value, value, jnp.zeros_like(value)], axis=0)
        out_v[:, c : c + n] = jnp.dot(
            comb_ref[...], stack, preferred_element_type=F32).astype(BF16)
        store = pltpu.make_async_copy(
            out_v.at[:, pl.ds(c, n)], out_ref.at[:, pl.ds(c, n)], out_sem.at[k])
        store.start()
        stores.append(store)
    for store in stores:
        store.wait()


def per_device(tokens, select, gates, w_gate, w_up, w_down):
    tok_dev, width = tokens.shape
    slot = select.shape[1]
    ff = w_gate.shape[2]
    chunk = RING * slot
    halfw = width // 2
    vmem, hbm = pl.BlockSpec(memory_space=pltpu.VMEM), pl.BlockSpec(memory_space=pltpu.HBM)
    slots, comb = pl.pallas_call(
        kernel,
        out_shape=(pltpu.VMEM((8 * slot, width), F32), pltpu.VMEM((tok_dev, 128), BF16)),
        in_specs=[hbm] * 6,
        out_specs=(vmem, vmem),
        scratch_shapes=[
            pltpu.SMEM((slot, 8), jnp.int32),
            pltpu.SMEM((slot, 8), F32),
            pltpu.VMEM((tok_dev, width), BF16),
            pltpu.VMEM((width, ff), BF16),
            pltpu.VMEM((width, ff), BF16),
            pltpu.VMEM((ff, width), BF16),
            pltpu.VMEM((8, slot, width), BF16),
            pltpu.VMEM((8, slot, width), BF16),
            pltpu.VMEM((8, slot, width), BF16),
            pltpu.VMEM((8, slot, width), BF16),
            pltpu.VMEM((2, 16, chunk, width), BF16),
            pltpu.VMEM((2, 16, chunk, width), BF16),
            pltpu.VMEM((2, 16 * chunk, ff), BF16),
            pltpu.VMEM((2, 2, 4, chunk, halfw), BF16),
            pltpu.VMEM((2, 2, 4, chunk, halfw), BF16),
            pltpu.VMEM((2, 2, 4, chunk, halfw), BF16),
            pltpu.VMEM((2, 2, 4, chunk, halfw), BF16),
            pltpu.VMEM((2, 2, chunk, halfw), BF16),
            pltpu.VMEM((2, 2, chunk, halfw), BF16),
            pltpu.VMEM((2, 2, chunk, halfw), BF16),
            pltpu.VMEM((8 * slot, width), F32),
            pltpu.SemaphoreType.DMA((7,)),
            pltpu.SemaphoreType.DMA((N_RECV,)),
            pltpu.SemaphoreType.DMA((9,)),
        ],
        compiler_params=pltpu.CompilerParams(
            collective_id=0, has_side_effects=True, vmem_limit_bytes=56 * 1024 * 1024
        ),
        name="moe",
    )(
        select.T, gates.T, tokens, w_gate[0], w_up[0], w_down[0],
    )
    return pl.pallas_call(
        combine_kernel,
        out_shape=jax.ShapeDtypeStruct((tok_dev, width), BF16),
        in_specs=[vmem, vmem],
        out_specs=hbm,
        scratch_shapes=[pltpu.VMEM((tok_dev, width), BF16), pltpu.SemaphoreType.DMA((4,))],
        compiler_params=pltpu.CompilerParams(vmem_limit_bytes=8 * 1024 * 1024),
        name="combine",
    )(slots, comb)


def solution(mesh):
    return jax.shard_map(
        per_device,
        mesh=mesh,
        in_specs=(
            P(("dp", "expert"), None),
            P(None, ("dp", "expert")),
            P(None, ("dp", "expert")),
            P("expert", None, "dp"),
            P("expert", None, "dp"),
            P("expert", "dp", None),
        ),
        out_specs=P(("dp", "expert"), None),
        check_vma=False,
    )
```

```python
import jax
import jax.numpy as jnp
from jax import lax
from jax.experimental import pallas as pl
from jax.experimental.pallas import tpu as pltpu
from jax.sharding import PartitionSpec as P

MESH = pl.DeviceIdType.MESH
BF16, F32 = jnp.bfloat16, jnp.float32
RING = 4
N_RECV = 141
DIRECT = (2,)
RSET, LSET = (0, 3), (2, 1)
ROUND = tuple((z, x) for z in range(RING) for x in range(RING))
EARLY = tuple(at for at in ROUND if 2 not in at and at != (1, 3))
LATE = tuple(at for at in ROUND if at not in EARLY)
PLACE = {at: i for i, at in enumerate(EARLY + LATE)}
BATCHES = ((0, 1), (2, 6, 3, 7), (4, 5))
SUBS = (1, 2, 1)
SPLIT = (1,)

ORDER = (
    ("own", 0), ("f", 0, 0, -1), ("f", 0, 1, -1), ("s", 0, 1, 0, -1), ("f", 0, 1, 1), ("s", 0, 0, 0, -1),
    ("f", 0, 0, 1), ("s", 0, 0, 0, 1), ("s", 0, 1, 0, 1), ("s", 0, 0, 1, -1), ("s", 0, 1, 1, -1), ("s", 0, 0, 1, 1),
    ("s", 0, 1, 1, 1), ("s", 0, 1, 3, -1), ("r", 0, 1, 1), ("r", 0, 0, 1), ("s", 0, 0, 3, 1), ("s", 0, 0, 3, -1),
    ("s", 0, 1, 3, 1), ("r", 0, 1, -1), ("r", 0, 0, -1), ("own", 1), ("f", 1, 0, -1), ("f", 1, 0, 1),
    ("s", 1, 1, 0, -1), ("s", 1, 1, 0, 1), ("f", 1, 1, -1), ("s", 1, 0, 0, -1), ("f", 1, 1, 1), ("s", 1, 0, 0, 1),
    ("t", 0, 0, 0), ("t", 0, 1, 0), ("own", 2), ("f", 2, 0, -1), ("f", 2, 0, 1), ("f", 2, 1, 1), ("s", 2, 1, 0, 1),
    ("s", 2, 0, 0, 1), ("s", 2, 0, 0, -1), ("f", 2, 1, -1), ("s", 2, 1, 0, -1), ("t", 0, 0, 1), ("t", 0, 1, 1),
    ("s", 0, 1, 2, -1), ("s", 0, 0, 2, -1), ("s", 0, 1, 2, 1), ("t", 0, 0, 3), ("t", 0, 1, 3), ("s", 0, 0, 2, 1),
    ("r", 1, 1, -1), ("r", 1, 0, -1), ("r", 1, 1, 1), ("s", 1, 0, 3, 1), ("s", 1, 1, 3, 1), ("r", 1, 0, 1),
    ("s", 1, 0, 3, -1), ("s", 1, 1, 1, -1), ("s", 1, 0, 1, 1), ("s", 1, 1, 3, -1), ("s", 1, 0, 1, -1),
    ("s", 1, 1, 1, 1), ("t", 1, 0, 0), ("t", 1, 1, 0), ("s", 2, 0, 1, -1), ("s", 2, 0, 1, 1), ("r", 2, 0, -1),
    ("s", 2, 1, 1, -1), ("r", 2, 1, -1), ("r", 2, 1, 1), ("r", 2, 0, 1), ("s", 2, 0, 3, -1), ("s", 2, 1, 3, 1),
    ("s", 2, 0, 3, 1), ("s", 2, 1, 3, -1), ("s", 2, 1, 1, 1), ("t", 2, 0, 0), ("t", 2, 1, 0), ("t", 0, 0, 2),
    ("t", 0, 1, 2), ("s", 1, 1, 2, -1), ("s", 1, 1, 2, 1), ("t", 1, 1, 1), ("t", 1, 1, 3), ("t", 1, 0, 3),
    ("s", 1, 0, 2, -1), ("s", 1, 0, 2, 1), ("t", 1, 0, 1), ("t", 2, 0, 1), ("up", 1, 0, 0), ("t", 2, 1, 1),
    ("up", 1, 0, 1), ("down", 1, 0, 0, 1), ("s", 2, 0, 2, -1), ("up", 0, 2, 0), ("s", 2, 1, 2, -1),
    ("down", 1, 0, 0, 0), ("R", 1, 0, 3, 0), ("down", 1, 0, 1, 1), ("R", 1, 1, 3, 1), ("t", 2, 0, 3),
    ("L", 1, 1, 1, 1), ("t", 1, 0, 2), ("t", 1, 1, 2), ("R", 1, 1, 0, 1), ("R", 1, 0, 0, 0), ("s", 2, 0, 2, 1),
    ("t", 2, 1, 3), ("R", 1, 0, 3, 1), ("down", 1, 0, 1, 0), ("L", 1, 1, 1, 0), ("up", 0, 2, 1), ("down", 0, 2, 0, 0),
    ("F", 0, 0, 1, 0), ("L", 0, 0, 1, 0), ("F", 0, 0, 2, 0), ("F", 0, 0, 3, 0), ("R", 0, 0, 3, 0), ("R", 0, 0, 0, 0),
    ("down", 0, 2, 1, 0), ("t", 2, 0, 2), ("F", 0, 1, 3, 0), ("F", 0, 1, 0, 0), ("F", 0, 1, 2, 0), ("F", 0, 1, 1, 0),
    ("R", 0, 1, 0, 0), ("R", 1, 1, 0, 0), ("R", 1, 1, 3, 0), ("L", 0, 0, 2, 0), ("s", 2, 1, 2, 1), ("t", 2, 1, 2),
    ("R", 0, 1, 3, 0), ("L", 1, 0, 1, 0), ("L", 0, 1, 1, 0), ("R", 1, 0, 0, 1), ("L", 1, 0, 1, 1), ("F", 0, 0, 0, 0),
    ("L", 0, 1, 2, 0), ("up", 1, 1, 0), ("up", 1, 1, 1), ("A", 0, 1, 3, 0), ("down", 1, 1, 0, 1), ("F", 1, 0, 3, 1),
    ("F", 1, 0, 0, 1), ("down", 1, 1, 1, 0), ("F", 1, 1, 2, 0), ("F", 1, 1, 0, 0), ("F", 1, 1, 3, 0),
    ("down", 1, 1, 0, 0), ("F", 1, 0, 0, 0), ("F", 1, 0, 2, 0), ("F", 1, 0, 2, 1), ("down", 1, 1, 1, 1),
    ("L", 1, 1, 2, 1), ("A", 0, 0, 2, 0), ("F", 1, 1, 0, 1), ("F", 1, 1, 2, 1), ("A", 0, 0, 1, 0), ("A", 0, 1, 0, 0),
    ("A", 0, 1, 1, 0), ("L", 1, 1, 2, 0), ("A", 0, 1, 2, 0), ("F", 1, 1, 1, 1), ("L", 1, 0, 2, 0), ("A", 0, 0, 3, 0),
    ("F", 1, 0, 1, 1), ("F", 1, 1, 1, 0), ("F", 1, 0, 3, 0), ("F", 1, 0, 1, 0), ("L", 1, 0, 2, 1), ("F", 1, 1, 3, 1),
    ("A", 0, 0, 0, 0), ("up", 2, 2, 0), ("S", 0, 1, 3, 0), ("A", 1, 1, 0, 0), ("up", 2, 2, 1), ("A", 1, 0, 2, 0),
    ("A", 1, 1, 2, 0), ("down", 2, 2, 1, 0), ("A", 1, 0, 0, 0), ("F", 2, 1, 3, 0), ("R", 2, 1, 3, 0),
    ("A", 1, 0, 2, 1), ("F", 2, 1, 0, 0), ("F", 2, 1, 2, 0), ("L", 2, 1, 1, 0), ("R", 2, 1, 0, 0), ("L", 2, 1, 2, 0),
    ("A", 1, 0, 0, 1), ("A", 1, 1, 2, 1), ("down", 2, 2, 0, 0), ("F", 2, 0, 3, 0), ("S", 0, 0, 2, 0),
    ("F", 2, 0, 2, 0), ("S", 0, 0, 3, 0), ("L", 2, 0, 1, 0), ("R", 2, 0, 0, 0), ("F", 2, 0, 0, 0), ("A", 1, 1, 0, 1),
    ("R", 2, 0, 3, 0), ("F", 2, 0, 1, 0), ("L", 2, 0, 2, 0), ("A", 1, 1, 3, 0), ("F", 2, 1, 1, 0), ("A", 1, 0, 3, 1),
    ("S", 0, 1, 1, 0), ("S", 0, 1, 0, 0), ("S", 0, 0, 1, 0), ("S", 0, 1, 2, 0), ("A", 1, 0, 3, 0), ("A", 1, 0, 1, 1),
    ("A", 1, 1, 1, 1), ("A", 1, 0, 1, 0), ("A", 1, 1, 1, 0), ("A", 1, 1, 3, 1), ("S", 0, 0, 0, 0), ("S", 1, 1, 2, 0),
    ("S", 1, 1, 0, 0), ("S", 1, 0, 2, 0), ("S", 1, 0, 0, 0), ("A", 2, 1, 3, 0), ("S", 1, 0, 2, 1), ("S", 1, 0, 0, 1),
    ("A", 2, 1, 2, 0), ("A", 2, 1, 0, 0), ("A", 2, 0, 2, 0), ("A", 2, 0, 3, 0), ("S", 1, 1, 2, 1), ("A", 2, 0, 0, 0),
    ("B", 0, 0, 1, 0), ("B", 0, 0, -1, 0), ("A", 2, 0, 1, 0), ("S", 1, 1, 0, 1), ("B", 0, 1, -1, 0),
    ("A", 2, 1, 1, 0), ("S", 1, 0, 3, 1), ("S", 1, 1, 3, 0), ("S", 1, 0, 1, 1), ("S", 1, 1, 1, 1), ("B", 0, 1, 1, 0),
    ("S", 1, 0, 1, 0), ("S", 1, 1, 1, 0), ("S", 1, 1, 3, 1), ("B", 1, 1, -1, 0), ("S", 1, 0, 3, 0),
    ("B", 1, 0, -1, 0), ("B", 1, 0, 1, 0), ("B", 1, 1, 1, 0), ("B", 1, 0, -1, 1), ("S", 2, 0, 2, 0),
    ("S", 2, 1, 3, 0), ("B", 1, 1, -1, 1), ("S", 2, 0, 3, 0), ("S", 2, 1, 2, 0), ("B", 1, 0, 1, 1), ("B", 1, 1, 1, 1),
    ("S", 2, 0, 1, 0), ("S", 2, 1, 0, 0), ("S", 2, 0, 0, 0), ("Z", 0, 0, 0), ("S", 2, 1, 1, 0), ("Z", 0, 1, 0),
    ("Z", 1, 0, 0), ("Z", 1, 1, 0), ("Z", 1, 0, 1), ("Z", 1, 1, 1), ("Z", 2, 0, 0), ("Z", 2, 1, 0), ("X", 0, 0, 0),
    ("X", 0, 1, 0), ("X", 1, 0, 0), ("X", 1, 1, 0), ("X", 1, 0, 1), ("X", 1, 1, 1), ("X", 2, 0, 0), ("X", 2, 1, 0),
)


def kernel(
    sel_hbm, gate_hbm, tok_ref, wg_ref, wu_ref, wd_ref, slots_ref, comb_ref,
    sel_ref, gate_ref, tok_v, wg_v, wu_v, wd_v, send4, recv4, exit4, ret4, rows, part, hid, relay, fin_l, fin_r,
    summed, relay1, fin1_l, fin1_r, slots32, send_sem, recv_sem, load_sem,
):
    slot = sel_hbm.shape[0]
    tok_dev, width = tok_ref.shape
    groups = 2 * RING
    n_slots = groups * slot
    halfw = width // 2
    quart = width // 4
    subw = [halfw // n for n in SUBS]
    chunk = [r.shape[1] for r in rows]
    batch_of = {g: h for h, batch in enumerate(BATCHES) for g in batch}

    dp = lax.axis_index("dp")
    ex = lax.axis_index("expert")
    my_x, my_z = dp // RING, dp % RING
    my_y, my_c = ex // 2, ex % 2

    def at_x(step):
        return (((my_x + step + RING) % RING) * RING + my_z, ex)

    def at_z(step):
        return (my_x * RING + (my_z + step + RING) % RING, ex)

    def expert_at(g):
        return ((my_y + g // 2) % RING) * 2 + (my_c + g % 2) % 2

    def at_group(g):
        return (dp, expert_at(g))

    def back(g):
        return ((RING - g // 2) % RING) * 2 + g % 2

    barrier = pltpu.get_barrier_semaphore()
    partners = [at(step) for at in (at_x, at_z) for step in (1, -1, 2)] + [at_group(g) for g in range(1, groups)]
    for who in partners:
        pl.semaphore_signal(barrier, inc=1, device_id=who, device_id_type=MESH)

    loads = {}
    loads["sel"] = pltpu.make_async_copy(sel_hbm, sel_ref, load_sem.at[7])
    loads["gate"] = pltpu.make_async_copy(gate_hbm, gate_ref, load_sem.at[8])
    loads["sel"].start()
    tokw = width // 4
    for i in range(4):
        cols = pl.ds(i * tokw, tokw)
        loads[i] = pltpu.make_async_copy(tok_ref.at[:, cols], tok_v.at[:, cols], load_sem.at[i])
        loads[i].start()
    for i, (name, src, dst) in enumerate(
        (("wg", wg_ref, wg_v), ("wu", wu_ref, wu_v), ("wd", wd_ref, wd_v)), 4
    ):
        loads[name] = pltpu.make_async_copy(src, dst, load_sem.at[i])
        loads[name].start()

    loads["gate"].start()

    def loaded(*names):
        for name in names:
            if name in loads:
                loads.pop(name).wait()

    recv_of, recv_bytes, send_bytes = {}, {}, {}

    def together(key):
        kind, h = key[0], key[1]
        if kind == "in":
            return ("own", batch_of[h])
        if kind == "r":
            return key[:3]
        if kind == "t":
            return ("up", h, 1 if h in SPLIT else 2)
        if kind == "s" and key[4] != (1 if key[3] in RSET else -1):
            return ("up", h, int(key[3] == 2) if h in SPLIT else 2)
        if kind in ("L", "R"):
            return ("S", *key[1:])
        if kind in ("l1", "r1") or (kind == "F1" and h in DIRECT):
            return ("Z", *key[1:])
        if kind == "b":
            return ("Z", h, key[2], key[4])
        return key[:4] if kind == "X" else key

    def outbox(key):
        kind, h = key[0], key[1]
        if kind == "in":
            return 0
        return (1 if kind in "fsrt" else 4 if kind != "X" else 7) + h

    def size(ref):
        n = 2
        for dim in ref.shape:
            n *= dim
        return n

    def wait_for(sem, n):
        unit = 2 * slot * width
        if n % (4 * unit) == 0:
            ref = rows[1].at[pl.ds(0, n // (4 * unit))]
        elif n % (2 * unit) == 0 and n > 8 * unit:
            ref = rows[0].at[pl.ds(0, n // (2 * unit))]
        elif n % unit == 0:
            ref = exit4.at[pl.ds(0, n // unit)]
        else:
            ref = exit4.at[pl.ds(0, 2 * n // unit), :, pl.ds(0, halfw)]
        assert size(ref) == n
        pltpu.make_async_copy(ref, ref, sem).wait()

    def remote(key, src, dst, who):
        name, box = together(key), outbox(key)
        i = recv_of.setdefault(name, len(recv_of))
        recv_bytes[name] = recv_bytes.get(name, 0) + size(dst)
        send_bytes[box] = send_bytes.get(box, 0) + size(src)
        pltpu.make_async_remote_copy(
            src_ref=src, dst_ref=dst, send_sem=send_sem.at[box], recv_sem=recv_sem.at[i],
            device_id=who, device_id_type=MESH,
        ).start()

    def need(*names):
        for name in names:
            if name in recv_bytes:
                wait_for(recv_sem.at[recv_of[name]], recv_bytes.pop(name))

    def drain(*boxes):
        for box in boxes:
            wait_for(send_sem.at[box], send_bytes.pop(box))

    near = [back(g) for g in BATCHES[0] + BATCHES[1] if g > 0]
    far = [back(g) for g in BATCHES[2]]
    with jax.named_scope("pick"):
        loaded("sel")
        row_id = lax.broadcasted_iota(jnp.int32, (n_slots, tok_dev), 0)
        lane_id = lax.broadcasted_iota(jnp.int32, (n_slots, tok_dev), 1)
        idx = jnp.full((n_slots, tok_dev), -1, jnp.int32)
        for g in range(groups):
            e = expert_at(g)
            for j in range(slot):
                idx = jnp.where(row_id == g * slot + j, sel_ref[j, e], idx)
        onehot = jnp.where(lane_id == idx, 1.0, 0.0).astype(BF16)
    for i in range(4):
        with jax.named_scope("tok"):
            loaded(i)
        with jax.named_scope("sel"):
            cols = slice(i * tokw, (i + 1) * tokw)
            slots32[:, cols] = jnp.dot(onehot, tok_v[:, cols], preferred_element_type=F32)
            for g in near:
                send4[g, :, cols] = slots32[g * slot : (g + 1) * slot, cols].astype(BF16)
    with jax.named_scope("barrier"):
        pl.semaphore_wait(barrier, len(partners))
    for g in near:
        remote(("in", back(g)), send4.at[g], recv4.at[back(g)], at_group(g))
    for g in far:
        send4[g] = slots32[g * slot : (g + 1) * slot, :].astype(BF16)
        remote(("in", back(g)), send4.at[g], recv4.at[back(g)], at_group(g))
    recv4[0] = slots32[0:slot, :].astype(BF16)
    loaded("gate")

    lane8 = lax.broadcasted_iota(jnp.int32, (8, 128), 1)
    idx_l = jnp.full((8, 128), -1, jnp.int32)
    gate_l = jnp.zeros((8, 128), F32)
    for g in range(groups):
        e = expert_at(g)
        for j in range(slot):
            here = lane8 % n_slots == g * slot + j
            idx_l = jnp.where(here, sel_ref[j, e], idx_l)
            gate_l = jnp.where(here, gate_ref[j, e], gate_l)
    g1 = gate_l.astype(BF16).astype(F32)
    rest = gate_l - g1
    g2 = rest.astype(BF16).astype(F32)
    g3 = (rest - g2).astype(BF16).astype(F32)
    term = lane8 // n_slots
    gate3 = jnp.where(term == 0, g1, jnp.where(term == 1, g2, jnp.where(term == 2, g3, 0.0)))
    tok_id = lax.broadcasted_iota(jnp.int32, (tok_dev, 128), 0)
    hit = tok_id == idx_l[0:1, :]
    comb_ref[...] = jnp.where(hit, gate3[0:1, :], 0.0).astype(BF16)

    def cut(p, lo=0, n=halfw):
        return pl.ds(p * halfw + lo, n)

    def pos(p, d1, d2):
        d1, d2 = d1 % RING, d2 % RING
        return PLACE[(d2, d1) if p == 0 else (d1, d2)]

    def first(p, step):
        return at_x(step) if p == 0 else at_z(step)

    def second(p, step):
        return at_z(step) if p == 0 else at_x(step)

    def own(h):
        need(("own", h))
        for i, g in enumerate(BATCHES[h]):
            slots32[i * slot : (i + 1) * slot, :] = recv4[g].astype(F32)
        rows[h][0] = slots32[0 : chunk[h], :].astype(BF16)

    def to_first(key, h, p, d1, step, lo, n):
        remote(
            key, rows[h].at[pos(p, d1, 0), :, cut(p, lo, n)],
            rows[h].at[pos(p, d1 - step, 0), :, cut(p, lo, n)], first(p, step),
        )

    def to_second(key, h, p, d1, d2, step):
        remote(
            key, rows[h].at[pos(p, d1, d2), :, cut(p)],
            rows[h].at[pos(p, d1, d2 - step), :, cut(p)], second(p, step),
        )

    def send_first(h, p, step):
        to_first(("f", h, p, step), h, p, 0, step, 0, halfw)

    def pass_first(h, p, step):
        need(("f", h, p, step))
        to_first(("r", h, p, step), h, p, -step, step, 0 if step == 1 else quart, quart)

    def send_second(h, p, d1, step):
        if d1 == 2:
            need(("r", h, p))
        elif d1 != 0:
            need(("f", h, p, 1 if d1 == 3 else -1))
        to_second(("s", h, p, d1, step), h, p, d1, 0, step)

    def pass_second(h, p, d1):
        step = 1 if d1 in RSET else -1
        need(("s", h, p, d1, step))
        to_second(("t", h, p, d1), h, p, d1, -step, step)

    tn = hid[0].shape[1] // 2
    places = (slice(0, len(EARLY)), slice(len(EARLY), RING * RING), slice(0, RING * RING))

    def held(h, b):
        return slice(places[b].start * chunk[h], places[b].stop * chunk[h])

    def up(h, b, n):
        for p in range(2):
            if b >= 1:
                need(("r", h, p))
            for step in (1, -1):
                need(("f", h, p, step))
                for d1 in RSET if step == 1 else LSET:
                    if b >= 1 or d1 != 2:
                        need(("s", h, p, d1, step))
        need(("up", h, b))
        loaded("wg", "wu")
        lhs = rows[h][places[b]].reshape(-1, width)
        cols = slice(n * tn, (n + 1) * tn)
        gate_val = jnp.dot(lhs, wg_v[:, cols], preferred_element_type=F32)
        up_val = jnp.dot(lhs, wu_v[:, cols], preferred_element_type=F32)
        hid[h][held(h, b), cols] = (gate_val / (1.0 + jnp.exp(-gate_val)) * up_val).astype(BF16)

    dn = 512

    def down(h, b, p, i):
        loaded("wd")
        start = p * halfw + i * subw[h]
        for c in range(start, start + subw[h], dn):
            cols = slice(c, c + dn)
            val = jnp.dot(hid[h][held(h, b), :], wd_v[:, cols], preferred_element_type=F32)
            part[h][places[b], :, cols] = val.astype(BF16).reshape(-1, chunk[h], dn)

    def sub(h, i, lo=0, n=None):
        return pl.ds(i * subw[h] + lo, subw[h] if n is None else n)

    def psub(h, p, i):
        return cut(p, i * subw[h], subw[h])

    def send_far(h, p, d1, i):
        step = 1 if d1 in RSET else -1
        remote(
            ("F", h, p, d1, i), part[h].at[pos(p, d1, 2), :, psub(h, p, i)],
            relay[h].at[p, d1, :, sub(h, i)], second(p, step),
        )

    def send_left_of(h, p, d1, i):
        remote(
            ("L", h, p, d1, i), part[h].at[pos(p, d1, 1), :, psub(h, p, i)],
            fin_l[h].at[p, d1, :, sub(h, i)], second(p, 1),
        )

    def send_right_of(h, p, d1, i):
        remote(
            ("R", h, p, d1, i), part[h].at[pos(p, d1, 3), :, psub(h, p, i)],
            fin_r[h].at[p, d1, :, sub(h, i)], second(p, -1),
        )

    def add_far(h, p, d1, i):
        need(("F", h, p, d1, i))
        right = d1 in RSET
        mine = part[h][pos(p, d1, 1 if right else 3), :, psub(h, p, i)]
        here = relay[h].at[p, d1, :, sub(h, i)]
        here[...] = (here[...].astype(F32) + mine.astype(F32)).astype(BF16)
        if right:
            remote(("L", h, p, d1, i), here, fin_l[h].at[p, d1, :, sub(h, i)], second(p, 1))
        else:
            remote(("R", h, p, d1, i), here, fin_r[h].at[p, d1, :, sub(h, i)], second(p, -1))

    def add_up(h, p, d1, i):
        need(("S", h, p, d1, i))
        mine = part[h][pos(p, d1, 0), :, psub(h, p, i)]
        total = (
            mine.astype(F32)
            + fin_l[h][p, d1, :, sub(h, i)].astype(F32)
            + fin_r[h][p, d1, :, sub(h, i)].astype(F32)
        )
        summed[h][p, d1, :, sub(h, i)] = total.astype(BF16)
        lo, hi = sub(h, i, 0, subw[h] // 2), sub(h, i, subw[h] // 2, subw[h] // 2)
        if h in DIRECT:
            if d1 != 0:
                name, dst, step = {2: ("F1", relay1, 2), 1: ("l1", fin1_l, 1), 3: ("r1", fin1_r, -1)}[d1]
                remote(
                    (name, h, p, i), summed[h].at[p, d1, :, sub(h, i)], dst[h].at[p, :, sub(h, i)],
                    first(p, step),
                )
            return
        if d1 == 2:
            remote(("F1", h, p, 1, i), summed[h].at[p, 2, :, lo], relay1[h].at[p, :, lo], first(p, 1))
            remote(("F1", h, p, -1, i), summed[h].at[p, 2, :, hi], relay1[h].at[p, :, hi], first(p, -1))
        elif d1 == 1:
            remote(("l1", h, p, i), summed[h].at[p, 1, :, hi], fin1_l[h].at[p, :, hi], first(p, 1))
        elif d1 == 3:
            remote(("r1", h, p, i), summed[h].at[p, 3, :, lo], fin1_r[h].at[p, :, lo], first(p, -1))

    def add_first(h, p, step, i):
        need(("F1", h, p, step, i))
        d1 = 1 if step == 1 else 3
        cols = sub(h, i, 0 if step == 1 else subw[h] // 2, subw[h] // 2)
        here = relay1[h].at[p, :, cols]
        here[...] = (here[...].astype(F32) + summed[h][p, d1, :, cols].astype(F32)).astype(BF16)
        dst = fin1_l if step == 1 else fin1_r
        remote(("b", h, p, step, i), here, dst[h].at[p, :, cols], first(p, step))

    def finish(h, p, i):
        need(("Z", h, p, i))
        total = (
            summed[h][p, 0, :, sub(h, i)].astype(F32)
            + fin1_l[h][p, :, sub(h, i)].astype(F32)
            + fin1_r[h][p, :, sub(h, i)].astype(F32)
        )
        if h in DIRECT:
            total += relay1[h][p, :, sub(h, i)].astype(F32)
        slots32[0 : chunk[h], psub(h, p, i)] = total
        for r, g in enumerate(BATCHES[h]):
            value = slots32[r * slot : (r + 1) * slot, psub(h, p, i)].astype(BF16)
            if g == 0:
                ret4[0, :, psub(h, p, i)] = value
            else:
                exit4[g, :, psub(h, p, i)] = value
                remote(
                    ("X", h, p, i, back(g)), exit4.at[g, :, psub(h, p, i)],
                    ret4.at[back(g), :, psub(h, p, i)], at_group(g),
                )

    def take(h, p, i):
        need(("X", h, p, i))
        for g in BATCHES[h]:
            slots_ref[g * slot : (g + 1) * slot, psub(h, p, i)] = ret4[g, :, psub(h, p, i)].astype(F32)

    steps = {
        "own": own, "f": send_first, "r": pass_first, "s": send_second, "t": pass_second,
        "up": up, "down": down, "F": send_far, "L": send_left_of, "R": send_right_of,
        "A": add_far, "S": add_up, "B": add_first, "Z": finish, "X": take,
    }
    ends = [i for i, entry in enumerate(ORDER) if entry[0] == "Z"]
    for at, (name, *args) in enumerate(ORDER):
        with jax.named_scope("_".join(str(a) for a in (name, *args))):
            steps[name](*args)
        if at == ends[-1]:
            with jax.named_scope("drain"):
                drain(*range(9))
    assert len(recv_of) == N_RECV, len(recv_of)
    with jax.named_scope("last_sends"):
        drain(9)


def combine_kernel(slots_ref, comb_ref, out_ref, out_v, out_sem):
    width = slots_ref.shape[1]
    n = 1024
    stores = []
    for k, c in enumerate(range(0, width, n)):
        value = slots_ref[:, c : c + n].astype(BF16)
        stack = jnp.concatenate([value, value, value, jnp.zeros_like(value)], axis=0)
        out_v[:, c : c + n] = jnp.dot(
            comb_ref[...], stack, preferred_element_type=F32).astype(BF16)
        store = pltpu.make_async_copy(
            out_v.at[:, pl.ds(c, n)], out_ref.at[:, pl.ds(c, n)], out_sem.at[k])
        store.start()
        stores.append(store)
    for store in stores:
        store.wait()


def per_device(tokens, select, gates, w_gate, w_up, w_down):
    tok_dev, width = tokens.shape
    slot = select.shape[1]
    ff = w_gate.shape[2]
    halfw = width // 2

    def vmems(shape):
        return [pltpu.VMEM(shape(slot * len(batch)), BF16) for batch in BATCHES]

    vmem, hbm = pl.BlockSpec(memory_space=pltpu.VMEM), pl.BlockSpec(memory_space=pltpu.HBM)
    slots, comb = pl.pallas_call(
        kernel,
        out_shape=(pltpu.VMEM((8 * slot, width), F32), pltpu.VMEM((tok_dev, 128), BF16)),
        in_specs=[hbm] * 6,
        out_specs=(vmem, vmem),
        scratch_shapes=[
            pltpu.SMEM((slot, 8), jnp.int32),
            pltpu.SMEM((slot, 8), F32),
            pltpu.VMEM((tok_dev, width), BF16),
            pltpu.VMEM((width, ff), BF16),
            pltpu.VMEM((width, ff), BF16),
            pltpu.VMEM((ff, width), BF16),
            pltpu.VMEM((8, slot, width), BF16),
            pltpu.VMEM((8, slot, width), BF16),
            pltpu.VMEM((8, slot, width), BF16),
            pltpu.VMEM((8, slot, width), BF16),
            vmems(lambda c: (16, c, width)),
            vmems(lambda c: (16, c, width)),
            vmems(lambda c: (16 * c, ff)),
            vmems(lambda c: (2, 4, c, halfw)),
            vmems(lambda c: (2, 4, c, halfw)),
            vmems(lambda c: (2, 4, c, halfw)),
            vmems(lambda c: (2, 4, c, halfw)),
            vmems(lambda c: (2, c, halfw)),
            vmems(lambda c: (2, c, halfw)),
            vmems(lambda c: (2, c, halfw)),
            pltpu.VMEM((8 * slot, width), F32),
            pltpu.SemaphoreType.DMA((10,)),
            pltpu.SemaphoreType.DMA((N_RECV,)),
            pltpu.SemaphoreType.DMA((9,)),
        ],
        compiler_params=pltpu.CompilerParams(
            collective_id=0, has_side_effects=True, vmem_limit_bytes=56 * 1024 * 1024
        ),
        name="moe",
    )(
        select.T, gates.T, tokens, w_gate[0], w_up[0], w_down[0],
    )
    return pl.pallas_call(
        combine_kernel,
        out_shape=jax.ShapeDtypeStruct((tok_dev, width), BF16),
        in_specs=[vmem, vmem],
        out_specs=hbm,
        scratch_shapes=[pltpu.VMEM((tok_dev, width), BF16), pltpu.SemaphoreType.DMA((4,))],
        compiler_params=pltpu.CompilerParams(vmem_limit_bytes=8 * 1024 * 1024),
        name="combine",
    )(slots, comb)


def solution(mesh):
    return jax.shard_map(
        per_device,
        mesh=mesh,
        in_specs=(
            P(("dp", "expert"), None),
            P(None, ("dp", "expert")),
            P(None, ("dp", "expert")),
            P("expert", None, "dp"),
            P("expert", None, "dp"),
            P("expert", "dp", None),
        ),
        out_specs=P(("dp", "expert"), None),
        check_vma=False,
    )
```

```python
import jax
import jax.numpy as jnp
from jax import lax
from jax.experimental import pallas as pl
from jax.experimental.pallas import tpu as pltpu
from jax.sharding import PartitionSpec as P

MESH = pl.DeviceIdType.MESH
BF16, F32 = jnp.bfloat16, jnp.float32
RING = 4
N_RECV = 137
DIRECT = (0, 2)
RSET, LSET = (0, 3), (2, 1)
ROUND = tuple((z, x) for z in range(RING) for x in range(RING))
EARLY = tuple(at for at in ROUND if 2 not in at and at != (1, 3))
LATE = tuple(at for at in ROUND if at not in EARLY)
PLACE = {at: i for i, at in enumerate(EARLY + LATE)}
BATCHES = ((0, 1), (2, 6, 3, 7), (4, 5))
SUBS = (1, 2, 1)
SPLIT = (1,)

ORDER = (
    ("own", 0), ("f", 0, 0, 1), ("f", 0, 1, -1), ("f", 0, 1, 1), ("f", 0, 0, -1), ("s", 0, 1, 0, -1),
    ("s", 0, 0, 0, -1), ("s", 0, 1, 0, 1), ("s", 0, 0, 0, 1), ("r", 0, 0, 1), ("r", 0, 1, -1), ("s", 0, 0, 3, -1),
    ("r", 0, 1, 1), ("r", 0, 0, -1), ("s", 0, 0, 1, -1), ("s", 0, 1, 3, 1), ("s", 0, 0, 1, 1), ("s", 0, 1, 1, 1),
    ("s", 0, 1, 3, -1), ("s", 0, 1, 1, -1), ("own", 1), ("f", 1, 0, 1), ("f", 1, 1, 1), ("f", 1, 0, -1),
    ("f", 1, 1, -1), ("s", 1, 1, 0, -1), ("s", 1, 0, 0, 1), ("s", 1, 0, 0, -1), ("s", 0, 0, 3, 1), ("s", 1, 1, 0, 1),
    ("t", 0, 1, 0), ("t", 0, 0, 0), ("own", 2), ("f", 2, 1, 1), ("f", 2, 0, 1), ("s", 2, 1, 0, 1), ("s", 2, 0, 0, 1),
    ("f", 2, 0, -1), ("f", 2, 1, -1), ("s", 2, 0, 0, -1), ("s", 0, 1, 2, -1), ("s", 0, 0, 2, -1), ("s", 0, 0, 2, 1),
    ("s", 0, 1, 2, 1), ("t", 0, 1, 3), ("t", 0, 0, 1), ("t", 0, 1, 1), ("r", 1, 1, 1), ("s", 1, 1, 3, 1),
    ("s", 1, 0, 3, -1), ("r", 1, 0, 1), ("s", 1, 1, 1, -1), ("s", 1, 0, 3, 1), ("s", 1, 0, 1, -1), ("r", 1, 0, -1),
    ("s", 1, 0, 1, 1), ("t", 1, 0, 0), ("s", 1, 1, 1, 1), ("t", 1, 1, 0), ("t", 0, 0, 3), ("r", 1, 1, -1),
    ("r", 2, 1, -1), ("s", 2, 1, 1, 1), ("s", 2, 1, 1, -1), ("r", 2, 0, -1), ("s", 2, 0, 1, -1), ("s", 2, 0, 1, 1),
    ("s", 1, 1, 3, -1), ("r", 2, 0, 1), ("s", 2, 0, 3, -1), ("s", 2, 1, 3, -1), ("t", 0, 1, 2), ("r", 2, 1, 1),
    ("s", 2, 0, 3, 1), ("t", 2, 1, 0), ("t", 0, 0, 2), ("t", 2, 0, 0), ("s", 2, 1, 0, -1), ("t", 1, 1, 3),
    ("t", 1, 0, 3), ("t", 2, 1, 1), ("s", 1, 0, 2, 1), ("s", 1, 0, 2, -1), ("t", 1, 0, 1), ("s", 1, 1, 2, -1),
    ("s", 2, 1, 3, 1), ("s", 1, 1, 2, 1), ("t", 1, 1, 1), ("up", 1, 0, 0), ("t", 2, 0, 1), ("up", 1, 0, 1),
    ("down", 1, 0, 1, 1), ("up", 0, 2, 0), ("s", 2, 1, 2, 1), ("s", 2, 1, 2, -1), ("s", 2, 0, 2, -1), ("up", 0, 2, 1),
    ("t", 2, 0, 3), ("t", 1, 0, 2), ("down", 0, 2, 0, 0), ("t", 1, 1, 2), ("L", 0, 0, 1, 0), ("F", 0, 0, 3, 0),
    ("R", 0, 0, 0, 0), ("F", 0, 0, 2, 0), ("down", 1, 0, 0, 1), ("L", 1, 0, 1, 1), ("R", 1, 0, 0, 1),
    ("s", 2, 0, 2, 1), ("F", 0, 0, 1, 0), ("down", 0, 2, 1, 0), ("F", 0, 1, 0, 0), ("R", 0, 1, 0, 0),
    ("F", 0, 1, 2, 0), ("F", 0, 1, 3, 0), ("L", 0, 1, 1, 0), ("down", 1, 0, 0, 0), ("L", 1, 0, 1, 0), ("t", 2, 1, 3),
    ("F", 0, 0, 0, 0), ("L", 0, 0, 2, 0), ("R", 1, 0, 0, 0), ("L", 1, 1, 1, 1), ("down", 1, 0, 1, 0),
    ("R", 1, 1, 0, 0), ("L", 1, 1, 1, 0), ("R", 0, 1, 3, 0), ("R", 1, 0, 3, 1), ("R", 1, 1, 3, 1), ("L", 0, 1, 2, 0),
    ("t", 2, 1, 2), ("t", 2, 0, 2), ("R", 1, 0, 3, 0), ("F", 0, 1, 1, 0), ("R", 0, 0, 3, 0), ("R", 1, 1, 3, 0),
    ("up", 1, 1, 0), ("A", 0, 0, 3, 0), ("up", 1, 1, 1), ("down", 1, 1, 1, 1), ("F", 1, 1, 3, 1),
    ("down", 1, 1, 1, 0), ("F", 1, 1, 3, 0), ("down", 1, 1, 0, 0), ("F", 1, 0, 3, 0), ("down", 1, 1, 0, 1),
    ("F", 1, 0, 2, 1), ("L", 1, 1, 2, 1), ("F", 1, 0, 0, 0), ("F", 1, 1, 1, 0), ("F", 1, 1, 0, 1), ("F", 1, 1, 1, 1),
    ("L", 1, 0, 2, 0), ("F", 1, 0, 3, 1), ("L", 1, 1, 2, 0), ("F", 1, 0, 1, 1), ("F", 1, 0, 2, 0), ("F", 1, 0, 1, 0),
    ("F", 1, 1, 2, 0), ("F", 1, 1, 2, 1), ("L", 1, 0, 2, 1), ("A", 0, 1, 0, 0), ("F", 1, 0, 0, 1), ("up", 2, 2, 0),
    ("up", 2, 2, 1), ("A", 0, 1, 1, 0), ("down", 2, 2, 1, 0), ("F", 2, 1, 3, 0), ("F", 2, 1, 2, 0), ("R", 2, 1, 0, 0),
    ("L", 2, 1, 1, 0), ("A", 1, 0, 2, 1), ("A", 1, 0, 3, 0), ("down", 2, 2, 0, 0), ("F", 2, 0, 2, 0),
    ("F", 2, 0, 1, 0), ("A", 1, 0, 1, 1), ("R", 2, 0, 3, 0), ("R", 2, 0, 0, 0), ("A", 1, 0, 0, 0), ("F", 2, 0, 3, 0),
    ("F", 2, 0, 0, 0), ("F", 2, 1, 0, 0), ("L", 2, 0, 1, 0), ("L", 2, 1, 2, 0), ("F", 2, 1, 1, 0), ("L", 2, 0, 2, 0),
    ("R", 2, 1, 3, 0), ("A", 1, 1, 0, 1), ("A", 0, 1, 3, 0), ("A", 1, 0, 2, 0), ("A", 1, 1, 2, 0), ("A", 1, 0, 3, 1),
    ("A", 1, 1, 2, 1), ("S", 0, 1, 1, 0), ("A", 1, 1, 3, 1), ("A", 1, 0, 0, 1), ("A", 2, 1, 3, 0), ("S", 1, 0, 2, 1),
    ("A", 2, 1, 2, 0), ("S", 1, 0, 3, 0), ("A", 2, 0, 2, 0), ("S", 1, 0, 0, 0), ("A", 2, 1, 0, 0), ("A", 2, 0, 1, 0),
    ("A", 2, 1, 1, 0), ("A", 1, 1, 1, 0), ("A", 2, 0, 3, 0), ("A", 1, 1, 1, 1), ("S", 1, 0, 1, 1), ("A", 1, 1, 3, 0),
    ("F", 1, 1, 0, 0), ("A", 2, 0, 0, 0), ("A", 1, 0, 1, 0), ("S", 1, 1, 2, 0), ("A", 0, 1, 2, 0), ("S", 1, 1, 2, 1),
    ("S", 1, 1, 3, 1), ("S", 1, 0, 2, 0), ("S", 1, 0, 3, 1), ("S", 2, 1, 2, 0), ("B", 1, 0, -1, 1), ("S", 2, 1, 3, 0),
    ("S", 2, 0, 2, 0), ("B", 1, 0, 1, 1), ("A", 0, 0, 2, 0), ("S", 2, 0, 1, 0), ("S", 2, 1, 1, 0), ("A", 0, 0, 1, 0),
    ("S", 2, 1, 0, 0), ("S", 1, 0, 0, 1), ("S", 1, 0, 1, 0), ("S", 1, 1, 1, 0), ("S", 2, 0, 3, 0), ("S", 1, 1, 3, 0),
    ("B", 1, 1, -1, 0), ("B", 1, 1, -1, 1), ("S", 1, 1, 1, 1), ("R", 1, 1, 0, 1), ("S", 2, 0, 0, 0),
    ("A", 1, 1, 0, 0), ("B", 1, 1, 1, 0), ("S", 0, 1, 2, 0), ("B", 1, 0, 1, 0), ("B", 1, 1, 1, 1), ("B", 1, 0, -1, 0),
    ("A", 0, 0, 0, 0), ("S", 0, 0, 3, 0), ("S", 0, 1, 3, 0), ("Z", 1, 0, 1), ("S", 0, 0, 2, 0), ("Z", 2, 1, 0),
    ("S", 0, 0, 1, 0), ("Z", 2, 0, 0), ("S", 1, 1, 0, 1), ("S", 1, 1, 0, 0), ("Z", 1, 1, 0), ("Z", 1, 0, 0),
    ("Z", 1, 1, 1), ("S", 0, 1, 0, 0), ("S", 0, 0, 0, 0), ("Z", 0, 1, 0), ("X", 1, 0, 1), ("Z", 0, 0, 0),
    ("X", 2, 1, 0), ("X", 0, 1, 0), ("X", 1, 1, 0), ("X", 2, 0, 0), ("X", 1, 0, 0), ("X", 0, 0, 0), ("X", 1, 1, 1),
)


def kernel(
    sel_hbm, gate_hbm, tok_ref, wg_ref, wu_ref, wd_ref, slots_ref, comb_ref,
    sel_ref, gate_ref, tok_v, wg_v, wu_v, wd_v, send4, recv4, exit4, ret4, rows, part, hid, relay, fin_l, fin_r,
    summed, relay1, fin1_l, fin1_r, slots32, send_sem, recv_sem, load_sem,
):
    slot = sel_hbm.shape[0]
    tok_dev, width = tok_ref.shape
    groups = 2 * RING
    n_slots = groups * slot
    halfw = width // 2
    quart = width // 4
    subw = [halfw // n for n in SUBS]
    chunk = [r.shape[1] for r in rows]
    batch_of = {g: h for h, batch in enumerate(BATCHES) for g in batch}

    dp = lax.axis_index("dp")
    ex = lax.axis_index("expert")
    my_x, my_z = dp // RING, dp % RING
    my_y, my_c = ex // 2, ex % 2

    def at_x(step):
        return (((my_x + step + RING) % RING) * RING + my_z, ex)

    def at_z(step):
        return (my_x * RING + (my_z + step + RING) % RING, ex)

    def expert_at(g):
        return ((my_y + g // 2) % RING) * 2 + (my_c + g % 2) % 2

    def at_group(g):
        return (dp, expert_at(g))

    def back(g):
        return ((RING - g // 2) % RING) * 2 + g % 2

    barrier = pltpu.get_barrier_semaphore()
    partners = [at(step) for at in (at_x, at_z) for step in (1, -1, 2)] + [at_group(g) for g in range(1, groups)]
    for who in partners:
        pl.semaphore_signal(barrier, inc=1, device_id=who, device_id_type=MESH)

    loads = {}
    loads["sel"] = pltpu.make_async_copy(sel_hbm, sel_ref, load_sem.at[7])
    loads["gate"] = pltpu.make_async_copy(gate_hbm, gate_ref, load_sem.at[8])
    loads["sel"].start()
    tokw = width // 4
    for i in range(4):
        cols = pl.ds(i * tokw, tokw)
        loads[i] = pltpu.make_async_copy(tok_ref.at[:, cols], tok_v.at[:, cols], load_sem.at[i])
        loads[i].start()
    for i, (name, src, dst) in enumerate(
        (("wg", wg_ref, wg_v), ("wu", wu_ref, wu_v), ("wd", wd_ref, wd_v)), 4
    ):
        loads[name] = pltpu.make_async_copy(src, dst, load_sem.at[i])
        loads[name].start()

    loads["gate"].start()

    def loaded(*names):
        for name in names:
            if name in loads:
                loads.pop(name).wait()

    recv_of, recv_bytes, send_bytes = {}, {}, {}

    def together(key):
        kind, h = key[0], key[1]
        if kind == "in":
            return ("own", batch_of[h])
        if kind == "r":
            return key[:3]
        if kind == "t":
            return ("up", h, 1 if h in SPLIT else 2)
        if kind == "s" and key[4] != (1 if key[3] in RSET else -1):
            return ("up", h, int(key[3] == 2) if h in SPLIT else 2)
        if kind in ("L", "R"):
            return ("S", *key[1:])
        if kind in ("l1", "r1") or (kind == "F1" and h in DIRECT):
            return ("Z", *key[1:])
        if kind == "b":
            return ("Z", h, key[2], key[4])
        return key[:4] if kind == "X" else key

    def outbox(key):
        kind, h = key[0], key[1]
        if kind == "in":
            return 0
        return (1 if kind in "fsrt" else 4 if kind != "X" else 7) + h

    def size(ref):
        n = 2
        for dim in ref.shape:
            n *= dim
        return n

    def wait_for(sem, n):
        unit = 2 * slot * width
        if n % (4 * unit) == 0:
            ref = rows[1].at[pl.ds(0, n // (4 * unit))]
        elif n % (2 * unit) == 0 and n > 8 * unit:
            ref = rows[0].at[pl.ds(0, n // (2 * unit))]
        elif n % unit == 0:
            ref = exit4.at[pl.ds(0, n // unit)]
        else:
            ref = exit4.at[pl.ds(0, 2 * n // unit), :, pl.ds(0, halfw)]
        assert size(ref) == n
        pltpu.make_async_copy(ref, ref, sem).wait()

    def remote(key, src, dst, who):
        name, box = together(key), outbox(key)
        i = recv_of.setdefault(name, len(recv_of))
        recv_bytes[name] = recv_bytes.get(name, 0) + size(dst)
        send_bytes[box] = send_bytes.get(box, 0) + size(src)
        pltpu.make_async_remote_copy(
            src_ref=src, dst_ref=dst, send_sem=send_sem.at[box], recv_sem=recv_sem.at[i],
            device_id=who, device_id_type=MESH,
        ).start()

    def need(*names):
        for name in names:
            if name in recv_bytes:
                wait_for(recv_sem.at[recv_of[name]], recv_bytes.pop(name))

    def drain(*boxes):
        for box in boxes:
            wait_for(send_sem.at[box], send_bytes.pop(box))

    near = [back(g) for g in BATCHES[0] + BATCHES[1] if g > 0]
    far = [back(g) for g in BATCHES[2]]
    with jax.named_scope("pick"):
        loaded("sel")
        row_id = lax.broadcasted_iota(jnp.int32, (n_slots, tok_dev), 0)
        lane_id = lax.broadcasted_iota(jnp.int32, (n_slots, tok_dev), 1)
        idx = jnp.full((n_slots, tok_dev), -1, jnp.int32)
        for g in range(groups):
            e = expert_at(g)
            for j in range(slot):
                idx = jnp.where(row_id == g * slot + j, sel_ref[j, e], idx)
        onehot = jnp.where(lane_id == idx, 1.0, 0.0).astype(BF16)
    for i in range(4):
        with jax.named_scope("tok"):
            loaded(i)
        with jax.named_scope("sel"):
            cols = slice(i * tokw, (i + 1) * tokw)
            slots32[:, cols] = jnp.dot(onehot, tok_v[:, cols], preferred_element_type=F32)
            for g in near:
                send4[g, :, cols] = slots32[g * slot : (g + 1) * slot, cols].astype(BF16)
    with jax.named_scope("barrier"):
        pl.semaphore_wait(barrier, len(partners))
    for g in near:
        remote(("in", back(g)), send4.at[g], recv4.at[back(g)], at_group(g))
    for g in far:
        send4[g] = slots32[g * slot : (g + 1) * slot, :].astype(BF16)
        remote(("in", back(g)), send4.at[g], recv4.at[back(g)], at_group(g))
    recv4[0] = slots32[0:slot, :].astype(BF16)
    loaded("gate")

    lane8 = lax.broadcasted_iota(jnp.int32, (8, 128), 1)
    idx_l = jnp.full((8, 128), -1, jnp.int32)
    gate_l = jnp.zeros((8, 128), F32)
    for g in range(groups):
        e = expert_at(g)
        for j in range(slot):
            here = lane8 % n_slots == g * slot + j
            idx_l = jnp.where(here, sel_ref[j, e], idx_l)
            gate_l = jnp.where(here, gate_ref[j, e], gate_l)
    g1 = gate_l.astype(BF16).astype(F32)
    rest = gate_l - g1
    g2 = rest.astype(BF16).astype(F32)
    g3 = (rest - g2).astype(BF16).astype(F32)
    term = lane8 // n_slots
    gate3 = jnp.where(term == 0, g1, jnp.where(term == 1, g2, jnp.where(term == 2, g3, 0.0)))
    tok_id = lax.broadcasted_iota(jnp.int32, (tok_dev, 128), 0)
    hit = tok_id == idx_l[0:1, :]
    comb_ref[...] = jnp.where(hit, gate3[0:1, :], 0.0).astype(BF16)

    def cut(p, lo=0, n=halfw):
        return pl.ds(p * halfw + lo, n)

    def pos(p, d1, d2):
        d1, d2 = d1 % RING, d2 % RING
        return PLACE[(d2, d1) if p == 0 else (d1, d2)]

    def first(p, step):
        return at_x(step) if p == 0 else at_z(step)

    def second(p, step):
        return at_z(step) if p == 0 else at_x(step)

    def own(h):
        need(("own", h))
        for i, g in enumerate(BATCHES[h]):
            slots32[i * slot : (i + 1) * slot, :] = recv4[g].astype(F32)
        rows[h][0] = slots32[0 : chunk[h], :].astype(BF16)

    def to_first(key, h, p, d1, step, lo, n):
        remote(
            key, rows[h].at[pos(p, d1, 0), :, cut(p, lo, n)],
            rows[h].at[pos(p, d1 - step, 0), :, cut(p, lo, n)], first(p, step),
        )

    def to_second(key, h, p, d1, d2, step):
        remote(
            key, rows[h].at[pos(p, d1, d2), :, cut(p)],
            rows[h].at[pos(p, d1, d2 - step), :, cut(p)], second(p, step),
        )

    def send_first(h, p, step):
        to_first(("f", h, p, step), h, p, 0, step, 0, halfw)

    def pass_first(h, p, step):
        need(("f", h, p, step))
        to_first(("r", h, p, step), h, p, -step, step, 0 if step == 1 else quart, quart)

    def send_second(h, p, d1, step):
        if d1 == 2:
            need(("r", h, p))
        elif d1 != 0:
            need(("f", h, p, 1 if d1 == 3 else -1))
        to_second(("s", h, p, d1, step), h, p, d1, 0, step)

    def pass_second(h, p, d1):
        step = 1 if d1 in RSET else -1
        need(("s", h, p, d1, step))
        to_second(("t", h, p, d1), h, p, d1, -step, step)

    tn = hid[0].shape[1] // 2
    places = (slice(0, len(EARLY)), slice(len(EARLY), RING * RING), slice(0, RING * RING))

    def held(h, b):
        return slice(places[b].start * chunk[h], places[b].stop * chunk[h])

    def up(h, b, n):
        for p in range(2):
            if b >= 1:
                need(("r", h, p))
            for step in (1, -1):
                need(("f", h, p, step))
                for d1 in RSET if step == 1 else LSET:
                    if b >= 1 or d1 != 2:
                        need(("s", h, p, d1, step))
        need(("up", h, b))
        loaded("wg", "wu")
        lhs = rows[h][places[b]].reshape(-1, width)
        cols = slice(n * tn, (n + 1) * tn)
        gate_val = jnp.dot(lhs, wg_v[:, cols], preferred_element_type=F32)
        up_val = jnp.dot(lhs, wu_v[:, cols], preferred_element_type=F32)
        hid[h][held(h, b), cols] = (gate_val / (1.0 + jnp.exp(-gate_val)) * up_val).astype(BF16)

    dn = 512

    def down(h, b, p, i):
        loaded("wd")
        start = p * halfw + i * subw[h]
        for c in range(start, start + subw[h], dn):
            cols = slice(c, c + dn)
            val = jnp.dot(hid[h][held(h, b), :], wd_v[:, cols], preferred_element_type=F32)
            part[h][places[b], :, cols] = val.astype(BF16).reshape(-1, chunk[h], dn)

    def sub(h, i, lo=0, n=None):
        return pl.ds(i * subw[h] + lo, subw[h] if n is None else n)

    def psub(h, p, i):
        return cut(p, i * subw[h], subw[h])

    def send_far(h, p, d1, i):
        step = 1 if d1 in RSET else -1
        remote(
            ("F", h, p, d1, i), part[h].at[pos(p, d1, 2), :, psub(h, p, i)],
            relay[h].at[p, d1, :, sub(h, i)], second(p, step),
        )

    def send_left_of(h, p, d1, i):
        remote(
            ("L", h, p, d1, i), part[h].at[pos(p, d1, 1), :, psub(h, p, i)],
            fin_l[h].at[p, d1, :, sub(h, i)], second(p, 1),
        )

    def send_right_of(h, p, d1, i):
        remote(
            ("R", h, p, d1, i), part[h].at[pos(p, d1, 3), :, psub(h, p, i)],
            fin_r[h].at[p, d1, :, sub(h, i)], second(p, -1),
        )

    def add_far(h, p, d1, i):
        need(("F", h, p, d1, i))
        right = d1 in RSET
        mine = part[h][pos(p, d1, 1 if right else 3), :, psub(h, p, i)]
        here = relay[h].at[p, d1, :, sub(h, i)]
        here[...] = (here[...].astype(F32) + mine.astype(F32)).astype(BF16)
        if right:
            remote(("L", h, p, d1, i), here, fin_l[h].at[p, d1, :, sub(h, i)], second(p, 1))
        else:
            remote(("R", h, p, d1, i), here, fin_r[h].at[p, d1, :, sub(h, i)], second(p, -1))

    def add_up(h, p, d1, i):
        need(("S", h, p, d1, i))
        mine = part[h][pos(p, d1, 0), :, psub(h, p, i)]
        total = (
            mine.astype(F32)
            + fin_l[h][p, d1, :, sub(h, i)].astype(F32)
            + fin_r[h][p, d1, :, sub(h, i)].astype(F32)
        )
        summed[h][p, d1, :, sub(h, i)] = total.astype(BF16)
        lo, hi = sub(h, i, 0, subw[h] // 2), sub(h, i, subw[h] // 2, subw[h] // 2)
        if h in DIRECT:
            if d1 != 0:
                name, dst, step = {2: ("F1", relay1, 2), 1: ("l1", fin1_l, 1), 3: ("r1", fin1_r, -1)}[d1]
                remote(
                    (name, h, p, i), summed[h].at[p, d1, :, sub(h, i)], dst[h].at[p, :, sub(h, i)],
                    first(p, step),
                )
            return
        if d1 == 2:
            remote(("F1", h, p, 1, i), summed[h].at[p, 2, :, lo], relay1[h].at[p, :, lo], first(p, 1))
            remote(("F1", h, p, -1, i), summed[h].at[p, 2, :, hi], relay1[h].at[p, :, hi], first(p, -1))
        elif d1 == 1:
            remote(("l1", h, p, i), summed[h].at[p, 1, :, hi], fin1_l[h].at[p, :, hi], first(p, 1))
        elif d1 == 3:
            remote(("r1", h, p, i), summed[h].at[p, 3, :, lo], fin1_r[h].at[p, :, lo], first(p, -1))

    def add_first(h, p, step, i):
        need(("F1", h, p, step, i))
        d1 = 1 if step == 1 else 3
        cols = sub(h, i, 0 if step == 1 else subw[h] // 2, subw[h] // 2)
        here = relay1[h].at[p, :, cols]
        here[...] = (here[...].astype(F32) + summed[h][p, d1, :, cols].astype(F32)).astype(BF16)
        dst = fin1_l if step == 1 else fin1_r
        remote(("b", h, p, step, i), here, dst[h].at[p, :, cols], first(p, step))

    def finish(h, p, i):
        need(("Z", h, p, i))
        total = (
            summed[h][p, 0, :, sub(h, i)].astype(F32)
            + fin1_l[h][p, :, sub(h, i)].astype(F32)
            + fin1_r[h][p, :, sub(h, i)].astype(F32)
        )
        if h in DIRECT:
            total += relay1[h][p, :, sub(h, i)].astype(F32)
        slots32[0 : chunk[h], psub(h, p, i)] = total
        for r, g in enumerate(BATCHES[h]):
            value = slots32[r * slot : (r + 1) * slot, psub(h, p, i)].astype(BF16)
            if g == 0:
                ret4[0, :, psub(h, p, i)] = value
            else:
                exit4[g, :, psub(h, p, i)] = value
                remote(
                    ("X", h, p, i, back(g)), exit4.at[g, :, psub(h, p, i)],
                    ret4.at[back(g), :, psub(h, p, i)], at_group(g),
                )

    def take(h, p, i):
        need(("X", h, p, i))
        for g in BATCHES[h]:
            slots_ref[g * slot : (g + 1) * slot, psub(h, p, i)] = ret4[g, :, psub(h, p, i)].astype(F32)

    steps = {
        "own": own, "f": send_first, "r": pass_first, "s": send_second, "t": pass_second,
        "up": up, "down": down, "F": send_far, "L": send_left_of, "R": send_right_of,
        "A": add_far, "S": add_up, "B": add_first, "Z": finish, "X": take,
    }
    ends = [i for i, entry in enumerate(ORDER) if entry[0] == "Z"]
    for at, (name, *args) in enumerate(ORDER):
        with jax.named_scope("_".join(str(a) for a in (name, *args))):
            steps[name](*args)
        if at == ends[-1]:
            with jax.named_scope("drain"):
                drain(*range(9))
    assert len(recv_of) == N_RECV, len(recv_of)
    with jax.named_scope("last_sends"):
        drain(9)


def combine_kernel(slots_ref, comb_ref, out_ref, out_v, out_sem):
    width = slots_ref.shape[1]
    n = 1024
    stores = []
    for k, c in enumerate(range(0, width, n)):
        value = slots_ref[:, c : c + n].astype(BF16)
        stack = jnp.concatenate([value, value, value, jnp.zeros_like(value)], axis=0)
        out_v[:, c : c + n] = jnp.dot(
            comb_ref[...], stack, preferred_element_type=F32).astype(BF16)
        store = pltpu.make_async_copy(
            out_v.at[:, pl.ds(c, n)], out_ref.at[:, pl.ds(c, n)], out_sem.at[k])
        store.start()
        stores.append(store)
    for store in stores:
        store.wait()


def per_device(tokens, select, gates, w_gate, w_up, w_down):
    tok_dev, width = tokens.shape
    slot = select.shape[1]
    ff = w_gate.shape[2]
    halfw = width // 2

    def vmems(shape):
        return [pltpu.VMEM(shape(slot * len(batch)), BF16) for batch in BATCHES]

    vmem, hbm = pl.BlockSpec(memory_space=pltpu.VMEM), pl.BlockSpec(memory_space=pltpu.HBM)
    slots, comb = pl.pallas_call(
        kernel,
        out_shape=(pltpu.VMEM((8 * slot, width), F32), pltpu.VMEM((tok_dev, 128), BF16)),
        in_specs=[hbm] * 6,
        out_specs=(vmem, vmem),
        scratch_shapes=[
            pltpu.SMEM((slot, 8), jnp.int32),
            pltpu.SMEM((slot, 8), F32),
            pltpu.VMEM((tok_dev, width), BF16),
            pltpu.VMEM((width, ff), BF16),
            pltpu.VMEM((width, ff), BF16),
            pltpu.VMEM((ff, width), BF16),
            pltpu.VMEM((8, slot, width), BF16),
            pltpu.VMEM((8, slot, width), BF16),
            pltpu.VMEM((8, slot, width), BF16),
            pltpu.VMEM((8, slot, width), BF16),
            vmems(lambda c: (16, c, width)),
            vmems(lambda c: (16, c, width)),
            vmems(lambda c: (16 * c, ff)),
            vmems(lambda c: (2, 4, c, halfw)),
            vmems(lambda c: (2, 4, c, halfw)),
            vmems(lambda c: (2, 4, c, halfw)),
            vmems(lambda c: (2, 4, c, halfw)),
            vmems(lambda c: (2, c, halfw)),
            vmems(lambda c: (2, c, halfw)),
            vmems(lambda c: (2, c, halfw)),
            pltpu.VMEM((8 * slot, width), F32),
            pltpu.SemaphoreType.DMA((10,)),
            pltpu.SemaphoreType.DMA((N_RECV,)),
            pltpu.SemaphoreType.DMA((9,)),
        ],
        compiler_params=pltpu.CompilerParams(
            collective_id=0, has_side_effects=True, vmem_limit_bytes=56 * 1024 * 1024
        ),
        name="moe",
    )(
        select.T, gates.T, tokens, w_gate[0], w_up[0], w_down[0],
    )
    return pl.pallas_call(
        combine_kernel,
        out_shape=jax.ShapeDtypeStruct((tok_dev, width), BF16),
        in_specs=[vmem, vmem],
        out_specs=hbm,
        scratch_shapes=[pltpu.VMEM((tok_dev, width), BF16), pltpu.SemaphoreType.DMA((4,))],
        compiler_params=pltpu.CompilerParams(vmem_limit_bytes=8 * 1024 * 1024),
        name="combine",
    )(slots, comb)


def solution(mesh):
    return jax.shard_map(
        per_device,
        mesh=mesh,
        in_specs=(
            P(("dp", "expert"), None),
            P(None, ("dp", "expert")),
            P(None, ("dp", "expert")),
            P("expert", None, "dp"),
            P("expert", None, "dp"),
            P("expert", "dp", None),
        ),
        out_specs=P(("dp", "expert"), None),
        check_vma=False,
    )
```

```python
import jax
import jax.numpy as jnp
from jax import lax
from jax.experimental import pallas as pl
from jax.experimental.pallas import tpu as pltpu
from jax.sharding import PartitionSpec as P

MESH = pl.DeviceIdType.MESH
BF16, F32 = jnp.bfloat16, jnp.float32
RING = 4
N_RECV = 137
DIRECT = (0, 2)
RSET, LSET = (0, 3), (2, 1)
ROUND = tuple((z, x) for z in range(RING) for x in range(RING))
EARLY = tuple(at for at in ROUND if 2 not in at and at != (1, 3))
LATE = tuple(at for at in ROUND if at not in EARLY)
PLACE = {at: i for i, at in enumerate(EARLY + LATE)}
BATCHES = ((0, 1), (2, 6, 3, 7), (4, 5))
SUBS = (1, 2, 1)
SPLIT = (1,)

ORDER = (
    ("own", 0), ("f", 0, 1, -1), ("f", 0, 0, -1), ("f", 0, 1, 1), ("f", 0, 0, 1), ("s", 0, 1, 0, -1),
    ("s", 0, 0, 0, 1), ("s", 0, 0, 0, -1), ("s", 0, 1, 0, 1), ("r", 0, 1, -1), ("r", 0, 0, -1), ("r", 0, 1, 1),
    ("s", 0, 1, 3, -1), ("r", 0, 0, 1), ("s", 0, 0, 3, 1), ("s", 0, 1, 3, 1), ("s", 0, 0, 1, -1), ("own", 1),
    ("f", 1, 1, -1), ("f", 1, 1, 1), ("s", 1, 0, 0, 1), ("f", 1, 0, -1), ("f", 1, 0, 1), ("own", 2),
    ("s", 1, 0, 0, -1), ("s", 0, 1, 1, 1), ("f", 2, 1, -1), ("s", 2, 0, 0, 1), ("s", 0, 0, 1, 1), ("t", 0, 1, 0),
    ("s", 0, 1, 1, -1), ("f", 2, 0, -1), ("s", 0, 0, 2, -1), ("s", 0, 1, 2, -1), ("s", 1, 1, 0, -1), ("f", 2, 0, 1),
    ("t", 0, 0, 0), ("s", 0, 0, 3, -1), ("s", 1, 1, 0, 1), ("r", 1, 1, -1), ("f", 2, 1, 1), ("s", 2, 1, 0, 1),
    ("r", 1, 1, 1), ("s", 1, 0, 3, 1), ("r", 1, 0, -1), ("t", 0, 1, 1), ("r", 1, 0, 1), ("s", 1, 1, 3, 1),
    ("s", 1, 0, 3, -1), ("s", 1, 0, 1, -1), ("s", 1, 1, 1, -1), ("s", 1, 1, 3, -1), ("s", 1, 1, 1, 1),
    ("r", 2, 1, -1), ("r", 2, 0, 1), ("s", 1, 0, 1, 1), ("t", 0, 0, 1), ("r", 2, 1, 1), ("r", 2, 0, -1),
    ("s", 1, 1, 2, -1), ("s", 2, 1, 3, 1), ("s", 0, 0, 2, 1), ("t", 0, 0, 3), ("t", 0, 1, 2), ("s", 0, 1, 2, 1),
    ("s", 2, 1, 1, -1), ("s", 2, 0, 1, -1), ("s", 2, 0, 3, 1), ("t", 0, 1, 3), ("t", 2, 0, 0), ("t", 1, 1, 0),
    ("t", 1, 0, 0), ("s", 1, 0, 2, -1), ("s", 2, 1, 1, 1), ("t", 1, 1, 1), ("s", 1, 1, 2, 1), ("t", 0, 0, 2),
    ("s", 2, 0, 3, -1), ("s", 1, 0, 2, 1), ("t", 1, 1, 3), ("s", 2, 1, 2, -1), ("s", 2, 1, 0, -1), ("s", 2, 0, 2, -1),
    ("up", 1, 0, 0), ("t", 1, 0, 1), ("up", 1, 0, 1), ("down", 1, 0, 1, 1), ("t", 1, 0, 2), ("t", 1, 0, 3),
    ("t", 2, 1, 0), ("down", 1, 0, 0, 1), ("s", 2, 0, 1, 1), ("t", 1, 1, 2), ("s", 2, 1, 3, -1), ("R", 1, 0, 3, 1),
    ("up", 0, 2, 0), ("R", 1, 1, 3, 1), ("up", 0, 2, 1), ("t", 2, 0, 1), ("t", 2, 0, 3), ("t", 2, 1, 3),
    ("t", 2, 1, 1), ("s", 2, 1, 2, 1), ("down", 1, 0, 1, 0), ("s", 2, 0, 0, -1), ("s", 2, 0, 2, 1),
    ("down", 1, 0, 0, 0), ("L", 1, 1, 1, 1), ("t", 2, 0, 2), ("t", 2, 1, 2), ("down", 0, 2, 1, 0), ("L", 1, 1, 1, 0),
    ("down", 0, 2, 0, 0), ("L", 0, 0, 2, 0), ("F", 0, 1, 0, 0), ("F", 0, 1, 2, 0), ("F", 0, 0, 2, 0),
    ("F", 0, 0, 3, 0), ("F", 0, 0, 1, 0), ("R", 0, 1, 0, 0), ("F", 0, 1, 1, 0), ("R", 0, 0, 0, 0), ("F", 0, 1, 3, 0),
    ("L", 1, 0, 1, 0), ("R", 1, 1, 3, 0), ("R", 1, 0, 0, 0), ("L", 0, 1, 1, 0), ("F", 0, 0, 0, 0), ("up", 1, 1, 0),
    ("up", 1, 1, 1), ("down", 1, 1, 1, 0), ("F", 1, 1, 3, 0), ("L", 1, 0, 1, 1), ("R", 0, 0, 3, 0),
    ("down", 1, 1, 0, 0), ("F", 1, 1, 1, 0), ("F", 1, 0, 1, 0), ("down", 1, 1, 1, 1), ("F", 1, 1, 1, 1),
    ("F", 1, 0, 2, 0), ("F", 1, 1, 2, 0), ("down", 1, 1, 0, 1), ("F", 1, 0, 0, 1), ("F", 1, 0, 0, 0),
    ("F", 1, 0, 2, 1), ("F", 1, 1, 0, 1), ("F", 1, 1, 2, 1), ("up", 2, 2, 0), ("F", 1, 0, 1, 1), ("L", 0, 1, 2, 0),
    ("up", 2, 2, 1), ("A", 0, 0, 3, 0), ("F", 1, 0, 3, 0), ("F", 1, 1, 3, 1), ("down", 2, 2, 1, 0), ("F", 2, 1, 2, 0),
    ("L", 1, 0, 2, 0), ("F", 1, 0, 3, 1), ("F", 2, 1, 1, 0), ("F", 2, 1, 0, 0), ("A", 0, 1, 0, 0),
    ("down", 2, 2, 0, 0), ("F", 2, 0, 3, 0), ("F", 2, 1, 3, 0), ("L", 1, 1, 2, 0), ("L", 2, 0, 2, 0),
    ("L", 2, 0, 1, 0), ("F", 2, 0, 2, 0), ("R", 2, 1, 0, 0), ("L", 1, 1, 2, 1), ("F", 1, 1, 0, 0), ("R", 1, 0, 3, 0),
    ("A", 0, 0, 2, 0), ("R", 0, 1, 3, 0), ("F", 2, 0, 1, 0), ("L", 1, 0, 2, 1), ("A", 1, 0, 1, 0), ("A", 1, 0, 2, 1),
    ("A", 1, 1, 2, 1), ("A", 1, 1, 2, 0), ("A", 1, 0, 2, 0), ("A", 2, 1, 2, 0), ("R", 2, 1, 3, 0), ("L", 2, 1, 1, 0),
    ("L", 2, 1, 2, 0), ("S", 0, 1, 0, 0), ("A", 1, 0, 0, 0), ("A", 2, 1, 3, 0), ("A", 2, 1, 0, 0), ("A", 1, 0, 0, 1),
    ("A", 1, 0, 1, 1), ("A", 2, 0, 2, 0), ("A", 1, 1, 3, 1), ("A", 2, 1, 1, 0), ("A", 1, 0, 3, 1), ("A", 1, 1, 1, 1),
    ("A", 2, 0, 1, 0), ("A", 1, 1, 3, 0), ("F", 2, 0, 0, 0), ("A", 1, 1, 1, 0), ("A", 2, 0, 3, 0), ("A", 1, 0, 3, 0),
    ("R", 2, 0, 3, 0), ("A", 0, 1, 1, 0), ("S", 1, 1, 2, 0), ("S", 1, 0, 2, 1), ("S", 1, 0, 0, 0), ("A", 0, 1, 3, 0),
    ("A", 0, 1, 2, 0), ("S", 1, 0, 2, 0), ("R", 1, 0, 0, 1), ("A", 1, 1, 0, 1), ("R", 1, 1, 0, 1), ("S", 1, 1, 2, 1),
    ("S", 2, 1, 2, 0), ("S", 2, 1, 1, 0), ("S", 2, 1, 3, 0), ("S", 2, 0, 2, 0), ("R", 2, 0, 0, 0), ("A", 0, 0, 1, 0),
    ("S", 1, 0, 1, 1), ("A", 2, 0, 0, 0), ("S", 1, 1, 3, 1), ("L", 0, 0, 1, 0), ("S", 2, 0, 3, 0), ("S", 2, 0, 1, 0),
    ("S", 1, 1, 3, 0), ("S", 1, 0, 3, 1), ("B", 1, 0, 1, 1), ("B", 1, 0, -1, 1), ("S", 1, 1, 1, 1), ("S", 1, 1, 1, 0),
    ("S", 2, 1, 0, 0), ("B", 1, 1, 1, 0), ("R", 1, 1, 0, 0), ("B", 1, 1, 1, 1), ("B", 1, 1, -1, 0), ("A", 1, 1, 0, 0),
    ("A", 0, 0, 0, 0), ("B", 1, 1, -1, 1), ("S", 1, 0, 1, 0), ("S", 0, 1, 1, 0), ("S", 1, 0, 3, 0), ("S", 0, 1, 3, 0),
    ("B", 1, 0, 1, 0), ("S", 0, 1, 2, 0), ("S", 1, 0, 0, 1), ("B", 1, 0, -1, 0), ("Z", 2, 1, 0), ("S", 0, 0, 2, 0),
    ("S", 0, 0, 3, 0), ("S", 1, 1, 0, 1), ("S", 2, 0, 0, 0), ("Z", 2, 0, 0), ("S", 0, 0, 1, 0), ("Z", 1, 0, 1),
    ("S", 1, 1, 0, 0), ("Z", 1, 1, 0), ("Z", 1, 1, 1), ("Z", 1, 0, 0), ("S", 0, 0, 0, 0), ("Z", 0, 0, 0),
    ("Z", 0, 1, 0), ("X", 0, 0, 0), ("X", 1, 0, 1), ("X", 2, 0, 0), ("X", 2, 1, 0), ("X", 1, 1, 0), ("X", 1, 1, 1),
    ("X", 0, 1, 0), ("X", 1, 0, 0),
)


def kernel(
    sel_hbm, gate_hbm, tok_ref, wg_ref, wu_ref, wd_ref, slots_ref, comb_ref,
    sel_ref, gate_ref, tok_v, wg_v, wu_v, wd_v, send4, recv4, exit4, ret4, rows, part, hid, relay, fin_l, fin_r,
    summed, relay1, fin1_l, fin1_r, slots32, send_sem, recv_sem, load_sem,
):
    slot = sel_hbm.shape[0]
    tok_dev, width = tok_ref.shape
    groups = 2 * RING
    n_slots = groups * slot
    halfw = width // 2
    quart = width // 4
    subw = [halfw // n for n in SUBS]
    chunk = [r.shape[1] for r in rows]
    batch_of = {g: h for h, batch in enumerate(BATCHES) for g in batch}

    dp = lax.axis_index("dp")
    ex = lax.axis_index("expert")
    my_x, my_z = dp // RING, dp % RING
    my_y, my_c = ex // 2, ex % 2

    def at_x(step):
        return (((my_x + step + RING) % RING) * RING + my_z, ex)

    def at_z(step):
        return (my_x * RING + (my_z + step + RING) % RING, ex)

    def expert_at(g):
        return ((my_y + g // 2) % RING) * 2 + (my_c + g % 2) % 2

    def at_group(g):
        return (dp, expert_at(g))

    def back(g):
        return ((RING - g // 2) % RING) * 2 + g % 2

    barrier = pltpu.get_barrier_semaphore()
    partners = [at(step) for at in (at_x, at_z) for step in (1, -1, 2)] + [at_group(g) for g in range(1, groups)]
    for who in partners:
        pl.semaphore_signal(barrier, inc=1, device_id=who, device_id_type=MESH)

    loads = {}
    loads["sel"] = pltpu.make_async_copy(sel_hbm, sel_ref, load_sem.at[7])
    loads["gate"] = pltpu.make_async_copy(gate_hbm, gate_ref, load_sem.at[8])
    loads["sel"].start()
    tokw = width // 4
    for i in range(4):
        cols = pl.ds(i * tokw, tokw)
        loads[i] = pltpu.make_async_copy(tok_ref.at[:, cols], tok_v.at[:, cols], load_sem.at[i])
        loads[i].start()
    for i, (name, src, dst) in enumerate(
        (("wg", wg_ref, wg_v), ("wu", wu_ref, wu_v), ("wd", wd_ref, wd_v)), 4
    ):
        loads[name] = pltpu.make_async_copy(src, dst, load_sem.at[i])
        loads[name].start()

    loads["gate"].start()

    def loaded(*names):
        for name in names:
            if name in loads:
                loads.pop(name).wait()

    recv_of, recv_bytes, send_bytes = {}, {}, {}

    def together(key):
        kind, h = key[0], key[1]
        if kind == "in":
            return ("own", batch_of[h])
        if kind == "r":
            return key[:3]
        if kind == "t":
            return ("up", h, 1 if h in SPLIT else 2)
        if kind == "s" and key[4] != (1 if key[3] in RSET else -1):
            return ("up", h, int(key[3] == 2) if h in SPLIT else 2)
        if kind in ("L", "R"):
            return ("S", *key[1:])
        if kind in ("l1", "r1") or (kind == "F1" and h in DIRECT):
            return ("Z", *key[1:])
        if kind == "b":
            return ("Z", h, key[2], key[4])
        return key[:4] if kind == "X" else key

    def outbox(key):
        kind, h = key[0], key[1]
        if kind == "in":
            return 0
        return (1 if kind in "fsrt" else 4 if kind != "X" else 7) + h

    def size(ref):
        n = 2
        for dim in ref.shape:
            n *= dim
        return n

    def wait_for(sem, n):
        unit = 2 * slot * width
        if n % (4 * unit) == 0:
            ref = rows[1].at[pl.ds(0, n // (4 * unit))]
        elif n % (2 * unit) == 0 and n > 8 * unit:
            ref = rows[0].at[pl.ds(0, n // (2 * unit))]
        elif n % unit == 0:
            ref = exit4.at[pl.ds(0, n // unit)]
        else:
            ref = exit4.at[pl.ds(0, 2 * n // unit), :, pl.ds(0, halfw)]
        assert size(ref) == n
        pltpu.make_async_copy(ref, ref, sem).wait()

    def remote(key, src, dst, who):
        name, box = together(key), outbox(key)
        i = recv_of.setdefault(name, len(recv_of))
        recv_bytes[name] = recv_bytes.get(name, 0) + size(dst)
        send_bytes[box] = send_bytes.get(box, 0) + size(src)
        pltpu.make_async_remote_copy(
            src_ref=src, dst_ref=dst, send_sem=send_sem.at[box], recv_sem=recv_sem.at[i],
            device_id=who, device_id_type=MESH,
        ).start()

    def need(*names):
        for name in names:
            if name in recv_bytes:
                wait_for(recv_sem.at[recv_of[name]], recv_bytes.pop(name))

    def drain(*boxes):
        for box in boxes:
            wait_for(send_sem.at[box], send_bytes.pop(box))

    near = [back(g) for g in BATCHES[0] + BATCHES[1] if g > 0]
    far = [back(g) for g in BATCHES[2]]
    with jax.named_scope("pick"):
        loaded("sel")
        row_id = lax.broadcasted_iota(jnp.int32, (n_slots, tok_dev), 0)
        lane_id = lax.broadcasted_iota(jnp.int32, (n_slots, tok_dev), 1)
        idx = jnp.full((n_slots, tok_dev), -1, jnp.int32)
        for g in range(groups):
            e = expert_at(g)
            for j in range(slot):
                idx = jnp.where(row_id == g * slot + j, sel_ref[j, e], idx)
        onehot = jnp.where(lane_id == idx, 1.0, 0.0).astype(BF16)
    for i in range(4):
        with jax.named_scope("tok"):
            loaded(i)
        with jax.named_scope("sel"):
            cols = slice(i * tokw, (i + 1) * tokw)
            slots32[:, cols] = jnp.dot(onehot, tok_v[:, cols], preferred_element_type=F32)
            for g in near:
                send4[g, :, cols] = slots32[g * slot : (g + 1) * slot, cols].astype(BF16)
    with jax.named_scope("barrier"):
        pl.semaphore_wait(barrier, len(partners))
    for g in near:
        remote(("in", back(g)), send4.at[g], recv4.at[back(g)], at_group(g))
    for g in far:
        send4[g] = slots32[g * slot : (g + 1) * slot, :].astype(BF16)
        remote(("in", back(g)), send4.at[g], recv4.at[back(g)], at_group(g))
    recv4[0] = slots32[0:slot, :].astype(BF16)
    loaded("gate")

    lane8 = lax.broadcasted_iota(jnp.int32, (8, 128), 1)
    idx_l = jnp.full((8, 128), -1, jnp.int32)
    gate_l = jnp.zeros((8, 128), F32)
    for g in range(groups):
        e = expert_at(g)
        for j in range(slot):
            here = lane8 % n_slots == g * slot + j
            idx_l = jnp.where(here, sel_ref[j, e], idx_l)
            gate_l = jnp.where(here, gate_ref[j, e], gate_l)
    g1 = gate_l.astype(BF16).astype(F32)
    rest = gate_l - g1
    g2 = rest.astype(BF16).astype(F32)
    g3 = (rest - g2).astype(BF16).astype(F32)
    term = lane8 // n_slots
    gate3 = jnp.where(term == 0, g1, jnp.where(term == 1, g2, jnp.where(term == 2, g3, 0.0)))
    tok_id = lax.broadcasted_iota(jnp.int32, (tok_dev, 128), 0)
    hit = tok_id == idx_l[0:1, :]
    comb_ref[...] = jnp.where(hit, gate3[0:1, :], 0.0).astype(BF16)

    def cut(p, lo=0, n=halfw):
        return pl.ds(p * halfw + lo, n)

    def pos(p, d1, d2):
        d1, d2 = d1 % RING, d2 % RING
        return PLACE[(d2, d1) if p == 0 else (d1, d2)]

    def first(p, step):
        return at_x(step) if p == 0 else at_z(step)

    def second(p, step):
        return at_z(step) if p == 0 else at_x(step)

    def own(h):
        need(("own", h))
        for i, g in enumerate(BATCHES[h]):
            slots32[i * slot : (i + 1) * slot, :] = recv4[g].astype(F32)
        rows[h][0] = slots32[0 : chunk[h], :].astype(BF16)

    def to_first(key, h, p, d1, step, lo, n):
        remote(
            key, rows[h].at[pos(p, d1, 0), :, cut(p, lo, n)],
            rows[h].at[pos(p, d1 - step, 0), :, cut(p, lo, n)], first(p, step),
        )

    def to_second(key, h, p, d1, d2, step):
        remote(
            key, rows[h].at[pos(p, d1, d2), :, cut(p)],
            rows[h].at[pos(p, d1, d2 - step), :, cut(p)], second(p, step),
        )

    def send_first(h, p, step):
        to_first(("f", h, p, step), h, p, 0, step, 0, halfw)

    def pass_first(h, p, step):
        need(("f", h, p, step))
        to_first(("r", h, p, step), h, p, -step, step, 0 if step == 1 else quart, quart)

    def send_second(h, p, d1, step):
        if d1 == 2:
            need(("r", h, p))
        elif d1 != 0:
            need(("f", h, p, 1 if d1 == 3 else -1))
        to_second(("s", h, p, d1, step), h, p, d1, 0, step)

    def pass_second(h, p, d1):
        step = 1 if d1 in RSET else -1
        need(("s", h, p, d1, step))
        to_second(("t", h, p, d1), h, p, d1, -step, step)

    tn = hid[0].shape[1] // 2
    places = (slice(0, len(EARLY)), slice(len(EARLY), RING * RING), slice(0, RING * RING))

    def held(h, b):
        return slice(places[b].start * chunk[h], places[b].stop * chunk[h])

    def up(h, b, n):
        for p in range(2):
            if b >= 1:
                need(("r", h, p))
            for step in (1, -1):
                need(("f", h, p, step))
                for d1 in RSET if step == 1 else LSET:
                    if b >= 1 or d1 != 2:
                        need(("s", h, p, d1, step))
        need(("up", h, b))
        loaded("wg", "wu")
        lhs = rows[h][places[b]].reshape(-1, width)
        cols = slice(n * tn, (n + 1) * tn)
        gate_val = jnp.dot(lhs, wg_v[:, cols], preferred_element_type=F32)
        up_val = jnp.dot(lhs, wu_v[:, cols], preferred_element_type=F32)
        hid[h][held(h, b), cols] = (gate_val / (1.0 + jnp.exp(-gate_val)) * up_val).astype(BF16)

    dn = 512

    def down(h, b, p, i):
        loaded("wd")
        start = p * halfw + i * subw[h]
        for c in range(start, start + subw[h], dn):
            cols = slice(c, c + dn)
            val = jnp.dot(hid[h][held(h, b), :], wd_v[:, cols], preferred_element_type=F32)
            part[h][places[b], :, cols] = val.astype(BF16).reshape(-1, chunk[h], dn)

    def sub(h, i, lo=0, n=None):
        return pl.ds(i * subw[h] + lo, subw[h] if n is None else n)

    def psub(h, p, i):
        return cut(p, i * subw[h], subw[h])

    def send_far(h, p, d1, i):
        step = 1 if d1 in RSET else -1
        remote(
            ("F", h, p, d1, i), part[h].at[pos(p, d1, 2), :, psub(h, p, i)],
            relay[h].at[p, d1, :, sub(h, i)], second(p, step),
        )

    def send_left_of(h, p, d1, i):
        remote(
            ("L", h, p, d1, i), part[h].at[pos(p, d1, 1), :, psub(h, p, i)],
            fin_l[h].at[p, d1, :, sub(h, i)], second(p, 1),
        )

    def send_right_of(h, p, d1, i):
        remote(
            ("R", h, p, d1, i), part[h].at[pos(p, d1, 3), :, psub(h, p, i)],
            fin_r[h].at[p, d1, :, sub(h, i)], second(p, -1),
        )

    def add_far(h, p, d1, i):
        need(("F", h, p, d1, i))
        right = d1 in RSET
        mine = part[h][pos(p, d1, 1 if right else 3), :, psub(h, p, i)]
        here = relay[h].at[p, d1, :, sub(h, i)]
        here[...] = (here[...].astype(F32) + mine.astype(F32)).astype(BF16)
        if right:
            remote(("L", h, p, d1, i), here, fin_l[h].at[p, d1, :, sub(h, i)], second(p, 1))
        else:
            remote(("R", h, p, d1, i), here, fin_r[h].at[p, d1, :, sub(h, i)], second(p, -1))

    def add_up(h, p, d1, i):
        need(("S", h, p, d1, i))
        mine = part[h][pos(p, d1, 0), :, psub(h, p, i)]
        total = (
            mine.astype(F32)
            + fin_l[h][p, d1, :, sub(h, i)].astype(F32)
            + fin_r[h][p, d1, :, sub(h, i)].astype(F32)
        )
        summed[h][p, d1, :, sub(h, i)] = total.astype(BF16)
        lo, hi = sub(h, i, 0, subw[h] // 2), sub(h, i, subw[h] // 2, subw[h] // 2)
        if h in DIRECT:
            if d1 != 0:
                name, dst, step = {2: ("F1", relay1, 2), 1: ("l1", fin1_l, 1), 3: ("r1", fin1_r, -1)}[d1]
                remote(
                    (name, h, p, i), summed[h].at[p, d1, :, sub(h, i)], dst[h].at[p, :, sub(h, i)],
                    first(p, step),
                )
            return
        if d1 == 2:
            remote(("F1", h, p, 1, i), summed[h].at[p, 2, :, lo], relay1[h].at[p, :, lo], first(p, 1))
            remote(("F1", h, p, -1, i), summed[h].at[p, 2, :, hi], relay1[h].at[p, :, hi], first(p, -1))
        elif d1 == 1:
            remote(("l1", h, p, i), summed[h].at[p, 1, :, hi], fin1_l[h].at[p, :, hi], first(p, 1))
        elif d1 == 3:
            remote(("r1", h, p, i), summed[h].at[p, 3, :, lo], fin1_r[h].at[p, :, lo], first(p, -1))

    def add_first(h, p, step, i):
        need(("F1", h, p, step, i))
        d1 = 1 if step == 1 else 3
        cols = sub(h, i, 0 if step == 1 else subw[h] // 2, subw[h] // 2)
        here = relay1[h].at[p, :, cols]
        here[...] = (here[...].astype(F32) + summed[h][p, d1, :, cols].astype(F32)).astype(BF16)
        dst = fin1_l if step == 1 else fin1_r
        remote(("b", h, p, step, i), here, dst[h].at[p, :, cols], first(p, step))

    def finish(h, p, i):
        need(("Z", h, p, i))
        total = (
            summed[h][p, 0, :, sub(h, i)].astype(F32)
            + fin1_l[h][p, :, sub(h, i)].astype(F32)
            + fin1_r[h][p, :, sub(h, i)].astype(F32)
        )
        if h in DIRECT:
            total += relay1[h][p, :, sub(h, i)].astype(F32)
        slots32[0 : chunk[h], psub(h, p, i)] = total
        for r, g in enumerate(BATCHES[h]):
            value = slots32[r * slot : (r + 1) * slot, psub(h, p, i)].astype(BF16)
            if g == 0:
                ret4[0, :, psub(h, p, i)] = value
            else:
                exit4[g, :, psub(h, p, i)] = value
                remote(
                    ("X", h, p, i, back(g)), exit4.at[g, :, psub(h, p, i)],
                    ret4.at[back(g), :, psub(h, p, i)], at_group(g),
                )

    def take(h, p, i):
        need(("X", h, p, i))
        for g in BATCHES[h]:
            slots_ref[g * slot : (g + 1) * slot, psub(h, p, i)] = ret4[g, :, psub(h, p, i)].astype(F32)

    steps = {
        "own": own, "f": send_first, "r": pass_first, "s": send_second, "t": pass_second,
        "up": up, "down": down, "F": send_far, "L": send_left_of, "R": send_right_of,
        "A": add_far, "S": add_up, "B": add_first, "Z": finish, "X": take,
    }
    ends = [i for i, entry in enumerate(ORDER) if entry[0] == "Z"]
    for at, (name, *args) in enumerate(ORDER):
        with jax.named_scope("_".join(str(a) for a in (name, *args))):
            steps[name](*args)
        if at == ends[-1]:
            with jax.named_scope("drain"):
                drain(*range(9))
    assert len(recv_of) == N_RECV, len(recv_of)
    with jax.named_scope("last_sends"):
        drain(9)


def combine_kernel(slots_ref, comb_ref, out_ref, out_v, out_sem):
    width = slots_ref.shape[1]
    n = 1024
    stores = []
    for k, c in enumerate(range(0, width, n)):
        value = slots_ref[:, c : c + n].astype(BF16)
        stack = jnp.concatenate([value, value, value, jnp.zeros_like(value)], axis=0)
        out_v[:, c : c + n] = jnp.dot(
            comb_ref[...], stack, preferred_element_type=F32).astype(BF16)
        store = pltpu.make_async_copy(
            out_v.at[:, pl.ds(c, n)], out_ref.at[:, pl.ds(c, n)], out_sem.at[k])
        store.start()
        stores.append(store)
    for store in stores:
        store.wait()


def per_device(tokens, select, gates, w_gate, w_up, w_down):
    tok_dev, width = tokens.shape
    slot = select.shape[1]
    ff = w_gate.shape[2]
    halfw = width // 2

    def vmems(shape):
        return [pltpu.VMEM(shape(slot * len(batch)), BF16) for batch in BATCHES]

    vmem, hbm = pl.BlockSpec(memory_space=pltpu.VMEM), pl.BlockSpec(memory_space=pltpu.HBM)
    slots, comb = pl.pallas_call(
        kernel,
        out_shape=(pltpu.VMEM((8 * slot, width), F32), pltpu.VMEM((tok_dev, 128), BF16)),
        in_specs=[hbm] * 6,
        out_specs=(vmem, vmem),
        scratch_shapes=[
            pltpu.SMEM((slot, 8), jnp.int32),
            pltpu.SMEM((slot, 8), F32),
            pltpu.VMEM((tok_dev, width), BF16),
            pltpu.VMEM((width, ff), BF16),
            pltpu.VMEM((width, ff), BF16),
            pltpu.VMEM((ff, width), BF16),
            pltpu.VMEM((8, slot, width), BF16),
            pltpu.VMEM((8, slot, width), BF16),
            pltpu.VMEM((8, slot, width), BF16),
            pltpu.VMEM((8, slot, width), BF16),
            vmems(lambda c: (16, c, width)),
            vmems(lambda c: (16, c, width)),
            vmems(lambda c: (16 * c, ff)),
            vmems(lambda c: (2, 4, c, halfw)),
            vmems(lambda c: (2, 4, c, halfw)),
            vmems(lambda c: (2, 4, c, halfw)),
            vmems(lambda c: (2, 4, c, halfw)),
            vmems(lambda c: (2, c, halfw)),
            vmems(lambda c: (2, c, halfw)),
            vmems(lambda c: (2, c, halfw)),
            pltpu.VMEM((8 * slot, width), F32),
            pltpu.SemaphoreType.DMA((10,)),
            pltpu.SemaphoreType.DMA((N_RECV,)),
            pltpu.SemaphoreType.DMA((9,)),
        ],
        compiler_params=pltpu.CompilerParams(
            collective_id=0, has_side_effects=True, vmem_limit_bytes=56 * 1024 * 1024
        ),
        name="moe",
    )(
        select.T, gates.T, tokens, w_gate[0], w_up[0], w_down[0],
    )
    return pl.pallas_call(
        combine_kernel,
        out_shape=jax.ShapeDtypeStruct((tok_dev, width), BF16),
        in_specs=[vmem, vmem],
        out_specs=hbm,
        scratch_shapes=[pltpu.VMEM((tok_dev, width), BF16), pltpu.SemaphoreType.DMA((4,))],
        compiler_params=pltpu.CompilerParams(vmem_limit_bytes=8 * 1024 * 1024),
        name="combine",
    )(slots, comb)


def solution(mesh):
    return jax.shard_map(
        per_device,
        mesh=mesh,
        in_specs=(
            P(("dp", "expert"), None),
            P(None, ("dp", "expert")),
            P(None, ("dp", "expert")),
            P("expert", None, "dp"),
            P("expert", None, "dp"),
            P("expert", "dp", None),
        ),
        out_specs=P(("dp", "expert"), None),
        check_vma=False,
    )
```
